32 devices in a mesh: dp: 8 (over y, x, core), tensor: 4 (over z).
Axes of the slice: x: 2, y: 2, z: 4, core: 2. Of those that a mesh axis runs over, the one named last changes fastest.
Arguments:
- tokens: bfloat16 [8192, 1024], P(('dp', 'tensor')), may hold values from -6 to 6
- block_ids: int32 [8, 1024], P('dp'), may hold values from 0 to 7, never falling along the last dimension, each value on 1 to 256 neighbouring positions
- norm1_gain: bfloat16 [1024], P('dp'), may hold values from 0.25 to 1.75
- q_weight: bfloat16 [1024, 2048], P('dp', 'tensor'), may hold values from -0.1875 to 0.1875
- key_projection: bfloat16 [1024, 1024], P('dp', 'tensor'), may hold values from -0.1875 to 0.1875
- value_projection: bfloat16 [1024, 1024], P('dp', 'tensor'), may hold values from -0.1875 to 0.1875
- q_gain: bfloat16 [128], P('dp'), may hold values from 0.25 to 1.75
- k_gain: bfloat16 [128], P('dp'), may hold values from 0.25 to 1.75
- o_weight: bfloat16 [2048, 1024], P('tensor', 'dp'), may hold values from -2 to 2
- norm2_gain: bfloat16 [1024], P('dp'), may hold values from 0.25 to 1.75
- gate_weight: bfloat16 [1024, 3072], P('dp', 'tensor'), may hold values from -0.1875 to 0.1875
- up_weight: bfloat16 [1024, 3072], P('dp', 'tensor'), may hold values from -0.1875 to 0.1875
- down_weight: bfloat16 [3072, 1024], P('tensor', 'dp'), may hold values from -0.109375 to 0.109375
- out_grad: bfloat16 [8192, 1024], P(('dp', 'tensor')), may hold values from -6 to 6
Outputs:
- layer_out: bfloat16 [8192, 1024], P(('dp', 'tensor'))
- tokens_grad: float32 [8192, 1024], P(('dp', 'tensor'))
- norm1_grad: float32 [1024], P('dp')
- q_weight_grad: float32 [1024, 2048], P('dp', 'tensor')
- k_weight_grad: float32 [1024, 1024], P('dp', 'tensor')
- v_weight_grad: float32 [1024, 1024], P('dp', 'tensor')
- q_gain_grad: float32 [128], P('dp')
- k_gain_grad: float32 [128], P('dp')
- o_weight_grad: float32 [2048, 1024], P('tensor', 'dp')
- norm2_grad: float32 [1024], P('dp')
- gate_weight_grad: float32 [1024, 3072], P('dp', 'tensor')
- up_weight_grad: float32 [1024, 3072], P('dp', 'tensor')
- down_weight_grad: float32 [3072, 1024], P('tensor', 'dp')
The draws below stay inside these ranges and needn't reach their ends.
Inputs may be any that keep to these rules, and one draw needn't show every extreme that they name: `block_ids`: in each row block numbers never fall and every number from the least to the largest is used; each block has 1 to 256 tokens and some block has exactly 256.
All inputs are finite; a program needn't handle non-finite values.
Results may differ from the reference program's by a relative error of at most 0.017.
Values may be sent and summed in bfloat16 or wider, within the bound.
A program may use at most 128 MiB of HBM per device.

```python
import math
import jax
import jax.numpy as jnp
import numpy as np
from jax import lax

MODEL_WIDTH = 1024
QUERY_HEADS = 16
KEY_VALUE_HEADS = 8
HEAD_SIZE = 128
FF = 3072
BLOCK = 256
LENGTH = 1024
SEQS = 8
TOKENS = 8192


def with_spikes(entries, own_key, source, target, blocks, factor):
    owner, partner = [(jnp.arange(entries.shape[position]) // (entries.shape[position] // blocks)).reshape([-1 if axis == position else 1 for axis in range(entries.ndim)]) for position in (source, target)]
    chosen = jax.random.permutation(own_key, blocks)[partner]
    strong = (owner == chosen) | (owner == (partner + blocks // 2) % blocks)
    return jnp.where(strong, factor * entries, entries)


def shard_levels(rng, dims, shards, smallest, high):
    level, own = 1.0, jax.random.fold_in(rng, 6)
    for position, parts in shards:
        steps = jnp.exp(jax.random.uniform(jax.random.fold_in(own, position), (parts,), jnp.float32, smallest / len(shards), high / len(shards)))
        level = level * jnp.repeat(steps, dims[position] // parts).reshape([-1 if axis == position else 1 for axis in range(len(dims))])
    return level


def length_profile(amount, total, bound, skew):
    portions = [(1 << 20) // math.isqrt(standing ** skew) + 1 for standing in range(2, amount + 1)]
    spare, counts = total - bound - (amount - 1), [1] * (amount - 1)
    while spare > 0:
        free = [i for i in range(amount - 1) if counts[i] < bound]
        whole, left = sum([portions[i] for i in free]), spare
        for i in free:
            extra = min(bound - counts[i], max(1, left * portions[i] // whole), spare)
            counts[i] = counts[i] + extra
            spare = spare - extra
    return np.array([bound] + counts)


def ragged_sizes(rng, amount, total, most, slope):
    if amount == 2:
        one = jax.random.randint(rng, (), max(1, total - most), min(most, total - 1) + 1)
        return jnp.stack([one, total - one])
    tallies = jnp.asarray(length_profile(amount, total, most, slope), jnp.int32)
    pairs = (amount - 1) // 2
    donor, sink = tallies[1:1 + 2 * pairs:2], tallies[2:2 + 2 * pairs:2]
    slack = jnp.minimum(donor - 1, most - sink)
    moved = jax.random.randint(jax.random.fold_in(rng, 1), (pairs,), 0, 1 << 20) % (slack + 1)
    tallies = tallies.at[1:1 + 2 * pairs:2].set(donor - moved).at[2:2 + 2 * pairs:2].set(sink + moved)
    return tallies[jax.random.permutation(jax.random.fold_in(rng, 2), amount)]


def scatter_about(key, extent, scale, bound, shards=(), kind=jnp.bfloat16):
    level = shard_levels(key, extent, shards, -0.22, 0.18) if shards else 1.0
    entries = jax.random.normal(key, extent, jnp.float32) * scale * level
    return jnp.minimum(jnp.maximum(entries, -bound), bound).astype(kind)


def noise_with(stream_key, dims, scale, reach, pieces, heavy, held_as=jnp.bfloat16):
    values = scale * jax.random.normal(stream_key, dims, jnp.float32)
    if pieces:
        values = values * shard_levels(stream_key, dims, pieces, -0.22, 0.18)
    return jnp.clip(with_spikes(values, jax.random.fold_in(stream_key, 3), *heavy), -reach, reach).astype(held_as)


def setup_inputs(seed: int = 0) -> dict:
    key_of = jax.random.split(jax.random.key(seed), 15)
    return {
        "tokens": scatter_about(key_of[0], (TOKENS, MODEL_WIDTH), 1.0, 6.0, ((0, 32),)),
        "block_ids": jax.vmap(lambda own: jnp.searchsorted(jnp.cumsum(ragged_sizes(own, 2 * LENGTH // BLOCK, LENGTH, BLOCK, 1)), jnp.arange(LENGTH), side="right"))(jax.random.split(key_of[1], SEQS)).reshape((SEQS, LENGTH)).astype(jnp.int32),
        "norm1_gain": jnp.clip(1.0 + 0.15 * jax.random.normal(key_of[2], (MODEL_WIDTH,), jnp.float32), 0.25, 1.75).astype(jnp.bfloat16),
        "q_weight": scatter_about(key_of[3], (MODEL_WIDTH, QUERY_HEADS * HEAD_SIZE), MODEL_WIDTH ** -0.5, 0.1875, ((0, 8), (1, 4))),
        "key_projection": scatter_about(key_of[4], (MODEL_WIDTH, KEY_VALUE_HEADS * HEAD_SIZE), MODEL_WIDTH ** -0.5, 0.1875, ((0, 8), (1, 4))),
        "value_projection": scatter_about(key_of[5], (MODEL_WIDTH, KEY_VALUE_HEADS * HEAD_SIZE), MODEL_WIDTH ** -0.5, 0.1875, ((0, 8), (1, 4))),
        "q_gain": jnp.clip(1.0 + 0.15 * jax.random.normal(key_of[6], (HEAD_SIZE,), jnp.float32), 0.25, 1.75).astype(jnp.bfloat16),
        "k_gain": jnp.clip(1.0 + 0.15 * jax.random.normal(key_of[7], (HEAD_SIZE,), jnp.float32), 0.25, 1.75).astype(jnp.bfloat16),
        "o_weight": scatter_about(key_of[8], (QUERY_HEADS * HEAD_SIZE, MODEL_WIDTH), 8 ** -0.5, 2.0, ((0, 4), (1, 8))),
        "norm2_gain": jnp.clip(1.0 + 0.15 * jax.random.normal(key_of[9], (MODEL_WIDTH,), jnp.float32), 0.25, 1.75).astype(jnp.bfloat16),
        "gate_weight": scatter_about(key_of[10], (MODEL_WIDTH, FF), MODEL_WIDTH ** -0.5, 0.1875, ((0, 8), (1, 4))),
        "up_weight": scatter_about(key_of[11], (MODEL_WIDTH, FF), MODEL_WIDTH ** -0.5, 0.1875, ((0, 8), (1, 4))),
        "down_weight": scatter_about(key_of[12], (FF, MODEL_WIDTH), FF ** -0.5, 0.109375, ((0, 4), (1, 8))),
        "out_grad": noise_with(key_of[13], (TOKENS, MODEL_WIDTH), 1.0, 6.0, ((0, 32),), (0, 1, 32, 2.75)),
    }


HIGHEST = lax.Precision.HIGHEST
EPSILON = 1e-06
BASE_FREQ = 1000000.0
MASKED = -1e+30

@jax.custom_vjp
def reduced_precision(v):
    return lax.optimization_barrier(v.astype(jnp.bfloat16)).astype(jnp.float32)

@jax.custom_vjp
def reduced_backward(v):
    return v

def low_keep(v):
    return (reduced_precision(v), None)

def low_pass(kept, grad):
    return (grad,)

def back_keep(v):
    return (v, None)

def back_low(kept, grad):
    return (reduced_precision(grad),)
reduced_precision.defvjp(low_keep, low_pass)
reduced_backward.defvjp(back_keep, back_low)

def rms_scale(values, gain):
    return values * lax.rsqrt(lax.optimization_barrier(jnp.mean(values * values, axis=-1, keepdims=True)) + EPSILON) * gain

def rotate(values, cosine, sine):
    half = values.shape[-1] // 2
    turned = jnp.concatenate([-values[..., half:], values[..., :half]], axis=-1)
    return values * cosine + turned * sine

def angles(sequence_length, width):
    half = width // 2
    inverse = BASE_FREQ ** (-2.0 * jnp.arange(half, dtype=jnp.float32) / width)
    places = jnp.arange(sequence_length, dtype=jnp.float32)
    turns = places[:, None] * inverse[None, :]
    turns = jnp.concatenate([turns, turns], axis=-1)
    return (jnp.cos(turns)[:, None, :], jnp.sin(turns)[:, None, :])

def matrix_product(left, right):
    return jnp.dot(left, right, precision=HIGHEST, preferred_element_type=jnp.float32)

def attend(queries_rot, keys_rot, rotated_values, block_of):
    sequence_length = queries_rot.shape[0]
    extent_size = min(512, sequence_length)
    count = sequence_length // extent_size
    head_group = QUERY_HEADS // KEY_VALUE_HEADS
    scale = HEAD_SIZE ** (-0.5)

    def one_block(inputs):
        query_block_index, block_rows = inputs
        grouped_heads = query_block_index.reshape(extent_size, KEY_VALUE_HEADS, head_group, HEAD_SIZE)
        scores = reduced_backward(jnp.einsum('qhgd,khd->hgqk', grouped_heads, keys_rot, precision=HIGHEST) * scale)
        seen = block_of[None, :] <= block_rows[:, None]
        scores = jnp.where(seen, scores, MASKED)
        weights = jax.nn.softmax(scores, axis=-1)
        mixed = jnp.einsum('hgqk,khd->qhgd', reduced_precision(weights), rotated_values, precision=HIGHEST)
        return mixed.reshape(extent_size, QUERY_HEADS * HEAD_SIZE)
    blocks = lax.map(jax.checkpoint(one_block), (queries_rot.reshape(count, extent_size, QUERY_HEADS, HEAD_SIZE), block_of.reshape(count, extent_size)))
    return blocks.reshape(sequence_length, QUERY_HEADS * HEAD_SIZE)

def layer(acts, block_of, gain_first, q_mat, key_matrix, value_matrix, q_scale, k_scale, o_mat, gain_second, gate_mat, up_mat, down_mat):
    sequence_length = acts.shape[0]
    normalized_input = reduced_precision(rms_scale(acts, gain_first))
    q_raw = reduced_backward(matrix_product(normalized_input, q_mat)).reshape(sequence_length, QUERY_HEADS, HEAD_SIZE)
    key_unrotated = reduced_backward(matrix_product(normalized_input, key_matrix)).reshape(sequence_length, KEY_VALUE_HEADS, HEAD_SIZE)
    rotated_values = reduced_precision(reduced_backward(matrix_product(normalized_input, value_matrix))).reshape(sequence_length, KEY_VALUE_HEADS, HEAD_SIZE)
    cosine, sine = angles(sequence_length, HEAD_SIZE)
    queries_rot = reduced_precision(rotate(rms_scale(q_raw, q_scale), cosine, sine))
    keys_rot = reduced_precision(rotate(rms_scale(key_unrotated, k_scale), cosine, sine))
    mixed = reduced_precision(reduced_backward(attend(queries_rot, keys_rot, rotated_values, block_of)))
    state = acts + reduced_backward(matrix_product(mixed, o_mat))
    normed_two = reduced_precision(rms_scale(state, gain_second))
    gate_pre = reduced_backward(matrix_product(normed_two, gate_mat))
    up_pre = reduced_backward(matrix_product(normed_two, up_mat))
    inner = reduced_precision(jax.nn.silu(gate_pre) * up_pre)
    return state + reduced_backward(matrix_product(inner, down_mat))

def reference(tokens, block_ids, norm1_gain, q_weight, key_projection, value_projection, q_gain, k_gain, o_weight, norm2_gain, gate_weight, up_weight, down_weight, out_grad):
    params = tuple((item.astype(jnp.float32) for item in (norm1_gain, q_weight, key_projection, value_projection, q_gain, k_gain, o_weight, norm2_gain, gate_weight, up_weight, down_weight)))
    acts_all = tokens.astype(jnp.float32).reshape(SEQS, LENGTH, MODEL_WIDTH)
    grads_all = out_grad.astype(jnp.float32).reshape(SEQS, LENGTH, MODEL_WIDTH)

    def per_sequence(totals, inputs):
        acts, block_of, cotangent = inputs

        def apply(acts_in, *weights):
            return layer(acts_in, block_of, *weights)
        result, pull = jax.vjp(apply, acts, *params)
        grads = pull(cotangent)
        new_totals = tuple((left + right for left, right in zip(totals, grads[1:])))
        return (new_totals, (result.astype(jnp.bfloat16), grads[0]))
    zeros = tuple((jnp.zeros_like(item) for item in params))
    totals, (results, acts_grads) = lax.scan(per_sequence, zeros, (acts_all, block_ids, grads_all))
    return (results.reshape(TOKENS, MODEL_WIDTH), acts_grads.reshape(TOKENS, MODEL_WIDTH), totals[0], totals[1], totals[2], totals[3], totals[4], totals[5], totals[6], totals[7], totals[8], totals[9], totals[10])
```

```python
from functools import partial

import jax
import jax.numpy as jnp
from jax import lax
from jax.sharding import PartitionSpec as P

EPSILON = 1e-06
BASE_FREQ = 1000000.0
MASKED = -1e30
AXES = ("dp", "tensor")


def rms_scale(values, gain):
    return values * lax.rsqrt(jnp.mean(values * values, axis=-1, keepdims=True) + EPSILON) * gain


def rotate(values, cosine, sine):
    half = values.shape[-1] // 2
    turned = jnp.concatenate([-values[..., half:], values[..., :half]], axis=-1)
    return values * cosine + turned * sine


def shape_heads(raw, gain, cosine, sine):
    return rotate(rms_scale(raw, gain), cosine, sine)


def contract_rows(left, right):
    return lax.dot_general(
        left, right, (((0,), (0,)), ((), ())), preferred_element_type=jnp.float32
    )


def contract_cols(left, right):
    return lax.dot_general(
        left, right, (((1,), (1,)), ((), ())), preferred_element_type=jnp.float32
    )


def attend_forward(queries_rot, keys_rot, rotated_values, block_of):
    sequence_length, heads, width = queries_rot.shape
    kv_heads = keys_rot.shape[1]
    head_group = heads // kv_heads
    extent_size = min(512, sequence_length)
    count = sequence_length // extent_size
    scale = width ** (-0.5)

    def one_block(inputs):
        query_block_index, block_rows = inputs
        grouped_heads = query_block_index.reshape(extent_size, kv_heads, head_group, width)
        scores = (
            jnp.einsum(
                "qhgd,khd->hgqk", grouped_heads, keys_rot, preferred_element_type=jnp.float32
            )
            * scale
        )
        seen = block_of[None, :] <= block_rows[:, None]
        scores = jnp.where(seen, scores, MASKED)
        highest = jnp.max(scores, axis=-1, keepdims=True)
        raised = jnp.exp(scores - highest)
        totals = jnp.sum(raised, axis=-1, keepdims=True)
        weights = (raised / totals).astype(jnp.bfloat16)
        mixed = jnp.einsum(
            "hgqk,khd->qhgd", weights, rotated_values, preferred_element_type=jnp.float32
        )
        return (
            mixed.reshape(extent_size, heads * width),
            highest[..., 0] + jnp.log(totals[..., 0]),
        )

    mixed, log_totals = lax.map(
        one_block,
        (
            queries_rot.reshape(count, extent_size, heads, width),
            block_of.reshape(count, extent_size),
        ),
    )
    return (mixed.reshape(sequence_length, heads * width), log_totals)


def attend_backward(queries_rot, keys_rot, rotated_values, block_of, log_totals, mixed_grad):
    sequence_length, heads, width = queries_rot.shape
    kv_heads = keys_rot.shape[1]
    head_group = heads // kv_heads
    extent_size = min(512, sequence_length)
    count = sequence_length // extent_size
    scale = width ** (-0.5)

    def one_block(carry, inputs):
        key_acc, value_acc = carry
        query_block_index, block_rows, log_block, grad_block = inputs
        grouped_heads = query_block_index.reshape(extent_size, kv_heads, head_group, width)
        grad_grouped = grad_block.reshape(extent_size, kv_heads, head_group, width)
        scores = (
            jnp.einsum(
                "qhgd,khd->hgqk", grouped_heads, keys_rot, preferred_element_type=jnp.float32
            )
            * scale
        )
        seen = block_of[None, :] <= block_rows[:, None]
        scores = jnp.where(seen, scores, MASKED)
        weights = jnp.exp(scores - log_block[..., None])
        weight_grad = jnp.einsum(
            "qhgd,khd->hgqk", grad_grouped, rotated_values, preferred_element_type=jnp.float32
        )
        centre = jnp.sum(weights * weight_grad, axis=-1, keepdims=True)
        score_grad = (weights * (weight_grad - centre)).astype(jnp.bfloat16)
        query_grad = (
            jnp.einsum("hgqk,khd->qhgd", score_grad, keys_rot, preferred_element_type=jnp.float32)
            * scale
        )
        key_acc = (
            key_acc
            + jnp.einsum(
                "hgqk,qhgd->khd", score_grad, grouped_heads, preferred_element_type=jnp.float32
            )
            * scale
        )
        value_acc = value_acc + jnp.einsum(
            "hgqk,qhgd->khd",
            weights.astype(jnp.bfloat16),
            grad_grouped,
            preferred_element_type=jnp.float32,
        )
        return ((key_acc, value_acc), query_grad.reshape(extent_size, heads * width))

    zeros = jnp.zeros((sequence_length, kv_heads, width), jnp.float32)
    (key_grad, value_grad), query_grad = lax.scan(
        one_block,
        (zeros, zeros),
        (
            queries_rot.reshape(count, extent_size, heads, width),
            block_of.reshape(count, extent_size),
            log_totals,
            mixed_grad.reshape(count, extent_size, heads, width),
        ),
    )
    return (query_grad.reshape(sequence_length, heads, width), key_grad, value_grad)


class Links:
    def __init__(self, dp, tensor):
        assert tensor == 4 and dp % 2 == 0 and dp & (dp - 1) == 0
        self.dp, self.tensor = dp, tensor
        self.bits = (dp // 2).bit_length() - 1
        every = [
            (a, c, zh, zl)
            for a in range(dp // 2)
            for c in range(2)
            for zh in range(2)
            for zl in range(2)
        ]

        def flat(a, c, zh, zl):
            return (2 * a + c) * 4 + 2 * zh + zl

        def table(fn):
            return [(flat(*d), flat(*fn(*d))) for d in every]

        self.core_t = table(lambda a, c, zh, zl: (a, 1 - c, zh, zl))
        self.near_t = table(lambda a, c, zh, zl: (a, c, zh, 1 - zl))
        self.swap_t = table(lambda a, c, zh, zl: (a, zh, c, zl))
        self.cross_t = table(lambda a, c, zh, zl: (a, zh, 1 - c, zl))
        self.cross_back_t = [(d, s) for s, d in self.cross_t]
        self.plane_t = [
            table(lambda a, c, zh, zl, b=b: (a ^ (1 << b), c, zh, zl)) for b in range(self.bits)
        ]

    def send(self, x, table):
        return lax.ppermute(x, AXES, table)

    def core(self, x):
        return self.send(x, self.core_t)

    def near(self, x):
        return self.send(x, self.near_t)

    def swap(self, x):
        return self.send(x, self.swap_t)

    def cross(self, x):
        return self.send(x, self.cross_t)

    def cross_back(self, x):
        return self.send(x, self.cross_back_t)

    def order(self, flip):
        return list(range(self.bits))[:: -1 if flip else 1]

    def gather_weight(self, shard, axis, flip):
        slots = {0: self.swap(shard), 1: self.cross(shard)}
        for bit in self.order(flip):
            keys = sorted(slots)
            size = shard.shape[axis]
            got = self.send(
                jnp.concatenate([slots[k] for k in keys], axis=axis), self.plane_t[bit]
            )
            for n, k in enumerate(keys):
                slots[k ^ (2 << bit)] = lax.slice_in_dim(got, n * size, (n + 1) * size, axis=axis)
        return jnp.concatenate([slots[k] for k in sorted(slots)], axis=axis)

    def scatter_grad(self, grad, axis, flip):
        size = grad.shape[axis] // self.dp
        slots = {
            k: lax.slice_in_dim(grad, k * size, (k + 1) * size, axis=axis) for k in range(self.dp)
        }
        for bit in self.order(flip)[::-1]:
            keep = [k for k in sorted(slots) if not k & (2 << bit)]
            sent = jnp.concatenate([slots[k ^ (2 << bit)] for k in keep], axis=axis)
            got = self.send(sent.astype(jnp.bfloat16), self.plane_t[bit])
            slots = {
                k: (
                    slots[k].astype(jnp.float32)
                    + lax.slice_in_dim(got, n * size, (n + 1) * size, axis=axis)
                ).astype(jnp.bfloat16)
                for n, k in enumerate(keep)
            }
        first = self.swap(slots[0])
        second = self.cross_back(slots[1])
        return first.astype(jnp.float32) + second.astype(jnp.float32)

    def gather_rows(self, own):
        beside = self.near(own)
        partner = self.core(own)
        return jnp.concatenate([own, beside, partner, self.core(beside)], axis=0)

    def scatter_rows(self, partial_sum):
        half = partial_sum.shape[0] // 2
        got = self.core(partial_sum[half:])
        both = partial_sum[:half].astype(jnp.float32) + got
        quarter = half // 2
        return both[:quarter] + self.near(both[quarter:].astype(jnp.bfloat16)).astype(jnp.float32)

    def sum_all(self, x):
        x = x + self.core(x)
        x = x + self.near(x)
        for bit in range(self.bits):
            x = x + self.send(x, self.plane_t[bit])
        far = [(d, d ^ 2) for d, _ in self.core_t]
        return x + self.send(x, far)


def reorder_columns(x, index, blocks):
    rows, width = x.shape[0], x.shape[1] // blocks
    return jnp.concatenate(
        [lax.dynamic_slice(x, (0, (index ^ r) * width), (rows, width)) for r in range(blocks)],
        axis=1,
    )


def body(
    links,
    tokens,
    block_ids,
    norm1_gain,
    q_weight,
    key_projection,
    value_projection,
    q_gain,
    k_gain,
    o_weight,
    norm2_gain,
    gate_weight,
    up_weight,
    down_weight,
    out_grad,
):
    dp = links.dp
    dp_index = lax.axis_index("dp")
    t_index = lax.axis_index("tensor")
    own_seq = (dp_index // 2) * 2 + t_index // 2
    own_part = (dp_index % 2) * 2 + t_index % 2

    tokens_own = links.swap(reorder_columns(tokens, dp_index, dp))
    block_of = links.swap(block_ids)[0]
    acts_bf = links.gather_rows(tokens_own)

    kv_weight = jnp.concatenate([key_projection, value_projection], axis=1)
    q_mat = links.gather_weight(q_weight, 0, False)
    kv_mat = links.gather_weight(kv_weight, 0, True)

    gain_width = norm1_gain.shape[0]
    head_part = q_gain.shape[0]
    gains = jnp.concatenate([norm1_gain, norm2_gain, q_gain, k_gain])[None, :]
    gains_all = links.gather_weight(gains, 0, False).astype(jnp.float32)
    first_gain = gains_all[:, :gain_width].reshape(-1)
    second_gain = gains_all[:, gain_width : 2 * gain_width].reshape(-1)
    head_gains = gains_all[own_seq ^ jnp.arange(dp), 2 * gain_width :]
    q_scale = head_gains[:, :head_part].reshape(-1)
    k_scale = head_gains[:, head_part:].reshape(-1)

    o_mat = links.gather_weight(o_weight, 1, False)
    gate_mat = links.gather_weight(gate_weight, 0, False)
    up_mat = links.gather_weight(up_weight, 0, True)
    down_mat = links.gather_weight(down_weight, 1, True)
    grad_full = links.gather_rows(links.swap(reorder_columns(out_grad, dp_index, dp)))

    length = block_of.shape[0]
    head_dim = q_scale.shape[0]
    q_cols = q_weight.shape[1]
    kv_cols = key_projection.shape[1]
    ff_local = gate_weight.shape[1]
    heads = q_cols // head_dim
    kv_heads = kv_cols // head_dim
    quarter = length // 4
    parts = own_part ^ jnp.arange(4)

    places = (parts[:, None] * quarter + jnp.arange(quarter)[None, :]).reshape(-1)
    half_dim = head_dim // 2
    inverse = BASE_FREQ ** (-2.0 * jnp.arange(half_dim, dtype=jnp.float32) / head_dim)
    turns = places.astype(jnp.float32)[:, None] * inverse[None, :]
    turns = jnp.concatenate([turns, turns], axis=-1)
    cosine, sine = jnp.cos(turns)[:, None, :], jnp.sin(turns)[:, None, :]
    block_here = block_of[places]

    acts = acts_bf.astype(jnp.float32)
    normed = rms_scale(acts, first_gain).astype(jnp.bfloat16)
    q_raw = jnp.dot(normed, q_mat, preferred_element_type=jnp.float32).reshape(
        length, heads, head_dim
    )
    kv_raw = jnp.dot(normed, kv_mat, preferred_element_type=jnp.float32)
    key_unrotated = kv_raw[:, :kv_cols].reshape(length, kv_heads, head_dim)
    rotated_values = kv_raw[:, kv_cols:].astype(jnp.bfloat16).reshape(length, kv_heads, head_dim)
    head_shaper = partial(shape_heads, cosine=cosine, sine=sine)
    q_shaped, q_pull = jax.vjp(head_shaper, q_raw, q_scale)
    k_shaped, k_pull = jax.vjp(head_shaper, key_unrotated, k_scale)
    queries_rot = q_shaped.astype(jnp.bfloat16)
    keys_rot = k_shaped.astype(jnp.bfloat16)
    mixed_full, log_totals = attend_forward(queries_rot, keys_rot, rotated_values, block_here)
    mixed = mixed_full.astype(jnp.bfloat16)
    state = acts[:quarter] + links.scatter_rows(
        jnp.dot(mixed, o_mat, preferred_element_type=jnp.float32).astype(jnp.bfloat16)
    )
    normed_two = links.gather_rows(rms_scale(state, second_gain).astype(jnp.bfloat16))
    gate_pre = jnp.dot(normed_two, gate_mat, preferred_element_type=jnp.float32)
    up_pre = jnp.dot(normed_two, up_mat, preferred_element_type=jnp.float32)
    sigmoid_gate = jax.nn.sigmoid(gate_pre)
    silu_gate = gate_pre * sigmoid_gate
    inner = (silu_gate * up_pre).astype(jnp.bfloat16)
    layer_sum = state + links.scatter_rows(
        jnp.dot(inner, down_mat, preferred_element_type=jnp.float32).astype(jnp.bfloat16)
    )
    layer_out = links.swap(reorder_columns(layer_sum.astype(jnp.bfloat16), own_seq, dp))

    inner_grad = contract_cols(grad_full, down_mat)
    down_grad = contract_rows(inner, grad_full).astype(jnp.bfloat16)
    down_sum = links.scatter_grad(down_grad, 1, True)
    gate_grad = (
        inner_grad * up_pre * sigmoid_gate * (1.0 + gate_pre * (1.0 - sigmoid_gate))
    ).astype(jnp.bfloat16)
    up_grad = (inner_grad * silu_gate).astype(jnp.bfloat16)
    normed_two_grad = links.scatter_rows(
        (contract_cols(gate_grad, gate_mat) + contract_cols(up_grad, up_mat)).astype(jnp.bfloat16)
    )
    gate_sum = links.scatter_grad(
        contract_rows(normed_two, gate_grad).astype(jnp.bfloat16), 0, False
    )
    up_sum = links.scatter_grad(contract_rows(normed_two, up_grad).astype(jnp.bfloat16), 0, True)
    state_back, second_part = jax.vjp(rms_scale, state, second_gain)[1](normed_two_grad)
    state_grad = grad_full[:quarter].astype(jnp.float32) + state_back
    state_low = links.gather_rows(state_grad.astype(jnp.bfloat16))
    mixed_grad = contract_cols(state_low, o_mat)
    o_sum = links.scatter_grad(contract_rows(mixed, state_low).astype(jnp.bfloat16), 1, False)
    q_rot_grad, k_rot_grad, v_grad = attend_backward(
        queries_rot, keys_rot, rotated_values, block_here, log_totals, mixed_grad.astype(jnp.bfloat16)
    )
    q_raw_grad, q_part = q_pull(q_rot_grad)
    k_raw_grad, k_part = k_pull(k_rot_grad)
    q_low = q_raw_grad.reshape(length, q_cols).astype(jnp.bfloat16)
    kv_low = jnp.concatenate(
        [k_raw_grad.reshape(length, kv_cols), v_grad.reshape(length, kv_cols)], axis=1
    ).astype(jnp.bfloat16)
    q_sum = links.scatter_grad(contract_rows(normed, q_low).astype(jnp.bfloat16), 0, False)
    kv_sum = links.scatter_grad(contract_rows(normed, kv_low).astype(jnp.bfloat16), 0, True)
    normed_grad = links.scatter_rows(
        (contract_cols(q_low, q_mat) + contract_cols(kv_low, kv_mat)).astype(jnp.bfloat16)
    )
    acts_back, first_part = jax.vjp(rms_scale, acts[:quarter], first_gain)[1](normed_grad)
    tokens_grad = links.swap(
        reorder_columns((state_grad + acts_back).astype(jnp.bfloat16), own_seq, dp)
    ).astype(jnp.float32)

    blocks = own_seq ^ jnp.arange(dp)
    width = gain_width
    shared = jnp.concatenate(
        [
            first_part.reshape(dp, width)[blocks].reshape(-1),
            second_part.reshape(dp, width)[blocks].reshape(-1),
            q_part,
            k_part,
        ]
    )
    shared = links.sum_all(shared)
    model = dp * width
    first_total = lax.dynamic_slice(shared, (dp_index * width,), (width,))
    second_total = lax.dynamic_slice(shared, (model + dp_index * width,), (width,))
    qs_total = lax.dynamic_slice(shared, (2 * model + dp_index * head_part,), (head_part,))
    ks_total = lax.dynamic_slice(
        shared, (2 * model + head_dim + dp_index * head_part,), (head_part,)
    )
    return (
        layer_out,
        tokens_grad,
        first_total,
        q_sum,
        kv_sum[:, :kv_cols],
        kv_sum[:, kv_cols:],
        qs_total,
        ks_total,
        o_sum,
        second_total,
        gate_sum,
        up_sum,
        down_sum,
    )


def solution(mesh):
    links = Links(mesh.shape["dp"], mesh.shape["tensor"])
    return jax.shard_map(
        partial(body, links),
        mesh=mesh,
        in_specs=(
            P(("dp", "tensor"), None),
            P("dp", None),
            P("dp"),
            P("dp", "tensor"),
            P("dp", "tensor"),
            P("dp", "tensor"),
            P("dp"),
            P("dp"),
            P("tensor", "dp"),
            P("dp"),
            P("dp", "tensor"),
            P("dp", "tensor"),
            P("tensor", "dp"),
            P(("dp", "tensor"), None),
        ),
        out_specs=(
            P(("dp", "tensor"), None),
            P(("dp", "tensor"), None),
            P("dp"),
            P("dp", "tensor"),
            P("dp", "tensor"),
            P("dp", "tensor"),
            P("dp"),
            P("dp"),
            P("tensor", "dp"),
            P("dp"),
            P("dp", "tensor"),
            P("dp", "tensor"),
            P("tensor", "dp"),
        ),
        check_vma=False,
    )
```

```python
from functools import partial

import jax
import jax.numpy as jnp
from jax import lax
from jax.experimental import pallas as pl
from jax.experimental.pallas import tpu as pltpu
from jax.sharding import PartitionSpec as P

EPSILON = 1e-06
BASE_FREQ = 1000000.0
AXES = ("dp", "tensor")
LOG2E = 1.4426950408889634


bf16, f32 = jnp.bfloat16, jnp.float32
NT = (((1,), (1,)), ((), ()))
TN = (((0,), (0,)), ((), ()))


def dot(left, right):
    return jnp.dot(left, right, preferred_element_type=f32)


def dot_nt(left, right):
    return lax.dot_general(left, right, NT, preferred_element_type=f32)


def dot_tn(left, right):
    return lax.dot_general(left, right, TN, preferred_element_type=f32)


def rms_rate(values):
    return lax.rsqrt(jnp.mean(values * values, axis=-1, keepdims=True) + EPSILON)


def rms_back(values, gain, grad):
    rate = rms_rate(values)
    shape = values * rate
    inward = grad * gain
    back = rate * (inward - shape * jnp.mean(inward * shape, axis=-1, keepdims=True))
    return back, grad * shape


class Links:
    def __init__(self, dp, tensor):
        assert tensor == 4 and dp % 2 == 0 and dp & (dp - 1) == 0
        self.dp = dp
        self.bits = (dp // 2).bit_length() - 1
        every = [
            (a, c, zh, zl)
            for a in range(dp // 2)
            for c in range(2)
            for zh in range(2)
            for zl in range(2)
        ]

        def flat(a, c, zh, zl):
            return (2 * a + c) * 4 + 2 * zh + zl

        def table(fn):
            return [(flat(*d), flat(*fn(*d))) for d in every]

        self.core_t = table(lambda a, c, zh, zl: (a, 1 - c, zh, zl))
        self.near_t = table(lambda a, c, zh, zl: (a, c, zh, 1 - zl))
        self.far_t = table(lambda a, c, zh, zl: (a, c, 1 - zh, zl))
        self.swap_t = table(lambda a, c, zh, zl: (a, zh, c, zl))
        self.cross_t = table(lambda a, c, zh, zl: (a, zh, 1 - c, zl))
        self.cross_back_t = [(d, s) for s, d in self.cross_t]
        self.plane_t = [
            table(lambda a, c, zh, zl, b=b: (a ^ (1 << b), c, zh, zl)) for b in range(self.bits)
        ]
        self.paths = (list(range(self.bits)), list(range(self.bits))[::-1])
        self.slots = []
        for half, path in enumerate(self.paths):
            for p in range(dp // 2):
                offset = sum(1 << bit for j, bit in enumerate(path) if p >> j & 1)
                self.slots.append(2 * offset + half)

    def send(self, x, table):
        return lax.ppermute(x, AXES, table)

    def core(self, x):
        return self.send(x, self.core_t)

    def near(self, x):
        return self.send(x, self.near_t)

    def swap(self, x):
        return self.send(x, self.swap_t)

    def gather_blocks(self, shard):
        out = []
        for half, path in enumerate(self.paths):
            pieces = [self.send(shard, (self.swap_t, self.cross_t)[half])]
            for bit in path:
                whole = jnp.concatenate(pieces, 0) if len(pieces) > 1 else pieces[0]
                pieces.append(self.send(whole, self.plane_t[bit]))
            out += pieces
        return out

    def scatter_blocks(self, grad):
        half_rows = grad.shape[0] // 2
        last = []
        for half, path in enumerate(self.paths):
            held = grad[half * half_rows : (half + 1) * half_rows]
            for bit in path[::-1]:
                mid = held.shape[0] // 2
                got = self.send(held[mid:], self.plane_t[bit])
                held = (held[:mid].astype(f32) + got.astype(f32)).astype(bf16)
            last.append(self.send(held, (self.swap_t, self.cross_back_t)[half]))
        return last[0].astype(f32) + last[1].astype(f32)

    def gather_rows(self, own):
        beside = self.near(own)
        partner = self.core(own)
        return jnp.concatenate([own, beside, partner, self.core(beside)], axis=0)

    def scatter_rows(self, low, high):
        got = self.core(high)
        quarter = low.shape[0] // 2
        sent = (low[quarter:].astype(f32) + got[quarter:].astype(f32)).astype(bf16)
        kept = low[:quarter].astype(f32) + got[:quarter].astype(f32)
        return kept + self.near(sent).astype(f32)

    def sum_all(self, x):
        for table in [self.core_t, self.near_t] + self.plane_t + [self.far_t]:
            x = x + self.send(x, table)
        return x


def reorder_columns(x, index, slots):
    rows, width = x.shape[0], x.shape[1] // len(slots)
    return jnp.concatenate(
        [lax.dynamic_slice(x, (0, (index ^ r) * width), (rows, width)) for r in slots], axis=1
    )


def restore_columns(x, index, slots):
    rows, width = x.shape[0], x.shape[1] // len(slots)
    place = [0] * len(slots)
    for n, r in enumerate(slots):
        place[r] = n
    place = jnp.asarray(place, jnp.int32)
    return jnp.concatenate(
        [
            lax.dynamic_slice(x, (0, place[index ^ b] * width), (rows, width))
            for b in range(len(slots))
        ],
        axis=1,
    )


def rows_of(part, size):
    return pl.ds(pl.multiple_of(part * size, size), size)


def load_blocks(pieces, columns, dest, sem):
    copies, at = [], 0
    for n, piece in enumerate(pieces):
        size = piece.shape[0]
        copies.append(
            pltpu.make_async_copy(
                piece.at[:, pl.ds(*columns)], dest.at[pl.ds(at, size), :], sem.at[n]
            )
        )
        copies[-1].start()
        at += size
    return copies


def front_kernel(n_pieces, dims, *refs):
    pieces = refs[:n_pieces]
    (tau_ref, x, gain, cos, sin, q_gain, k_gain, normed, qkv, raw, weight, sem) = refs[n_pieces:]
    q_cols, kv_cols, width = dims
    copies = load_blocks(pieces, (0, q_cols + 2 * kv_cols), weight, sem)
    tau = tau_ref[0]
    size = x.shape[0] // 4
    for copy in copies:
        copy.wait()

    def part(k, carry):
        rows, place = rows_of(k, size), rows_of(tau ^ k, size)
        values = x[rows, :].astype(f32)
        low = (values * rms_rate(values) * gain[...]).astype(bf16)
        normed[rows, :] = low
        product = dot(low, weight[...])
        c, s = cos[place, :], sin[place, :]
        for at in range(0, q_cols + kv_cols, width):
            head = product[:, at : at + width]
            raw[rows, at : at + width] = head
            head = head * rms_rate(head) * (q_gain if at < q_cols else k_gain)[...]
            turned = head * c + pltpu.roll(head, width // 2, 1) * s
            qkv[rows, at : at + width] = turned.astype(bf16)
        qkv[rows, q_cols + kv_cols :] = product[:, q_cols + kv_cols :].astype(bf16)
        return carry

    lax.fori_loop(0, 4, part, 0)


def attend_kernel(n_pieces, dims, *refs):
    pieces = refs[:n_pieces]
    (tau_ref, qkv, block_row, block_rep, mixed, totals, low, high, weight, sem) = refs[n_pieces:]
    q_cols, kv_cols, width = dims
    copies = load_blocks(pieces, (0, q_cols), weight, sem)
    tau = tau_ref[0]
    size = qkv.shape[0] // 4
    factor = width ** (-0.5) * LOG2E
    ones = jnp.ones((4 * size, width), bf16)
    group = q_cols // kv_cols
    assert group == 2
    for quarter in range(4):
        rows, count = rows_of(tau ^ quarter, size), min(quarter + 2, 4)
        seen_by = block_rep[quarter * size : (quarter + 1) * size, :]
        seen_by = jnp.concatenate([seen_by] * (size // width), axis=1)
        for h in range(kv_cols // width):
            q_at, k_at = 2 * h * width, q_cols + h * width
            v_at = k_at + kv_cols
            query = jnp.concatenate(
                [qkv[rows, q_at : q_at + width], qkv[rows, q_at + width : q_at + 2 * width]], 0
            )
            probs, values = [], []
            for key_quarter in range(count):
                there = rows_of(tau ^ key_quarter, size)
                prob = jnp.exp2(dot_nt(query, qkv[there, k_at : k_at + width]) * factor)
                if key_quarter >= quarter:
                    seen = block_row[:, key_quarter * size : (key_quarter + 1) * size] <= seen_by
                    prob = jnp.where(jnp.concatenate([seen, seen], 0), prob, 0.0)
                probs.append(prob.astype(bf16))
                values.append(qkv[there, v_at : v_at + width])
            value = jnp.concatenate([jnp.concatenate(values, 0), ones[: count * size]], axis=1)
            out = dot(jnp.concatenate(probs, axis=1), value)
            total = out[:, width:]
            out = (out[:, :width] / total).astype(bf16)
            mixed[rows, q_at : q_at + width] = out[:size]
            mixed[rows, q_at + width : q_at + 2 * width] = out[size:]
            n = quarter * (kv_cols // width) + h
            totals[n : n + 1, :] = total.T[0:1]
    for copy in copies:
        copy.wait()
    for k in range(4):
        dest = low if k < 2 else high
        at = (k % 2) * size
        dest[at : at + size, :] = dot_nt(mixed[k * size : (k + 1) * size, :], weight[...]).astype(
            bf16
        )


def units_kernel(n_pieces, dims, *refs):
    pieces = refs[:n_pieces]
    (x, grad, inner, gate_grad, up_grad, low, high, weight, sem) = refs[n_pieces:]
    start, units = dims
    copies = load_blocks(pieces, (start, 3 * units), weight, sem)
    size = x.shape[0] // 4
    for copy in copies:
        copy.wait()

    def part(k, dest, at):
        rows = rows_of(k, size)
        there = rows_of(at, size)
        values, back = x[rows, :], grad[rows, :]
        gate = dot(values, weight[:, :units])
        up = dot(values, weight[:, units : 2 * units])
        inward = dot(back, weight[:, 2 * units :])
        sg = jax.nn.sigmoid(gate)
        silu = gate * sg
        inner[rows, :] = (silu * up).astype(bf16)
        d_gate = (inward * up * sg * (1.0 + gate * (1.0 - sg))).astype(bf16)
        d_up = (inward * silu).astype(bf16)
        gate_grad[rows, :] = d_gate
        up_grad[rows, :] = d_up
        dest[there, :] = (
            dot_nt(d_gate, weight[:, :units]) + dot_nt(d_up, weight[:, units : 2 * units])
        ).astype(bf16)

    def pair(k, carry):
        part(k, low, k)
        part(k + 2, high, k)
        return carry

    lax.fori_loop(0, 2, pair, 0)


def unit_grads_kernel(n_pieces, dims, *refs):
    pieces = refs[:n_pieces]
    (x, grad, inner, gate_grad, up_grad, total, low, high, weight, sem) = refs[n_pieces:]
    start, units = dims
    copies = load_blocks(pieces, (start + 2 * units, units), weight, sem)
    size = x.shape[0] // 4

    def block(n, carry):
        columns = rows_of(n, 256)
        into = x[:, columns]
        total[columns, :units] = dot_tn(into, gate_grad[...]).astype(bf16)
        total[columns, units : 2 * units] = dot_tn(into, up_grad[...]).astype(bf16)
        total[columns, 2 * units :] = dot_tn(grad[:, columns], inner[...]).astype(bf16)
        return carry

    lax.fori_loop(0, x.shape[1] // 256, block, 0)
    for copy in copies:
        copy.wait()
    for k in range(4):
        dest = low if k < 2 else high
        at = (k % 2) * size
        dest[at : at + size, :] = dot_nt(inner[k * size : (k + 1) * size, :], weight[...]).astype(
            bf16
        )


def attend_back_kernel(n_in, n_out, dims, *refs):
    in_pieces, out_pieces = refs[:n_in], refs[n_in : n_in + n_out]
    (
        tau_ref,
        state_grad,
        qkv,
        raw,
        mixed,
        totals,
        block_row,
        block_rep,
        cos,
        sin,
        q_gain,
        k_gain,
        qkv_grad,
        gain_grads,
        low,
        high,
        in_weight,
        out_weight,
        mixed_grad,
        q_grad,
        k_acc,
        v_acc,
        in_sem,
        out_sem,
    ) = refs[n_in + n_out :]
    q_cols, kv_cols, width = dims
    out_copies = load_blocks(out_pieces, (0, q_cols), out_weight, out_sem)
    in_copies = load_blocks(in_pieces, (0, q_cols + 2 * kv_cols), in_weight, in_sem)
    tau = tau_ref[0]
    size = qkv.shape[0] // 4
    scale = width ** (-0.5)
    factor = scale * LOG2E
    for copy in out_copies:
        copy.wait()

    def project(k, carry):
        rows = rows_of(k, size)
        mixed_grad[rows, :] = dot(state_grad[rows, :], out_weight[...]).astype(bf16)
        return carry

    lax.fori_loop(0, 4, project, 0)
    k_acc[...] = jnp.zeros_like(k_acc)
    v_acc[...] = jnp.zeros_like(v_acc)
    ones = jnp.ones((8, width), bf16)
    for quarter in (3, 2, 1, 0):
        rows, count = rows_of(tau ^ quarter, size), min(quarter + 2, 4)
        row_ids = block_row[:, quarter * size : (quarter + 1) * size]
        row_ids = jnp.concatenate([row_ids, row_ids], axis=1)
        for h in range(kv_cols // width):
            q_at, k_at = 2 * h * width, q_cols + h * width
            v_at = k_at + kv_cols

            def both(ref):
                return jnp.concatenate(
                    [ref[rows, q_at : q_at + width], ref[rows, q_at + width : q_at + 2 * width]], 0
                )

            query, out_grad = both(qkv), both(mixed_grad)
            product = out_grad.astype(f32) * both(mixed).astype(f32)
            product_high = product.astype(bf16)
            product_low = (product - product_high.astype(f32)).astype(bf16)
            centre = (dot_nt(ones, product_high) + dot_nt(ones, product_low))[0:1]
            n = quarter * (kv_cols // width) + h
            level = -jnp.log2(totals[n : n + 1, :])
            columns = slice(h * width, (h + 1) * width)
            score_grads, keys = [], []
            for key_quarter in range(count):
                there = rows_of(tau ^ key_quarter, size)
                key, value = qkv[there, k_at : k_at + width], qkv[there, v_at : v_at + width]
                prob = jnp.exp2(dot_nt(key, query) * factor + level)
                if key_quarter >= quarter:
                    ids = block_rep[key_quarter * size : (key_quarter + 1) * size, :]
                    seen = jnp.concatenate([ids] * (2 * size // width), axis=1) <= row_ids
                    prob = jnp.where(seen, prob, 0.0)
                score_grad = (prob * (dot_nt(value, out_grad) - centre)).astype(bf16)
                v_acc[there, columns] += dot(prob.astype(bf16), out_grad)
                k_acc[there, columns] += dot(score_grad, query)
                score_grads.append(score_grad)
                keys.append(key)
            back = dot_tn(jnp.concatenate(score_grads, 0), jnp.concatenate(keys, 0))
            q_grad[rows, q_at : q_at + width] = back[:size]
            q_grad[rows, q_at + width : q_at + 2 * width] = back[size:]
    for copy in in_copies:
        copy.wait()
    gain_grads[...] = jnp.zeros_like(gain_grads)

    def part(k, dest, at):
        rows, place, there = rows_of(k, size), rows_of(tau ^ k, size), rows_of(at, size)
        c, s = cos[place, :], sin[place, :]
        for at in range(0, q_cols + kv_cols, width):
            is_q = at < q_cols
            turned = (q_grad[rows, at : at + width] if is_q else k_acc[rows, at - q_cols : at - q_cols + width]) * scale
            grad = turned * c - pltpu.roll(turned, width // 2, 1) * s
            back, gain_part = rms_back(
                raw[rows, at : at + width], (q_gain if is_q else k_gain)[...], grad
            )
            qkv_grad[rows, at : at + width] = back.astype(bf16)
            n = 0 if is_q else 8
            gain_grads[n : n + 8, :] += jnp.sum(gain_part.reshape(size // 8, 8, width), axis=0)
        qkv_grad[rows, q_cols + kv_cols :] = v_acc[rows, :].astype(bf16)
        dest[there, :] = dot_nt(qkv_grad[rows, :], in_weight[...]).astype(bf16)

    def pair(k, carry):
        part(k, low, k)
        part(k + 2, high, k)
        return carry

    lax.fori_loop(0, 2, pair, 0)


VMEM_SPEC = pl.BlockSpec(memory_space=pltpu.VMEM)
SMEM_SPEC = pl.BlockSpec(memory_space=pltpu.SMEM)
ANY_SPEC = pl.BlockSpec(memory_space=pl.ANY)


def run(kernel, name, pieces, scalars, args, outs, scratch, flops):
    moved = sum(a.size * a.dtype.itemsize for a in list(pieces) + list(args))
    moved += sum(o.size * o.dtype.itemsize for o in outs)
    return pl.pallas_call(
        kernel,
        name=name,
        out_shape=outs,
        in_specs=[ANY_SPEC] * len(pieces) + [SMEM_SPEC] * len(scalars) + [VMEM_SPEC] * len(args),
        out_specs=[VMEM_SPEC] * len(outs),
        scratch_shapes=scratch,
        compiler_params=pltpu.CompilerParams(vmem_limit_bytes=56 * 2**20),
        cost_estimate=pl.CostEstimate(flops=flops, bytes_accessed=moved, transcendentals=0),
    )(*pieces, *scalars, *args)


def body(
    links,
    tokens,
    block_ids,
    norm1_gain,
    q_weight,
    key_projection,
    value_projection,
    q_gain,
    k_gain,
    o_weight,
    norm2_gain,
    gate_weight,
    up_weight,
    down_weight,
    out_grad,
):
    dp, slots = links.dp, links.slots
    dp_index = lax.axis_index("dp")
    t_index = lax.axis_index("tensor")
    own_seq = (dp_index // 2) * 2 + t_index // 2
    own_part = (dp_index % 2) * 2 + t_index % 2
    tau = own_part[None].astype(jnp.int32)

    in_shard = jnp.concatenate([q_weight, key_projection, value_projection], axis=1)
    tokens_own = links.swap(reorder_columns(tokens, dp_index, slots))
    in_pieces = links.gather_blocks(in_shard)
    acts_all = links.gather_rows(tokens_own)
    block_of = links.swap(block_ids)

    gain_width, head_part = norm1_gain.shape[0], q_gain.shape[0]
    gains = jnp.concatenate([norm1_gain, norm2_gain, q_gain, k_gain])[None, :]
    gains_all = jnp.concatenate(links.gather_blocks(gains), 0).astype(f32)
    first_gain = gains_all[:, :gain_width].reshape(1, -1)
    second_gain = gains_all[:, gain_width : 2 * gain_width].reshape(1, -1)
    place = [0] * dp
    for n, r in enumerate(slots):
        place[r] = n
    place = jnp.asarray(place, jnp.int32)[own_seq ^ jnp.arange(dp)]
    head_gains = gains_all[place, 2 * gain_width :]
    q_scale = head_gains[:, :head_part].reshape(1, -1)
    k_scale = head_gains[:, head_part:].reshape(1, -1)

    out_shard = jnp.concatenate([o_weight.T, gate_weight, up_weight, down_weight.T], axis=1)
    out_pieces = links.gather_blocks(out_shard)
    grad_all = links.gather_rows(links.swap(reorder_columns(out_grad, dp_index, slots)))

    length = block_of.shape[1]
    model = tokens.shape[1]
    width = q_scale.shape[1]
    q_cols = q_weight.shape[1]
    kv_cols = key_projection.shape[1]
    units = gate_weight.shape[1]
    quarter = length // 4
    dims = (q_cols, kv_cols, width)
    shape = jax.ShapeDtypeStruct
    n_sem = pltpu.SemaphoreType.DMA((len(in_pieces),))

    half_dim = width // 2
    inverse = BASE_FREQ ** (-2.0 * jnp.arange(half_dim, dtype=f32) / width)
    turns = jnp.arange(length, dtype=f32)[:, None] * inverse[None, :]
    cosine, sine = jnp.cos(turns), jnp.sin(turns)
    cosine = jnp.concatenate([cosine, cosine], axis=1)
    sine = jnp.concatenate([-sine, sine], axis=1)
    block_rep = jnp.broadcast_to(block_of.reshape(length, 1), (length, 128))

    n_qkv = q_cols + 2 * kv_cols
    halves = [shape((length // 2, model), bf16)] * 2
    normed, qkv, raw = run(
        partial(front_kernel, len(in_pieces), dims),
        "front",
        in_pieces,
        [tau],
        [acts_all, first_gain, cosine, sine, q_scale, k_scale],
        [
            shape((length, model), bf16),
            shape((length, n_qkv), bf16),
            shape((length, q_cols + kv_cols), f32),
        ],
        [pltpu.VMEM((model, n_qkv), bf16), n_sem],
        2 * length * model * n_qkv,
    )
    mixed, totals, low, high = run(
        partial(attend_kernel, len(out_pieces), dims),
        "attend",
        out_pieces,
        [tau],
        [qkv, block_of, block_rep],
        [shape((length, q_cols), bf16), shape((4 * kv_cols // width, 2 * quarter), f32)] + halves,
        [pltpu.VMEM((model, q_cols), bf16), n_sem],
        6 * length * length * q_cols,
    )
    state = acts_all[:quarter].astype(f32) + links.scatter_rows(low, high)
    normed_two = links.gather_rows((state * rms_rate(state) * second_gain).astype(bf16))
    inner, gate_grad, up_grad, low, high = run(
        partial(units_kernel, len(out_pieces), (q_cols, units)),
        "units",
        out_pieces,
        [],
        [normed_two, grad_all],
        [shape((length, units), bf16)] * 3 + halves,
        [pltpu.VMEM((model, 3 * units), bf16), n_sem],
        10 * length * model * units,
    )
    normed_two_grad = links.scatter_rows(low, high)
    unit_total, low, high = run(
        partial(unit_grads_kernel, len(out_pieces), (q_cols, units)),
        "unit_grads",
        out_pieces,
        [],
        [normed_two, grad_all, inner, gate_grad, up_grad],
        [shape((model, 3 * units), bf16)] + halves,
        [pltpu.VMEM((model, units), bf16), n_sem],
        8 * length * model * units,
    )
    layer_sum = state + links.scatter_rows(low, high)
    layer_out = links.swap(restore_columns(layer_sum.astype(bf16), own_seq, slots))
    unit_sum = links.scatter_blocks(unit_total)

    state_back, second_part = rms_back(state, second_gain, normed_two_grad)
    second_part = jnp.sum(second_part, axis=0)
    state_grad = grad_all[:quarter].astype(f32) + state_back
    state_low = links.gather_rows(state_grad.astype(bf16))
    qkv_grad, gain_grads, low, high = run(
        partial(attend_back_kernel, len(in_pieces), len(out_pieces), dims),
        "attend_back",
        in_pieces + out_pieces,
        [tau],
        [state_low, qkv, raw, mixed, totals, block_of, block_rep, cosine, sine, q_scale, k_scale],
        [shape((length, n_qkv), bf16), shape((16, width), f32)] + halves,
        [
            pltpu.VMEM((model, n_qkv), bf16),
            pltpu.VMEM((model, q_cols), bf16),
            pltpu.VMEM((length, q_cols), bf16),
            pltpu.VMEM((length, q_cols), f32),
            pltpu.VMEM((length, kv_cols), f32),
            pltpu.VMEM((length, kv_cols), f32),
            n_sem,
            n_sem,
        ],
        14 * length * length * q_cols,
    )
    normed_grad = links.scatter_rows(low, high)
    in_total = dot_tn(normed, qkv_grad).astype(bf16)
    in_sum = links.scatter_blocks(in_total)
    o_total = dot_tn(state_low, mixed).astype(bf16)
    o_sum = links.scatter_blocks(o_total).T
    acts_back, first_part = rms_back(acts_all[:quarter].astype(f32), first_gain, normed_grad)
    first_part = jnp.sum(first_part, axis=0)
    tokens_grad = links.swap(
        restore_columns((state_grad + acts_back).astype(bf16), own_seq, slots)
    ).astype(f32)

    shared = jnp.concatenate(
        [
            first_part.reshape(dp, gain_width)[place].reshape(-1),
            second_part.reshape(dp, gain_width)[place].reshape(-1),
            jnp.sum(gain_grads[:8], axis=0),
            jnp.sum(gain_grads[8:], axis=0),
        ]
    )
    shared = links.sum_all(shared)
    first_total = lax.dynamic_slice(shared, (dp_index * gain_width,), (gain_width,))
    second_total = lax.dynamic_slice(shared, (model + dp_index * gain_width,), (gain_width,))
    qs_total = lax.dynamic_slice(shared, (2 * model + dp_index * head_part,), (head_part,))
    ks_total = lax.dynamic_slice(shared, (2 * model + width + dp_index * head_part,), (head_part,))
    return (
        layer_out,
        tokens_grad,
        first_total,
        in_sum[:, :q_cols],
        in_sum[:, q_cols : q_cols + kv_cols],
        in_sum[:, q_cols + kv_cols :],
        qs_total,
        ks_total,
        o_sum,
        second_total,
        unit_sum[:, :units],
        unit_sum[:, units : 2 * units],
        unit_sum[:, 2 * units :].T,
    )


def solution(mesh):
    links = Links(mesh.shape["dp"], mesh.shape["tensor"])
    return jax.shard_map(
        partial(body, links),
        mesh=mesh,
        in_specs=(
            P(("dp", "tensor"), None),
            P("dp", None),
            P("dp"),
            P("dp", "tensor"),
            P("dp", "tensor"),
            P("dp", "tensor"),
            P("dp"),
            P("dp"),
            P("tensor", "dp"),
            P("dp"),
            P("dp", "tensor"),
            P("dp", "tensor"),
            P("tensor", "dp"),
            P(("dp", "tensor"), None),
        ),
        out_specs=(
            P(("dp", "tensor"), None),
            P(("dp", "tensor"), None),
            P("dp"),
            P("dp", "tensor"),
            P("dp", "tensor"),
            P("dp", "tensor"),
            P("dp"),
            P("dp"),
            P("tensor", "dp"),
            P("dp"),
            P("dp", "tensor"),
            P("dp", "tensor"),
            P("tensor", "dp"),
        ),
        check_vma=False,
    )
```

```python
from functools import partial

import jax
import jax.numpy as jnp
import numpy as np
from jax import lax
from jax.experimental import pallas as pl
from jax.experimental.pallas import tpu as pltpu
from jax.sharding import PartitionSpec as P

EPSILON = 1e-06
BASE_FREQ = 1000000.0
AXES = ("dp", "tensor")
LOG2E = 1.4426950408889634


bf16, f32 = jnp.bfloat16, jnp.float32
NT = (((1,), (1,)), ((), ()))
TN = (((0,), (0,)), ((), ()))


def dot(left, right):
    return jnp.dot(left, right, preferred_element_type=f32)


def dot_nt(left, right):
    return lax.dot_general(left, right, NT, preferred_element_type=f32)


def dot_tn(left, right):
    return lax.dot_general(left, right, TN, preferred_element_type=f32)


def rms_rate(values):
    return lax.rsqrt(jnp.mean(values * values, axis=-1, keepdims=True) + EPSILON)


def rms_back(values, gain, grad):
    rate = rms_rate(values)
    shape = values * rate
    inward = grad * gain
    back = rate * (inward - shape * jnp.mean(inward * shape, axis=-1, keepdims=True))
    return back, grad * shape


class Links:
    def __init__(self, dp, tensor):
        assert tensor == 4 and dp % 2 == 0 and dp & (dp - 1) == 0
        self.dp = dp
        self.bits = (dp // 2).bit_length() - 1
        every = [
            (a, c, zh, zl)
            for a in range(dp // 2)
            for c in range(2)
            for zh in range(2)
            for zl in range(2)
        ]

        def flat(a, c, zh, zl):
            return (2 * a + c) * 4 + 2 * zh + zl

        def table(fn):
            return [(flat(*d), flat(*fn(*d))) for d in every]

        self.core_t = table(lambda a, c, zh, zl: (a, 1 - c, zh, zl))
        self.near_t = table(lambda a, c, zh, zl: (a, c, zh, 1 - zl))
        self.far_t = table(lambda a, c, zh, zl: (a, c, 1 - zh, zl))
        self.swap_t = table(lambda a, c, zh, zl: (a, zh, c, zl))
        self.cross_t = table(lambda a, c, zh, zl: (a, zh, 1 - c, zl))
        self.cross_back_t = [(d, s) for s, d in self.cross_t]
        self.plane_t = [
            table(lambda a, c, zh, zl, b=b: (a ^ (1 << b), c, zh, zl)) for b in range(self.bits)
        ]
        self.paths = (list(range(self.bits)), list(range(self.bits))[::-1])
        self.slots = []
        for half, path in enumerate(self.paths):
            for p in range(dp // 2):
                offset = sum(1 << bit for j, bit in enumerate(path) if p >> j & 1)
                self.slots.append(2 * offset + half)

    def send(self, x, table):
        return lax.ppermute(x, AXES, table)

    def core(self, x):
        return self.send(x, self.core_t)

    def near(self, x):
        return self.send(x, self.near_t)

    def swap(self, x):
        return self.send(x, self.swap_t)

    def gather_blocks(self, shard):
        out = []
        for half, path in enumerate(self.paths):
            pieces = [self.send(shard, (self.swap_t, self.cross_t)[half])]
            for bit in path:
                whole = jnp.concatenate(pieces, 0) if len(pieces) > 1 else pieces[0]
                pieces.append(self.send(whole, self.plane_t[bit]))
            out += pieces
        return out

    def scatter_blocks(self, grad):
        half_rows = grad.shape[0] // 2
        last = []
        for half, path in enumerate(self.paths):
            held = grad[half * half_rows : (half + 1) * half_rows]
            for bit in path[::-1]:
                mid = held.shape[0] // 2
                got = self.send(held[mid:], self.plane_t[bit])
                held = (held[:mid].astype(f32) + got.astype(f32)).astype(bf16)
            last.append(self.send(held, (self.swap_t, self.cross_back_t)[half]))
        return last[0].astype(f32) + last[1].astype(f32)

    def gather_rows(self, own):
        beside = self.near(own)
        partner = self.core(own)
        return jnp.concatenate([own, beside, partner, self.core(beside)], axis=0)

    def scatter_rows(self, low, high):
        got = self.core(high)
        quarter = low.shape[0] // 2
        sent = (low[quarter:].astype(f32) + got[quarter:].astype(f32)).astype(bf16)
        kept = low[:quarter].astype(f32) + got[:quarter].astype(f32)
        return kept + self.near(sent).astype(f32)

    def sum_all(self, x):
        for table in [self.core_t, self.near_t] + self.plane_t + [self.far_t]:
            x = x + self.send(x, table)
        return x


def reorder_columns(x, index, slots):
    rows, width = x.shape[0], x.shape[1] // len(slots)
    return jnp.concatenate(
        [lax.dynamic_slice(x, (0, (index ^ r) * width), (rows, width)) for r in slots], axis=1
    )


def restore_columns(x, index, slots):
    rows, width = x.shape[0], x.shape[1] // len(slots)
    place = [0] * len(slots)
    for n, r in enumerate(slots):
        place[r] = n
    place = jnp.asarray(place, jnp.int32)
    return jnp.concatenate(
        [
            lax.dynamic_slice(x, (0, place[index ^ b] * width), (rows, width))
            for b in range(len(slots))
        ],
        axis=1,
    )


def rows_of(part, size):
    return pl.ds(pl.multiple_of(part * size, size), size)


def load_blocks(pieces, columns, dest, sem):
    copies, at = [], 0
    for n, piece in enumerate(pieces):
        size = piece.shape[0]
        copies.append(
            pltpu.make_async_copy(
                piece.at[:, pl.ds(*columns)], dest.at[pl.ds(at, size), :], sem.at[n]
            )
        )
        copies[-1].start()
        at += size
    return copies


def attend_back_kernel(n_in, n_out, dims, *refs):
    in_pieces, out_pieces = refs[:n_in], refs[n_in : n_in + n_out]
    (
        tau_ref,
        state_grad,
        qkv,
        raw,
        mixed,
        totals,
        block_row,
        block_rep,
        cos,
        sin,
        q_gain,
        k_gain,
        qkv_grad,
        gain_grads,
        low,
        high,
        in_weight,
        out_weight,
        mixed_grad,
        q_grad,
        k_acc,
        v_acc,
        in_sem,
        out_sem,
    ) = refs[n_in + n_out :]
    q_cols, kv_cols, width = dims
    out_copies = load_blocks(out_pieces, (0, q_cols), out_weight, out_sem)
    in_copies = load_blocks(in_pieces, (0, q_cols + 2 * kv_cols), in_weight, in_sem)
    tau = tau_ref[0]
    size = qkv.shape[0] // 4
    scale = width ** (-0.5)
    factor = scale * LOG2E
    for copy in out_copies:
        copy.wait()

    def project(k, carry):
        rows = rows_of(k, size)
        mixed_grad[rows, :] = dot(state_grad[rows, :], out_weight[...]).astype(bf16)
        return carry

    lax.fori_loop(0, 4, project, 0)
    k_acc[...] = jnp.zeros_like(k_acc)
    v_acc[...] = jnp.zeros_like(v_acc)
    ones = jnp.ones((8, width), bf16)
    for quarter in (3, 2, 1, 0):
        rows, count = rows_of(tau ^ quarter, size), min(quarter + 2, 4)
        row_ids = block_row[:, quarter * size : (quarter + 1) * size]
        row_ids = jnp.concatenate([row_ids, row_ids], axis=1)
        for h in range(kv_cols // width):
            q_at, k_at = 2 * h * width, q_cols + h * width
            v_at = k_at + kv_cols

            def both(ref):
                return jnp.concatenate(
                    [ref[rows, q_at : q_at + width], ref[rows, q_at + width : q_at + 2 * width]], 0
                )

            query, out_grad = both(qkv), both(mixed_grad)
            product = out_grad.astype(f32) * both(mixed).astype(f32)
            product_high = product.astype(bf16)
            product_low = (product - product_high.astype(f32)).astype(bf16)
            centre = (dot_nt(ones, product_high) + dot_nt(ones, product_low))[0:1]
            n = quarter * (kv_cols // width) + h
            level = -jnp.log2(totals[n : n + 1, :])
            columns = slice(h * width, (h + 1) * width)
            score_grads, keys = [], []
            for key_quarter in range(count):
                there = rows_of(tau ^ key_quarter, size)
                key, value = qkv[there, k_at : k_at + width], qkv[there, v_at : v_at + width]
                prob = jnp.exp2(dot_nt(key, query) * factor + level)
                if key_quarter >= quarter:
                    ids = block_rep[key_quarter * size : (key_quarter + 1) * size, :]
                    seen = jnp.concatenate([ids] * (2 * size // width), axis=1) <= row_ids
                    prob = jnp.where(seen, prob, 0.0)
                score_grad = (prob * (dot_nt(value, out_grad) - centre)).astype(bf16)
                v_acc[there, columns] += dot(prob.astype(bf16), out_grad)
                k_acc[there, columns] += dot(score_grad, query)
                score_grads.append(score_grad)
                keys.append(key)
            back = dot_tn(jnp.concatenate(score_grads, 0), jnp.concatenate(keys, 0))
            q_grad[rows, q_at : q_at + width] = back[:size]
            q_grad[rows, q_at + width : q_at + 2 * width] = back[size:]
    for copy in in_copies:
        copy.wait()
    gain_grads[...] = jnp.zeros_like(gain_grads)

    def part(k, dest, at):
        rows, there = rows_of(k, size), rows_of(at, size)
        c, s = cos[rows, :], sin[rows, :]
        for at in range(0, q_cols + kv_cols, width):
            is_q = at < q_cols
            turned = (q_grad[rows, at : at + width] if is_q else k_acc[rows, at - q_cols : at - q_cols + width]) * scale
            grad = turned * c - pltpu.roll(turned, width // 2, 1) * s
            back, gain_part = rms_back(
                raw[rows, at : at + width], (q_gain if is_q else k_gain)[...], grad
            )
            qkv_grad[rows, at : at + width] = back.astype(bf16)
            n = 0 if is_q else 8
            gain_grads[n : n + 8, :] += jnp.sum(gain_part.reshape(size // 8, 8, width), axis=0)
        qkv_grad[rows, q_cols + kv_cols :] = v_acc[rows, :].astype(bf16)
        dest[there, :] = dot_nt(qkv_grad[rows, :], in_weight[...]).astype(bf16)

    def pair(k, carry):
        part(k, low, k)
        part(k + 2, high, k)
        return carry

    lax.fori_loop(0, 2, pair, 0)


MESH = pl.DeviceIdType.MESH


def flip_bits(value, mask, bits):
    out = value
    for b in range(bits):
        if mask >> b & 1:
            out = out + (1 << b) * (1 - 2 * lax.rem(lax.div(value, 1 << b), 2))
    return out


class Wire:
    def __init__(self, bits, send_sem, recv_sem):
        dp, t = lax.axis_index("dp"), lax.axis_index("tensor")
        self.dp, self.bits = dp, bits
        self.c, self.a = lax.rem(dp, 2), lax.div(dp, 2)
        self.zh, self.zl = lax.div(t, 2), lax.rem(t, 2)
        self.send_sem, self.recv_sem = send_sem, recv_sem
        self.count, self.drains = 0, []
        c, a, zh, zl = self.c, self.a, self.zh, self.zl
        self.core = (2 * a + 1 - c, t)
        self.near = (dp, 2 * zh + 1 - zl)
        self.swapped = (2 * a + zh, 2 * c + zl)
        self.crossed = (2 * a + zh, 2 * (1 - c) + zl)
        self.far = [(2 * a + n, 2 * (1 - zh) + zl) for n in range(2)]
        self.plane = [(2 * flip_bits(a, 1 << b, bits) + c, t) for b in range(bits)]
        self.moves = c != zh

    def barrier(self):
        sem = pltpu.get_barrier_semaphore()
        peers = [self.core, self.near] + self.far + self.plane
        for peer in peers:
            pl.semaphore_signal(sem, inc=1, device_id=peer, device_id_type=MESH)
        pl.semaphore_wait(sem, len(peers))

    def part(self, k):
        c, zl = self.c, self.zl
        return 2 * (1 - c if k & 2 else c) + (1 - zl if k & 1 else zl)

    def slot(self, quarter):
        high, low = lax.div(quarter, 2), lax.rem(quarter, 2)
        return 2 * (high + self.c - 2 * high * self.c) + (low + self.zl - 2 * low * self.zl)

    def describe(self, src, dst, n, peer):
        return pltpu.make_async_remote_copy(
            src_ref=src,
            dst_ref=dst,
            send_sem=self.send_sem.at[n],
            recv_sem=self.recv_sem.at[n],
            device_id=peer,
            device_id_type=MESH,
        )

    def post(self, pairs, whole, peer):
        n = self.count
        self.count += 1
        for src, dst in pairs:
            self.describe(src, dst, n, peer).start()
        together = self.describe(whole, whole, n, peer)
        self.drains.append(together.wait_send)
        return together.wait_recv

    def post_one(self, src, dst, peer):
        return self.post([(src, dst)], dst, peer)

    def post_swap(self, pairs, whole):
        n = self.count
        self.count += 1
        together = self.describe(whole, whole, n, self.swapped)
        stays = pltpu.make_async_copy(whole, whole, self.recv_sem.at[n])

        @pl.when(self.moves)
        def _():
            for src, dst in pairs:
                self.describe(src, dst, n, self.swapped).start()

        @pl.when(jnp.logical_not(self.moves))
        def _():
            for src, dst in pairs:
                pltpu.make_async_copy(src, dst, self.recv_sem.at[n]).start()

        def arrive():
            pl.when(self.moves)(together.wait_recv)
            pl.when(jnp.logical_not(self.moves))(stays.wait)

        self.drains.append(lambda: pl.when(self.moves)(together.wait_send))
        return arrive

    def drain(self):
        for wait in self.drains:
            wait()
        self.drains = []


def spread_rows(wire, array):
    size = array.shape[0] // 4
    beside = wire.post_one(array.at[0:size, :], array.at[size : 2 * size, :], wire.near)
    partner = wire.post_one(array.at[0:size, :], array.at[2 * size : 3 * size, :], wire.core)

    def relay():
        beside()
        return wire.post_one(array.at[size : 2 * size, :], array.at[3 * size :, :], wire.core)

    return partner, relay


class Reduce:
    def __init__(self, wire, beside, own, landed, total):
        self.wire, self.beside, self.own = wire, beside, own
        self.landed, self.total = landed, total

    def send_beside(self):
        self.first = self.wire.post_one(self.beside.at[1], self.landed.at[0], self.wire.core)

    def forward(self):
        self.first()
        self.total[...] = (self.beside[0].astype(f32) + self.landed[0].astype(f32)).astype(bf16)
        self.third = self.wire.post_one(self.total, self.landed.at[2], self.wire.near)

    def send_own(self):
        self.second = self.wire.post_one(self.own.at[1], self.landed.at[1], self.wire.core)

    def result(self):
        self.second()
        self.third()
        return self.own[0].astype(f32) + self.landed[1].astype(f32) + self.landed[2].astype(f32)


class Columns:
    def __init__(self, q_cols, kv_cols, units):
        self.q_cols, self.kv_cols, self.units = q_cols, kv_cols, units
        self.n_in = q_cols + 2 * kv_cols
        self.gains = self.n_in
        self.o = self.gains + 128
        self.gate = self.o + q_cols
        self.up = self.gate + units
        self.down = self.up + units
        self.total = self.down + units
        self.back = self.gate


def forward_kernel(bits, slots, cols, width, head_part, reorder, *refs):
    (
        q_w, k_w, v_w, gains_w, o_w, gate_w, up_w, down_w, tokens, out_grad, ids_in, inverse,
        normed_o, qkv_o, raw_o, mixed_o, totals_o, low_o, grad_o, layer_o, unit_o, second_o,
        weight_o, gains_o, heads_o, cos_o, sin_o, ids_o, rep_o, acts_o,
        weight, acts, grad, normed_two, state_low, normed, qkv, raw, mixed, totals, cos, sin,
        gate, up, inner, gate_grad, up_grad, unit_stage, gains, heads, ids, rep, state, state_grad,
        layer, second, beside_a, own_a, landed_a, total_a, beside_b, own_b, landed_b, total_b,
        send_sem, recv_sem, out_sem,
    ) = refs
    wire = Wire(bits, send_sem, recv_sem)
    size, model = tokens.shape
    q_cols, kv_cols, units = cols.q_cols, cols.kv_cols, cols.units
    n_in = cols.n_in
    dp = len(slots)
    block = model // dp
    half_rows = model // 2
    outs = []

    def write(src, dst):
        outs.append(pltpu.make_async_copy(src, dst, out_sem.at[len(outs)]))
        outs[-1].start()

    def rows(k):
        return slice(k * size, (k + 1) * size)

    wire.barrier()

    groups = {
        "in": (0, cols.o, [q_w, k_w, v_w, gains_w]),
        "o": (cols.o, cols.gate, [o_w]),
        "gate": (cols.gate, cols.up, [gate_w]),
        "up": (cols.up, cols.down, [up_w]),
        "down": (cols.down, cols.total, [down_w]),
    }
    paths = (list(range(bits)), list(range(bits))[::-1])
    pending = {}

    def start_weights(name):
        low, high, shards = groups[name]
        for half in range(2):
            there = pl.ds(half * half_rows, block)
            pairs, at = [], low
            for shard in shards:
                pairs.append((shard, weight.at[there, at : at + shard.shape[1]]))
                at += shard.shape[1]
            whole = weight.at[there, low:high]
            if half == 0:
                pending[name, half, 0] = wire.post_swap(pairs, whole)
            else:
                pending[name, half, 0] = wire.post(pairs, whole, wire.crossed)

    def step_weights(name, step):
        low, high, _ = groups[name]
        for half in range(2):
            pending.pop((name, half, step))()
            if step < bits:
                have = block << step
                start = half * half_rows
                pending[name, half, step + 1] = wire.post_one(
                    weight.at[start : start + have, low:high],
                    weight.at[start + have : start + 2 * have, low:high],
                    wire.plane[paths[half][step]],
                )

    def swap_rows(source, dest):
        own = dest.at[0:size, :]
        if reorder:
            pairs = [
                (
                    source.at[
                        :,
                        pl.ds(
                            pl.multiple_of(flip_bits(wire.dp, r, bits + 1) * block, block), block
                        ),
                    ],
                    dest.at[0:size, n * block : (n + 1) * block],
                )
                for n, r in enumerate(slots)
            ]
        else:
            pairs = [(source, own)]
        return wire.post_swap(pairs, own)

    start_weights("in")
    acts_here = swap_rows(tokens, acts)
    ids_here = wire.post_swap([(ids_in, ids)], ids)
    start_weights("o")
    start_weights("gate")
    start_weights("up")
    grad_here = swap_rows(out_grad, grad)
    start_weights("down")

    base = lax.broadcasted_iota(jnp.int32, (size, width), 0).astype(f32) * inverse[0:1, :]
    base_cos, base_sin = jnp.cos(base), jnp.sin(base)
    sign = jnp.where(lax.broadcasted_iota(jnp.int32, (1, width), 1) < width // 2, -1.0, 1.0)
    for k in range(4):
        more = (wire.part(k) * size).astype(f32) * inverse[...]
        more_cos, more_sin = jnp.cos(more)[0:1], jnp.sin(more)[0:1]
        cos[rows(k), :] = base_cos * more_cos - base_sin * more_sin
        sin[rows(k), :] = (base_sin * more_cos + base_cos * more_sin) * sign
    write(cos, cos_o)
    write(sin, sin_o)

    step_weights("in", 0)
    acts_here()
    acts_partner, acts_relay = spread_rows(wire, acts)
    ids_here()
    rep[...] = jnp.broadcast_to(ids[0:1, :], (128, 4 * size)).T
    write(ids, ids_o)
    write(rep, rep_o)
    write(acts.at[0:size, :], acts_o)
    for step in range(1, bits):
        step_weights("in", step)
    step_weights("o", 0)
    step_weights("in", bits)

    turned = weight[:, cols.gains : cols.gains + 128].astype(f32).T
    gains[...] = turned[0:8, :]
    piece = min(block, width)
    for which in range(2):
        parts = []
        for j in range(width // piece):
            row = turned[2 + which * (width // piece) + j :][:1]
            part = row[:, 0:piece]
            for n in range(1, dp):
                part = part + row[:, n * block : n * block + piece]
            parts.append(part)
        heads[which * 8 : which * 8 + 8, :] = jnp.broadcast_to(
            jnp.concatenate(parts, axis=1), (8, width)
        )
    write(gains, gains_o)
    write(heads, heads_o)
    first_gain, second_gain = gains[0:1, :], gains[1:2, :]
    q_gain, k_gain = heads[0:1, :], heads[8:9, :]

    def front(k):
        here = rows(k)
        values = acts[here, :].astype(f32)
        low = (values * rms_rate(values) * first_gain).astype(bf16)
        normed[here, :] = low
        product = dot(low, weight[:, :n_in])
        c, s = cos[here, :], sin[here, :]
        for at in range(0, q_cols + kv_cols, width):
            head = product[:, at : at + width]
            raw[here, at : at + width] = head
            head = head * rms_rate(head) * (q_gain if at < q_cols else k_gain)
            turn = head * c + pltpu.roll(head, width // 2, 1) * s
            qkv[here, at : at + width] = turn.astype(bf16)
        qkv[here, q_cols + kv_cols :] = product[:, q_cols + kv_cols :].astype(bf16)

    front(0)
    acts_partner()
    acts_across = acts_relay()
    front(2)
    for step in range(1, bits):
        step_weights("o", step)
    front(1)
    acts_across()
    step_weights("gate", 0)
    front(3)
    write(normed, normed_o)
    write(qkv, qkv_o)
    write(raw, raw_o)

    factor = width ** (-0.5) * LOG2E
    ones = jnp.ones((4 * size, width), bf16)
    assert q_cols == 2 * kv_cols

    def attend(quarter, count, masked):
        place = pl.multiple_of(wire.slot(quarter) * size, size)
        here = pl.ds(place, size)
        seen_by = rep[pl.ds(pl.multiple_of(quarter * size, size), size), :]
        seen_by = jnp.concatenate([seen_by] * (size // 128), axis=1)
        for h in range(kv_cols // width):
            q_at, k_at = 2 * h * width, q_cols + h * width
            v_at = k_at + kv_cols
            query = jnp.concatenate(
                [qkv[here, q_at : q_at + width], qkv[here, q_at + width : q_at + 2 * width]], 0
            )
            probs, values = [], []
            for n in range(count):
                there = rows_of(wire.slot(jnp.int32(n)), size)
                prob = jnp.exp2(dot_nt(query, qkv[there, k_at : k_at + width]) * factor)
                if n in masked:
                    seen = ids[0:1, n * size : (n + 1) * size] <= seen_by
                    prob = jnp.where(jnp.concatenate([seen, seen], 0), prob, 0.0)
                probs.append(prob.astype(bf16))
                values.append(qkv[there, v_at : v_at + width])
            value = jnp.concatenate([jnp.concatenate(values, 0), ones[: count * size]], axis=1)
            out = dot(jnp.concatenate(probs, axis=1), value)
            total = out[:, width:]
            out = (out[:, :width] / total).astype(bf16)
            mixed[here, q_at : q_at + width] = out[:size]
            mixed[here, q_at + width : q_at + 2 * width] = out[size:]
            totals[pl.ds(quarter * (kv_cols // width) + h, 1), :] = total.T[0:1]
        return here

    def attend_pair(first, dest):
        here = attend(first, 3, (0, 1, 2))
        dest[wire.c] = dot_nt(mixed[here, :], weight[:, cols.o : cols.gate]).astype(bf16)
        here = attend(first + 2, 4, (2, 3))
        dest[1 - wire.c] = dot_nt(mixed[here, :], weight[:, cols.o : cols.gate]).astype(bf16)

    step_weights("o", bits)
    reduce_o = Reduce(wire, beside_a, own_a, landed_a, total_a)
    for step in range(1, bits):
        step_weights("gate", step)
    step_weights("up", 0)
    attend_pair(1 - wire.zl, beside_a)
    reduce_o.send_beside()
    grad_here()
    grad_partner, grad_relay = spread_rows(wire, grad)
    for step in range(1, bits):
        step_weights("up", step)
    reduce_o.forward()
    step_weights("down", 0)
    attend_pair(wire.zl, own_a)
    reduce_o.send_own()
    write(mixed, mixed_o)
    write(totals, totals_o)
    write(weight.at[:, : cols.back], weight_o)
    for step in range(1, bits):
        step_weights("down", step)
    state[...] = acts[0:size, :].astype(f32) + reduce_o.result()
    values = state[...]
    normed_two[0:size, :] = (values * rms_rate(values) * second_gain).astype(bf16)
    two_partner, two_relay = spread_rows(wire, normed_two)
    step_weights("gate", bits)
    step_weights("up", bits)

    def units_forward(k):
        values = normed_two[rows(k), :]
        gate[rows(k), :] = dot(values, weight[:, cols.gate : cols.up])
        up[rows(k), :] = dot(values, weight[:, cols.up : cols.down])

    def units_back(k, dest):
        here = rows(k)
        gate_here, up_here = gate[here, :], up[here, :]
        inward = dot(grad[here, :], weight[:, cols.down : cols.total])
        sg = jax.nn.sigmoid(gate_here)
        silu = gate_here * sg
        inner[here, :] = (silu * up_here).astype(bf16)
        d_gate = (inward * up_here * sg * (1.0 + gate_here * (1.0 - sg))).astype(bf16)
        d_up = (inward * silu).astype(bf16)
        gate_grad[here, :] = d_gate
        up_grad[here, :] = d_up
        dest[...] = (
            dot_nt(d_gate, weight[:, cols.gate : cols.up])
            + dot_nt(d_up, weight[:, cols.up : cols.down])
        ).astype(bf16)

    units_forward(0)
    two_partner()
    units_forward(2)
    grad_partner()
    grad_across = grad_relay()
    two_across = two_relay()
    units_forward(1)
    two_across()
    units_forward(3)
    grad_across()
    step_weights("down", bits)
    reduce_two = Reduce(wire, beside_b, own_b, landed_b, total_b)
    units_back(3, beside_b.at[1])
    reduce_two.send_beside()
    units_back(1, beside_b.at[0])
    reduce_two.forward()
    units_back(2, own_b.at[1])
    reduce_two.send_own()
    units_back(0, own_b.at[0])

    held = {}

    def unit_block(n):
        slot = n % 2
        if slot in held:
            held.pop(slot).wait()
        columns = slice(n * 256, (n + 1) * 256)
        into = normed_two[:, columns]
        dest = unit_stage.at[slot]
        dest[:, :units] = dot_tn(into, gate_grad[...]).astype(bf16)
        dest[:, units : 2 * units] = dot_tn(into, up_grad[...]).astype(bf16)
        dest[:, 2 * units :] = dot_tn(grad[:, columns], inner[...]).astype(bf16)
        held[slot] = pltpu.make_async_copy(dest, unit_o.at[columns, :], out_sem.at[24 + n])
        held[slot].start()

    for n in range(model // 256 - 1):
        unit_block(n)
    back, gain_part = rms_back(state[...], second_gain, reduce_two.result())
    second[...] = jnp.broadcast_to(jnp.sum(gain_part, axis=0, keepdims=True), second.shape)
    state_grad[...] = grad[0:size, :].astype(f32) + back
    state_low[0:size, :] = state_grad[...].astype(bf16)
    wire.drain()
    low_partner, low_relay = spread_rows(wire, state_low)
    write(second, second_o)
    write(state_grad, grad_o)
    unit_block(model // 256 - 1)


    def layer_part(k):
        return dot_nt(inner[rows(k), :], weight[:, cols.down : cols.total]).astype(bf16)

    reduce_out = Reduce(wire, beside_a, own_a, landed_a, total_a)
    beside_a[1] = layer_part(3)
    reduce_out.send_beside()
    beside_a[0] = layer_part(1)
    reduce_out.forward()
    own_a[1] = layer_part(2)
    reduce_out.send_own()
    own_a[0] = layer_part(0)
    low_partner()
    low_across = low_relay()
    low_across()
    write(state_low, low_o)
    layer[...] = (state[...] + reduce_out.result()).astype(bf16)
    write(layer, layer_o)
    for copy in list(held.values()) + outs:
        copy.wait()
    wire.drain()


VMEM_SPEC = pl.BlockSpec(memory_space=pltpu.VMEM)
SMEM_SPEC = pl.BlockSpec(memory_space=pltpu.SMEM)
ANY_SPEC = pl.BlockSpec(memory_space=pl.ANY)


def run(kernel, name, pieces, scalars, args, outs, scratch, flops):
    moved = sum(a.size * a.dtype.itemsize for a in list(pieces) + list(args))
    moved += sum(o.size * o.dtype.itemsize for o in outs)
    return pl.pallas_call(
        kernel,
        name=name,
        out_shape=outs,
        in_specs=[ANY_SPEC] * len(pieces) + [SMEM_SPEC] * len(scalars) + [VMEM_SPEC] * len(args),
        out_specs=[VMEM_SPEC] * len(outs),
        scratch_shapes=scratch,
        compiler_params=pltpu.CompilerParams(vmem_limit_bytes=56 * 2**20),
        cost_estimate=pl.CostEstimate(flops=flops, bytes_accessed=moved, transcendentals=0),
    )(*pieces, *scalars, *args)


def forward(links, shards, tokens, out_grad, ids, inverse, width, head_part, reorder, length):
    q_w, k_w, v_w, gains_w, o_w, gate_w, up_w, down_w = shards
    cols = Columns(q_w.shape[1], k_w.shape[1], gate_w.shape[1])
    model = tokens.shape[1]
    size = length // 4
    shape = jax.ShapeDtypeStruct
    n_qk, units = cols.q_cols + cols.kv_cols, cols.units
    n_totals = 4 * cols.kv_cols // width
    outs = [
        ((length, model), bf16),
        ((length, cols.n_in), bf16),
        ((length, n_qk), f32),
        ((length, cols.q_cols), bf16),
        ((n_totals, 2 * size), f32),
        ((length, model), bf16),
        ((size, model), f32),
        ((size, model), bf16),
        ((model, 3 * units), bf16),
        ((8, model), f32),
        ((model, cols.back), bf16),
        ((8, model), f32),
        ((16, width), f32),
        ((length, width), f32),
        ((length, width), f32),
        ((8, length), f32),
        ((length, 128), f32),
        ((size, model), bf16),
    ]
    reduce_set = [((2, size, model), bf16)] * 2 + [((3, size, model), bf16), ((size, model), bf16)]
    scratch = (
        [((model, cols.total), bf16)]
        + [((length, model), bf16)] * 5
        + [
            ((length, cols.n_in), bf16),
            ((length, n_qk), f32),
            ((length, cols.q_cols), bf16),
            ((n_totals, 2 * size), f32),
            ((length, width), f32),
            ((length, width), f32),
            ((length, units), f32),
            ((length, units), f32),
            ((length, units), bf16),
            ((length, units), bf16),
            ((length, units), bf16),
            ((2, 256, 3 * units), bf16),
            ((8, model), f32),
            ((16, width), f32),
            ((8, length), f32),
            ((length, 128), f32),
            ((size, model), f32),
            ((size, model), f32),
            ((size, model), bf16),
            ((8, model), f32),
        ]
        + reduce_set * 2
    )
    n_wire = 2 * 5 * (links.bits + 1) + 32
    args = list(shards) + [tokens, out_grad, ids]
    return pl.pallas_call(
        partial(forward_kernel, links.bits, links.slots, cols, width, head_part, reorder),
        name="forward",
        out_shape=[shape(*o) for o in outs],
        in_specs=[ANY_SPEC] * len(args) + [VMEM_SPEC],
        out_specs=[ANY_SPEC] * len(outs),
        scratch_shapes=[pltpu.VMEM(*s) for s in scratch]
        + [pltpu.SemaphoreType.DMA((n_wire,))] * 2
        + [pltpu.SemaphoreType.DMA((32,))],
        compiler_params=pltpu.CompilerParams(
            vmem_limit_bytes=66 * 10**6, collective_id=0, has_side_effects=True
        ),
    )(*args, inverse)


def body(
    links,
    tokens,
    block_ids,
    norm1_gain,
    q_weight,
    key_projection,
    value_projection,
    q_gain,
    k_gain,
    o_weight,
    norm2_gain,
    gate_weight,
    up_weight,
    down_weight,
    out_grad,
):
    dp, slots = links.dp, links.slots
    dp_index = lax.axis_index("dp")
    t_index = lax.axis_index("tensor")
    own_seq = (dp_index // 2) * 2 + t_index // 2
    own_part = (dp_index % 2) * 2 + t_index % 2
    tau = own_part[None].astype(jnp.int32)

    length, model = block_ids.shape[1], tokens.shape[1]
    gain_width, head_part = norm1_gain.shape[0], q_gain.shape[0]
    width = head_part * dp
    q_cols, kv_cols, units = q_weight.shape[1], key_projection.shape[1], gate_weight.shape[1]
    quarter = length // 4
    dims = (q_cols, kv_cols, width)
    shape = jax.ShapeDtypeStruct

    piece = min(gain_width, width)

    def as_columns(part):
        whole = lax.dynamic_update_slice(jnp.zeros((width,), bf16), part, (dp_index * head_part,))
        columns = whole.reshape(width // piece, piece).T
        return jnp.pad(columns, ((0, gain_width - piece), (0, 0)))

    gains_tile = jnp.concatenate(
        [norm1_gain[:, None], norm2_gain[:, None], as_columns(q_gain), as_columns(k_gain)], axis=1
    )
    gains_tile = jnp.pad(gains_tile, ((0, 0), (0, 128 - gains_tile.shape[1])))
    inverse = BASE_FREQ ** (-2.0 * (np.arange(width) % (width // 2)) / width)
    inverse = jnp.asarray(np.broadcast_to(inverse[None, :], (8, width)), f32)
    reorder = gain_width % 128 == 0
    if not reorder:
        tokens = reorder_columns(tokens, dp_index, slots)
        out_grad = reorder_columns(out_grad, dp_index, slots)
    shards = [
        q_weight,
        key_projection,
        value_projection,
        gains_tile,
        o_weight.T,
        gate_weight,
        up_weight,
        down_weight.T,
    ]
    (
        normed,
        qkv,
        raw,
        mixed,
        totals,
        state_low,
        state_grad,
        layer_sum,
        unit_total,
        second_part,
        weight,
        gains,
        heads,
        cosine,
        sine,
        block_of,
        block_rep,
        acts,
    ) = forward(
        links,
        shards,
        tokens,
        out_grad,
        jnp.broadcast_to(block_ids.astype(f32), (8, length)),
        inverse,
        width,
        head_part,
        reorder,
        length,
    )
    n_qkv = q_cols + 2 * kv_cols
    halves = [shape((length // 2, model), bf16)] * 2
    one_sem = pltpu.SemaphoreType.DMA((1,))
    layer_out = links.swap(restore_columns(layer_sum, own_seq, slots))
    unit_sum = links.scatter_blocks(unit_total)
    first_gain, second_part = gains[0:1], second_part[0]
    in_mat, o_mat = weight[:, :n_qkv], weight[:, n_qkv + 128 :]
    qkv_grad, gain_grads, low, high = run(
        partial(attend_back_kernel, 1, 1, dims),
        "attend_back",
        [in_mat, o_mat],
        [tau],
        [
            state_low,
            qkv,
            raw,
            mixed,
            totals,
            block_of[0:1],
            block_rep,
            cosine,
            sine,
            heads[0:1],
            heads[8:9],
        ],
        [shape((length, n_qkv), bf16), shape((16, width), f32)] + halves,
        [
            pltpu.VMEM((model, n_qkv), bf16),
            pltpu.VMEM((model, q_cols), bf16),
            pltpu.VMEM((length, q_cols), bf16),
            pltpu.VMEM((length, q_cols), f32),
            pltpu.VMEM((length, kv_cols), f32),
            pltpu.VMEM((length, kv_cols), f32),
            one_sem,
            one_sem,
        ],
        14 * length * length * q_cols,
    )
    normed_grad = links.scatter_rows(low, high)
    in_total = dot_tn(normed, qkv_grad).astype(bf16)
    in_sum = links.scatter_blocks(in_total)
    o_total = dot_tn(state_low, mixed).astype(bf16)
    o_sum = links.scatter_blocks(o_total).T
    acts_back, first_part = rms_back(acts.astype(f32), first_gain, normed_grad)
    first_part = jnp.sum(first_part, axis=0)
    tokens_grad = links.swap(
        restore_columns((state_grad + acts_back).astype(bf16), own_seq, slots)
    ).astype(f32)

    place = [0] * dp
    for n, r in enumerate(slots):
        place[r] = n
    place = jnp.asarray(place, jnp.int32)[own_seq ^ jnp.arange(dp)]
    shared = jnp.concatenate(
        [
            first_part.reshape(dp, gain_width)[place].reshape(-1),
            second_part.reshape(dp, gain_width)[place].reshape(-1),
            jnp.sum(gain_grads[:8], axis=0),
            jnp.sum(gain_grads[8:], axis=0),
        ]
    )
    shared = links.sum_all(shared)
    first_total = lax.dynamic_slice(shared, (dp_index * gain_width,), (gain_width,))
    second_total = lax.dynamic_slice(shared, (model + dp_index * gain_width,), (gain_width,))
    qs_total = lax.dynamic_slice(shared, (2 * model + dp_index * head_part,), (head_part,))
    ks_total = lax.dynamic_slice(shared, (2 * model + width + dp_index * head_part,), (head_part,))
    return (
        layer_out,
        tokens_grad,
        first_total,
        in_sum[:, :q_cols],
        in_sum[:, q_cols : q_cols + kv_cols],
        in_sum[:, q_cols + kv_cols :],
        qs_total,
        ks_total,
        o_sum,
        second_total,
        unit_sum[:, :units],
        unit_sum[:, units : 2 * units],
        unit_sum[:, 2 * units :].T,
    )


def solution(mesh):
    links = Links(mesh.shape["dp"], mesh.shape["tensor"])
    return jax.shard_map(
        partial(body, links),
        mesh=mesh,
        in_specs=(
            P(("dp", "tensor"), None),
            P("dp", None),
            P("dp"),
            P("dp", "tensor"),
            P("dp", "tensor"),
            P("dp", "tensor"),
            P("dp"),
            P("dp"),
            P("tensor", "dp"),
            P("dp"),
            P("dp", "tensor"),
            P("dp", "tensor"),
            P("tensor", "dp"),
            P(("dp", "tensor"), None),
        ),
        out_specs=(
            P(("dp", "tensor"), None),
            P(("dp", "tensor"), None),
            P("dp"),
            P("dp", "tensor"),
            P("dp", "tensor"),
            P("dp", "tensor"),
            P("dp"),
            P("dp"),
            P("tensor", "dp"),
            P("dp"),
            P("dp", "tensor"),
            P("dp", "tensor"),
            P("tensor", "dp"),
        ),
        check_vma=False,
    )
```

```python
from functools import partial

import jax
import jax.numpy as jnp
import numpy as np
from jax import lax
from jax.experimental import pallas as pl
from jax.experimental.pallas import tpu as pltpu
from jax.sharding import PartitionSpec as P

EPSILON = 1e-06
BASE_FREQ = 1000000.0
AXES = ("dp", "tensor")
LOG2E = 1.4426950408889634


bf16, f32 = jnp.bfloat16, jnp.float32
NT = (((1,), (1,)), ((), ()))
TN = (((0,), (0,)), ((), ()))


def dot(left, right):
    return jnp.dot(left, right, preferred_element_type=f32)


def dot_nt(left, right):
    return lax.dot_general(left, right, NT, preferred_element_type=f32)


def dot_tn(left, right):
    return lax.dot_general(left, right, TN, preferred_element_type=f32)


def rms_rate(values):
    return lax.rsqrt(jnp.mean(values * values, axis=-1, keepdims=True) + EPSILON)


def rms_back(values, gain, grad):
    rate = rms_rate(values)
    shape = values * rate
    inward = grad * gain
    back = rate * (inward - shape * jnp.mean(inward * shape, axis=-1, keepdims=True))
    return back, grad * shape


class Links:
    def __init__(self, dp, tensor):
        assert tensor == 4 and dp % 2 == 0 and dp & (dp - 1) == 0
        self.dp = dp
        self.bits = (dp // 2).bit_length() - 1
        self.paths = (list(range(self.bits)), list(range(self.bits))[::-1])
        self.slots = []
        for half, path in enumerate(self.paths):
            for p in range(dp // 2):
                offset = sum(1 << bit for j, bit in enumerate(path) if p >> j & 1)
                self.slots.append(2 * offset + half)


def reorder_columns(x, index, slots):
    rows, width = x.shape[0], x.shape[1] // len(slots)
    return jnp.concatenate(
        [lax.dynamic_slice(x, (0, (index ^ r) * width), (rows, width)) for r in slots], axis=1
    )


def restore_columns(x, index, slots):
    rows, width = x.shape[0], x.shape[1] // len(slots)
    place = [0] * len(slots)
    for n, r in enumerate(slots):
        place[r] = n
    place = jnp.asarray(place, jnp.int32)
    return jnp.concatenate(
        [
            lax.dynamic_slice(x, (0, place[index ^ b] * width), (rows, width))
            for b in range(len(slots))
        ],
        axis=1,
    )


def rows_of(part, size):
    return pl.ds(pl.multiple_of(part * size, size), size)


MESH = pl.DeviceIdType.MESH


def flip_bits(value, mask, bits):
    out = value
    for b in range(bits):
        if mask >> b & 1:
            out = out + (1 << b) * (1 - 2 * lax.rem(lax.div(value, 1 << b), 2))
    return out


class Wire:
    def __init__(self, bits, send_sem, recv_sem):
        dp, t = lax.axis_index("dp"), lax.axis_index("tensor")
        self.dp, self.bits = dp, bits
        self.c, self.a = lax.rem(dp, 2), lax.div(dp, 2)
        self.zh, self.zl = lax.div(t, 2), lax.rem(t, 2)
        self.send_sem, self.recv_sem = send_sem, recv_sem
        self.count, self.drains = 0, []
        c, a, zh, zl = self.c, self.a, self.zh, self.zl
        self.core = (2 * a + 1 - c, t)
        self.near = (dp, 2 * zh + 1 - zl)
        self.swapped = (2 * a + zh, 2 * c + zl)
        self.crossed = (2 * a + zh, 2 * (1 - c) + zl)
        self.crossed_back = (2 * a + 1 - zh, 2 * c + zl)
        self.far = [(2 * a + n, 2 * (1 - zh) + zl) for n in range(2)]
        self.plane = [(2 * flip_bits(a, 1 << b, bits) + c, t) for b in range(bits)]
        self.moves = c != zh

    def barrier(self):
        sem = pltpu.get_barrier_semaphore()
        peers = [self.core, self.near] + self.far + self.plane
        for peer in peers:
            pl.semaphore_signal(sem, inc=1, device_id=peer, device_id_type=MESH)
        pl.semaphore_wait(sem, len(peers))

    def part(self, k):
        c, zl = self.c, self.zl
        return 2 * (1 - c if k & 2 else c) + (1 - zl if k & 1 else zl)

    def slot(self, quarter):
        high, low = lax.div(quarter, 2), lax.rem(quarter, 2)
        return 2 * (high + self.c - 2 * high * self.c) + (low + self.zl - 2 * low * self.zl)

    def describe(self, src, dst, n, peer):
        return pltpu.make_async_remote_copy(
            src_ref=src,
            dst_ref=dst,
            send_sem=self.send_sem.at[n],
            recv_sem=self.recv_sem.at[n],
            device_id=peer,
            device_id_type=MESH,
        )

    def post(self, pairs, whole, peer):
        n = self.count
        self.count += 1
        for src, dst in pairs:
            self.describe(src, dst, n, peer).start()
        together = self.describe(whole, whole, n, peer)
        self.drains.append(together.wait_send)
        return together.wait_recv

    def post_one(self, src, dst, peer):
        return self.post([(src, dst)], dst, peer)

    def post_swap(self, pairs, whole):
        n = self.count
        self.count += 1
        together = self.describe(whole, whole, n, self.swapped)
        stays = pltpu.make_async_copy(whole, whole, self.recv_sem.at[n])

        @pl.when(self.moves)
        def _():
            for src, dst in pairs:
                self.describe(src, dst, n, self.swapped).start()

        @pl.when(jnp.logical_not(self.moves))
        def _():
            for src, dst in pairs:
                pltpu.make_async_copy(src, dst, self.recv_sem.at[n]).start()

        def arrive():
            pl.when(self.moves)(together.wait_recv)
            pl.when(jnp.logical_not(self.moves))(stays.wait)

        self.drains.append(lambda: pl.when(self.moves)(together.wait_send))
        return arrive

    def drain(self):
        for wait in self.drains:
            wait()
        self.drains = []


def spread_rows(wire, array):
    size = array.shape[0] // 4
    beside = wire.post_one(array.at[0:size, :], array.at[size : 2 * size, :], wire.near)
    partner = wire.post_one(array.at[0:size, :], array.at[2 * size : 3 * size, :], wire.core)

    def relay():
        beside()
        return wire.post_one(array.at[size : 2 * size, :], array.at[3 * size :, :], wire.core)

    return partner, relay


class Reduce:
    def __init__(self, wire, beside, own, landed, total):
        self.wire, self.beside, self.own = wire, beside, own
        self.landed, self.total = landed, total

    def drain(self):
        for n in self.sent:
            self.wire.drains[n]()
            self.wire.drains[n] = lambda: None

    def send_beside(self):
        self.sent = [len(self.wire.drains)]
        self.first = self.wire.post_one(self.beside.at[1], self.landed.at[0], self.wire.core)

    def forward(self):
        self.first()
        self.total[...] = (self.beside[0].astype(f32) + self.landed[0].astype(f32)).astype(bf16)
        self.sent.append(len(self.wire.drains))
        self.third = self.wire.post_one(self.total, self.landed.at[2], self.wire.near)

    def send_own(self):
        self.sent.append(len(self.wire.drains))
        self.second = self.wire.post_one(self.own.at[1], self.landed.at[1], self.wire.core)

    def result(self):
        self.second()
        self.third()
        return self.own[0].astype(f32) + self.landed[1].astype(f32) + self.landed[2].astype(f32)


class Columns:
    def __init__(self, q_cols, kv_cols, units):
        self.q_cols, self.kv_cols, self.units = q_cols, kv_cols, units
        self.n_in = q_cols + 2 * kv_cols
        self.gains = self.n_in
        self.o = self.gains + 128
        self.gate = self.o + q_cols
        self.up = self.gate + units
        self.down = self.up + units
        self.total = self.down + units
        self.back = self.gate


def forward_kernel(bits, slots, cols, width, head_part, reorder, *refs):
    (
        q_w, k_w, v_w, gains_w, o_w, gate_w, up_w, down_w, tokens, out_grad, ids_in, inverse,
        normed_o, qkv_o, raw_o, mixed_o, totals_o, low_o, grad_o, layer_o, unit_o, second_o,
        weight_o, gains_o, heads_o, cos_o, sin_o, ids_o, rep_o, acts_o,
        weight, acts, grad, normed_two, state_low, normed, qkv, raw, mixed, totals, cos, sin,
        gate, up, inner, gate_grad, up_grad, unit_total, unit_landed, gains, heads, ids, rep, state, state_grad,
        layer, second, beside_a, own_a, landed_a, total_a, beside_b, own_b, landed_b, total_b,
        send_sem, recv_sem, out_sem,
    ) = refs
    wire = Wire(bits, send_sem, recv_sem)
    size, model = tokens.shape
    q_cols, kv_cols, units = cols.q_cols, cols.kv_cols, cols.units
    n_in = cols.n_in
    dp = len(slots)
    block = model // dp
    half_rows = model // 2
    outs = []

    def write(src, dst):
        outs.append(pltpu.make_async_copy(src, dst, out_sem.at[len(outs)]))
        outs[-1].start()

    def rows(k):
        return slice(k * size, (k + 1) * size)

    wire.barrier()

    groups = {
        "in": (0, cols.o, [q_w, k_w, v_w, gains_w]),
        "o": (cols.o, cols.gate, [o_w]),
        "gate": (cols.gate, cols.up, [gate_w]),
        "up": (cols.up, cols.down, [up_w]),
        "down": (cols.down, cols.total, [down_w]),
    }
    paths = (list(range(bits)), list(range(bits))[::-1])
    pending = {}

    def start_weights(name):
        low, high, shards = groups[name]
        for half in range(2):
            there = pl.ds(half * half_rows, block)
            pairs, at = [], low
            for shard in shards:
                pairs.append((shard, weight.at[there, at : at + shard.shape[1]]))
                at += shard.shape[1]
            whole = weight.at[there, low:high]
            if half == 0:
                pending[name, half, 0] = wire.post_swap(pairs, whole)
            else:
                pending[name, half, 0] = wire.post(pairs, whole, wire.crossed)

    def step_weights(name, step):
        low, high, _ = groups[name]
        for half in range(2):
            pending.pop((name, half, step))()
            if step < bits:
                have = block << step
                start = half * half_rows
                pending[name, half, step + 1] = wire.post_one(
                    weight.at[start : start + have, low:high],
                    weight.at[start + have : start + 2 * have, low:high],
                    wire.plane[paths[half][step]],
                )

    def swap_rows(source, dest):
        own = dest.at[0:size, :]
        if reorder:
            pairs = [
                (
                    source.at[
                        :,
                        pl.ds(
                            pl.multiple_of(flip_bits(wire.dp, r, bits + 1) * block, block), block
                        ),
                    ],
                    dest.at[0:size, n * block : (n + 1) * block],
                )
                for n, r in enumerate(slots)
            ]
        else:
            pairs = [(source, own)]
        return wire.post_swap(pairs, own)

    start_weights("in")
    acts_here = swap_rows(tokens, acts)
    ids_here = wire.post_swap([(ids_in, ids)], ids)
    start_weights("o")
    start_weights("gate")
    start_weights("up")
    grad_here = swap_rows(out_grad, grad)
    start_weights("down")

    base = lax.broadcasted_iota(jnp.int32, (size, width), 0).astype(f32) * inverse[0:1, :]
    base_cos, base_sin = jnp.cos(base), jnp.sin(base)
    sign = jnp.where(lax.broadcasted_iota(jnp.int32, (1, width), 1) < width // 2, -1.0, 1.0)
    for k in range(4):
        more = (wire.part(k) * size).astype(f32) * inverse[...]
        more_cos, more_sin = jnp.cos(more)[0:1], jnp.sin(more)[0:1]
        cos[rows(k), :] = base_cos * more_cos - base_sin * more_sin
        sin[rows(k), :] = (base_sin * more_cos + base_cos * more_sin) * sign
    write(cos, cos_o)
    write(sin, sin_o)

    step_weights("in", 0)
    acts_here()
    acts_partner, acts_relay = spread_rows(wire, acts)
    ids_here()
    rep[...] = jnp.broadcast_to(ids[0:1, :], (128, 4 * size)).T
    write(ids, ids_o)
    write(rep, rep_o)
    write(acts.at[0:size, :], acts_o)
    for step in range(1, bits):
        step_weights("in", step)
    step_weights("o", 0)
    step_weights("in", bits)

    turned = weight[:, cols.gains : cols.gains + 128].astype(f32).T
    gains[...] = turned[0:8, :]
    piece = min(block, width)
    for which in range(2):
        parts = []
        for j in range(width // piece):
            row = turned[2 + which * (width // piece) + j :][:1]
            part = row[:, 0:piece]
            for n in range(1, dp):
                part = part + row[:, n * block : n * block + piece]
            parts.append(part)
        heads[which * 8 : which * 8 + 8, :] = jnp.broadcast_to(
            jnp.concatenate(parts, axis=1), (8, width)
        )
    write(gains, gains_o)
    write(heads, heads_o)
    first_gain, second_gain = gains[0:1, :], gains[1:2, :]
    q_gain, k_gain = heads[0:1, :], heads[8:9, :]

    def front(k):
        here = rows(k)
        values = acts[here, :].astype(f32)
        low = (values * rms_rate(values) * first_gain).astype(bf16)
        normed[here, :] = low
        product = dot(low, weight[:, :n_in])
        c, s = cos[here, :], sin[here, :]
        for at in range(0, q_cols + kv_cols, width):
            head = product[:, at : at + width]
            raw[here, at : at + width] = head
            head = head * rms_rate(head) * (q_gain if at < q_cols else k_gain)
            turn = head * c + pltpu.roll(head, width // 2, 1) * s
            qkv[here, at : at + width] = turn.astype(bf16)
        qkv[here, q_cols + kv_cols :] = product[:, q_cols + kv_cols :].astype(bf16)

    front(0)
    acts_partner()
    acts_across = acts_relay()
    front(2)
    for step in range(1, bits):
        step_weights("o", step)
    front(1)
    acts_across()
    step_weights("gate", 0)
    front(3)
    write(normed, normed_o)
    write(qkv, qkv_o)
    write(raw, raw_o)

    factor = width ** (-0.5) * LOG2E
    ones = jnp.ones((4 * size, width), bf16)
    assert q_cols == 2 * kv_cols

    def attend(quarter, count, masked):
        place = pl.multiple_of(wire.slot(quarter) * size, size)
        here = pl.ds(place, size)
        seen_by = rep[pl.ds(pl.multiple_of(quarter * size, size), size), :]
        seen_by = jnp.concatenate([seen_by] * (size // 128), axis=1)
        for h in range(kv_cols // width):
            q_at, k_at = 2 * h * width, q_cols + h * width
            v_at = k_at + kv_cols
            query = jnp.concatenate(
                [qkv[here, q_at : q_at + width], qkv[here, q_at + width : q_at + 2 * width]], 0
            )
            probs, values = [], []
            for n in range(count):
                there = rows_of(wire.slot(jnp.int32(n)), size)
                prob = jnp.exp2(dot_nt(query, qkv[there, k_at : k_at + width]) * factor)
                if n in masked:
                    seen = ids[0:1, n * size : (n + 1) * size] <= seen_by
                    prob = jnp.where(jnp.concatenate([seen, seen], 0), prob, 0.0)
                probs.append(prob.astype(bf16))
                values.append(qkv[there, v_at : v_at + width])
            value = jnp.concatenate([jnp.concatenate(values, 0), ones[: count * size]], axis=1)
            out = dot(jnp.concatenate(probs, axis=1), value)
            total = out[:, width:]
            out = (out[:, :width] / total).astype(bf16)
            mixed[here, q_at : q_at + width] = out[:size]
            mixed[here, q_at + width : q_at + 2 * width] = out[size:]
            totals[pl.ds(quarter * (kv_cols // width) + h, 1), :] = total.T[0:1]
        return here

    def attend_pair(first, dest):
        here = attend(first, 3, (0, 1, 2))
        dest[wire.c] = dot_nt(mixed[here, :], weight[:, cols.o : cols.gate]).astype(bf16)
        here = attend(first + 2, 4, (2, 3))
        dest[1 - wire.c] = dot_nt(mixed[here, :], weight[:, cols.o : cols.gate]).astype(bf16)

    step_weights("o", bits)
    reduce_o = Reduce(wire, beside_a, own_a, landed_a, total_a)
    for step in range(1, bits):
        step_weights("gate", step)
    step_weights("up", 0)
    attend_pair(1 - wire.zl, beside_a)
    reduce_o.send_beside()
    grad_here()
    grad_partner, grad_relay = spread_rows(wire, grad)
    for step in range(1, bits):
        step_weights("up", step)
    reduce_o.forward()
    step_weights("down", 0)
    attend_pair(wire.zl, own_a)
    reduce_o.send_own()
    write(mixed, mixed_o)
    write(totals, totals_o)
    write(weight.at[:, : cols.back], weight_o)
    for step in range(1, bits):
        step_weights("down", step)
    state[...] = acts[0:size, :].astype(f32) + reduce_o.result()
    values = state[...]
    normed_two[0:size, :] = (values * rms_rate(values) * second_gain).astype(bf16)
    two_partner, two_relay = spread_rows(wire, normed_two)
    step_weights("gate", bits)
    step_weights("up", bits)

    def units_forward(k):
        values = normed_two[rows(k), :]
        gate[rows(k), :] = dot(values, weight[:, cols.gate : cols.up])
        up[rows(k), :] = dot(values, weight[:, cols.up : cols.down])

    def units_back(k, dest):
        here = rows(k)
        gate_here, up_here = gate[here, :], up[here, :]
        inward = dot(grad[here, :], weight[:, cols.down : cols.total])
        sg = jax.nn.sigmoid(gate_here)
        silu = gate_here * sg
        inner[here, :] = (silu * up_here).astype(bf16)
        d_gate = (inward * up_here * sg * (1.0 + gate_here * (1.0 - sg))).astype(bf16)
        d_up = (inward * silu).astype(bf16)
        gate_grad[here, :] = d_gate
        up_grad[here, :] = d_up
        dest[...] = (
            dot_nt(d_gate, weight[:, cols.gate : cols.up])
            + dot_nt(d_up, weight[:, cols.up : cols.down])
        ).astype(bf16)

    units_forward(0)
    two_partner()
    units_forward(2)
    grad_partner()
    grad_across = grad_relay()
    two_across = two_relay()
    units_forward(1)
    two_across()
    units_forward(3)
    grad_across()
    step_weights("down", bits)
    reduce_two = Reduce(wire, beside_b, own_b, landed_b, total_b)
    units_back(3, beside_b.at[1])
    reduce_two.send_beside()
    units_back(1, beside_b.at[0])
    reduce_two.forward()
    units_back(2, own_b.at[1])
    reduce_two.send_own()
    units_back(0, own_b.at[0])

    quarter_rows = half_rows // 2

    def unit_block(n):
        columns = slice(n * quarter_rows, (n + 1) * quarter_rows)
        into = normed_two[:, columns]
        unit_total[columns, :units] = dot_tn(into, gate_grad[...]).astype(bf16)
        unit_total[columns, units : 2 * units] = dot_tn(into, up_grad[...]).astype(bf16)
        unit_total[columns, 2 * units :] = dot_tn(grad[:, columns], inner[...]).astype(bf16)

    for n in (1, 3):
        unit_block(n)
    unit_here = []
    for half in range(2):
        there = slice(half * half_rows + quarter_rows, (half + 1) * half_rows)
        unit_here.append(
            wire.post_one(
                unit_total.at[there, :], unit_landed.at[half], wire.plane[paths[half][bits - 1]]
            )
        )
    unit_block(0)
    back, gain_part = rms_back(state[...], second_gain, reduce_two.result())
    second[...] = jnp.broadcast_to(jnp.sum(gain_part, axis=0, keepdims=True), second.shape)
    state_grad[...] = grad[0:size, :].astype(f32) + back
    state_low[0:size, :] = state_grad[...].astype(bf16)
    reduce_o.drain()
    low_partner, low_relay = spread_rows(wire, state_low)
    write(second, second_o)
    write(state_grad, grad_o)
    unit_block(2)


    def layer_part(k):
        return dot_nt(inner[rows(k), :], weight[:, cols.down : cols.total]).astype(bf16)

    reduce_out = Reduce(wire, beside_a, own_a, landed_a, total_a)
    beside_a[1] = layer_part(3)
    reduce_out.send_beside()
    beside_a[0] = layer_part(1)
    reduce_out.forward()
    own_a[1] = layer_part(2)
    reduce_out.send_own()
    own_a[0] = layer_part(0)
    low_partner()
    low_across = low_relay()
    low_across()
    write(state_low, low_o)
    layer[...] = (state[...] + reduce_out.result()).astype(bf16)
    write(layer, layer_o)
    for half in range(2):
        unit_here[half]()

        def add(n, carry):
            at = pl.multiple_of(n * 64, 64)
            to = pl.ds(half * half_rows + at, 64)
            unit_total[to, :] = (
                unit_total[to, :].astype(f32) + unit_landed[half, pl.ds(at, 64), :].astype(f32)
            ).astype(bf16)
            return carry

        lax.fori_loop(0, quarter_rows // 64, add, 0)
        write(
            unit_total.at[half * half_rows : half * half_rows + quarter_rows, :],
            unit_o.at[half * quarter_rows : (half + 1) * quarter_rows, :],
        )
    for copy in outs:
        copy.wait()
    wire.drain()


def back_kernel(bits, slots, cols, width, restore, *refs):
    (
        weight_i, qkv_i, raw_i, mixed_i, totals_i, low_i, normed_i, cos_i, sin_i, ids_i, rep_i,
        gains_i, heads_i, grad_i, acts_i, second_i, layer_i, unit_i,
        layer_o, tokens_o, in_o, o_o, unit_o, gain_o,
        weight, qkv, raw, mixed, totals, state_low, normed, cos, sin, ids, rep, gains, heads,
        state_grad, acts, second, unit,
        mixed_grad, q_grad, k_acc, v_acc, qkv_grad, in_total, o_total, gain_total,
        in_landed, o_landed, unit_landed, gain_landed, layer_landed, tokens_own, tokens_landed,
        tokens_out, in_sum, o_sum, unit_sum, gain_sum, head_grads, shared, shared_landed, spread,
        beside, own, landed, total, send_sem, recv_sem, in_sem, out_sem,
    ) = refs
    wire = Wire(bits, send_sem, recv_sem)
    size, model = acts.shape
    q_cols, kv_cols, units, n_in = cols.q_cols, cols.kv_cols, cols.units, cols.n_in
    dp = len(slots)
    block, half_rows = model // dp, model // 2
    paths = (list(range(bits)), list(range(bits))[::-1])
    loads, outs = {}, []

    def load(name, src, dst):
        loads[name] = pltpu.make_async_copy(src, dst, in_sem.at[len(loads)])
        loads[name].start()

    taken = set()

    def need(*names):
        for name in names:
            if name not in taken:
                taken.add(name)
                loads[name].wait()

    def write(src, dst):
        outs.append(pltpu.make_async_copy(src, dst, out_sem.at[len(outs)]))
        outs[-1].start()

    def rows(k):
        return slice(k * size, (k + 1) * size)

    for name, src, dst in (
        ("low", low_i, state_low),
        ("weight", weight_i, weight),
        ("mixed", mixed_i, mixed),
        ("unit", unit_i, unit),
        ("qkv", qkv_i, qkv),
        ("totals", totals_i, totals),
        ("ids", ids_i, ids),
        ("rep", rep_i, rep),
        ("cos", cos_i, cos),
        ("sin", sin_i, sin),
        ("raw", raw_i, raw),
        ("heads", heads_i, heads),
        ("normed", normed_i, normed),
        ("gains", gains_i, gains),
        ("grad", grad_i, state_grad),
        ("acts", acts_i, acts),
        ("second", second_i, second),
    ):
        load(name, src, dst)
    wire.barrier()

    class Scatter:
        def __init__(self, total, landed, rows_of_half, result):
            self.total, self.landed, self.result = total, landed, result
            self.half_rows, self.waits = rows_of_half, {}

        def send(self, step):
            have = block << step
            for half in range(2):
                start = half * self.half_rows
                there = slice(start + have, start + 2 * have)
                self.waits[half, step] = wire.post_one(
                    self.total.at[there, :],
                    self.landed.at[there, :],
                    wire.plane[paths[half][step]],
                )

        def add(self, step):
            have = block << step
            chunk = min(have, 64)
            for half in range(2):
                start = half * self.half_rows
                self.waits.pop((half, step))()

                def body(n, carry):
                    at = pl.multiple_of(n * chunk, chunk)
                    to = pl.ds(start + at, chunk)
                    more = self.landed[pl.ds(start + have + at, chunk), :]
                    self.total[to, :] = (
                        self.total[to, :].astype(f32) + more.astype(f32)
                    ).astype(bf16)
                    return carry

                lax.fori_loop(0, have // chunk, body, 0)

        def finish(self):
            first = slice(0, block)
            other = slice(self.half_rows, self.half_rows + block)
            self.waits[0] = wire.post_swap(
                [(self.total.at[first, :], self.landed.at[first, :])], self.landed.at[first, :]
            )
            self.waits[1] = wire.post_one(
                self.total.at[other, :], self.landed.at[other, :], wire.crossed_back
            )

        def store(self, dest):
            self.waits.pop(0)()
            self.waits.pop(1)()
            other = slice(self.half_rows, self.half_rows + block)
            self.result[...] = self.landed[0:block, :].astype(f32) + self.landed[other, :].astype(
                f32
            )
            write(self.result, dest)

    def swap_out(source, dest):
        if restore:
            seq = 2 * wire.a + wire.zh
            pairs = [
                (
                    source.at[:, n * block : (n + 1) * block],
                    dest.at[
                        :,
                        pl.ds(
                            pl.multiple_of(flip_bits(seq, r, bits + 1) * block, block), block
                        ),
                    ],
                )
                for n, r in enumerate(slots)
            ]
        else:
            pairs = [(source, dest)]
        return wire.post_swap(pairs, dest)

    layer_here = swap_out(layer_i, layer_landed)
    scatter_unit = Scatter(unit, unit_landed, unit.shape[0] // 2, unit_sum)
    need("unit")
    if bits > 1:
        scatter_unit.send(bits - 2)
    scatter_in = Scatter(in_total, in_landed, half_rows, in_sum)
    scatter_o = Scatter(o_total, o_landed, half_rows, o_sum)
    scatter_gain = Scatter(gain_total, gain_landed, half_rows, gain_sum)

    need("low", "weight")
    for k in range(4):
        mixed_grad[rows(k), :] = dot(
            state_low[rows(k), :], weight[:, cols.o : cols.o + q_cols]
        ).astype(bf16)
    need("mixed")
    scale = width ** (-0.5)
    factor = scale * LOG2E
    k_acc[...] = jnp.zeros_like(k_acc)
    v_acc[...] = jnp.zeros_like(v_acc)
    ones = jnp.ones((8, width), bf16)
    need("qkv", "totals", "ids", "rep")

    def there_of(quarter):
        return rows_of(wire.slot(jnp.int32(quarter)), size)

    def attend_back(quarter):
        here, count = there_of(quarter), min(quarter + 2, 4)
        row_ids = ids[0:1, quarter * size : (quarter + 1) * size]
        row_ids = jnp.concatenate([row_ids, row_ids], axis=1)
        for h in range(kv_cols // width):
            q_at, k_at = 2 * h * width, q_cols + h * width
            v_at = k_at + kv_cols

            def both(ref):
                return jnp.concatenate(
                    [ref[here, q_at : q_at + width], ref[here, q_at + width : q_at + 2 * width]], 0
                )

            query, out_grad = both(qkv), both(mixed_grad)
            product = out_grad.astype(f32) * both(mixed).astype(f32)
            product_high = product.astype(bf16)
            product_low = (product - product_high.astype(f32)).astype(bf16)
            centre = (dot_nt(ones, product_high) + dot_nt(ones, product_low))[0:1]
            n = quarter * (kv_cols // width) + h
            level = -jnp.log2(totals[n : n + 1, :])
            columns = slice(h * width, (h + 1) * width)
            score_grads, keys = [], []
            for m in range(count):
                there = there_of(m)
                key, value = qkv[there, k_at : k_at + width], qkv[there, v_at : v_at + width]
                prob = jnp.exp2(dot_nt(key, query) * factor + level)
                if m >= quarter:
                    key_ids = rep[m * size : (m + 1) * size, :]
                    seen = jnp.concatenate([key_ids] * (2 * size // 128), axis=1) <= row_ids
                    prob = jnp.where(seen, prob, 0.0)
                score_grad = (prob * (dot_nt(value, out_grad) - centre)).astype(bf16)
                v_acc[there, columns] += dot(prob.astype(bf16), out_grad)
                k_acc[there, columns] += dot(score_grad, query)
                score_grads.append(score_grad)
                keys.append(key)
            back = dot_tn(jnp.concatenate(score_grads, 0), jnp.concatenate(keys, 0))
            q_grad[here, q_at : q_at + width] = back[:size]
            q_grad[here, q_at + width : q_at + 2 * width] = back[size:]

    def o_block(n):
        columns = slice(n * half_rows // 2, (n + 1) * half_rows // 2)
        o_total[columns, :] = dot_tn(state_low[:, columns], mixed[...]).astype(bf16)

    attend_back(3)
    attend_back(2)
    for n in range(4):
        o_block(n)
    scatter_o.send(bits - 1)
    if bits > 1:
        scatter_unit.add(bits - 2)
        for step in range(bits - 3, -1, -1):
            scatter_unit.send(step)
            scatter_unit.add(step)
    scatter_unit.finish()
    attend_back(1)
    attend_back(0)

    need("cos", "sin", "raw", "heads")
    head_grads[...] = jnp.zeros_like(head_grads)

    def heads_back(k, dest):
        here = rows(k)
        c, s = cos[here, :], sin[here, :]
        for at in range(0, q_cols + kv_cols, width):
            is_q = at < q_cols
            source = q_grad[here, at : at + width] if is_q else k_acc[here, at - q_cols :][:, :width]
            turned = source * scale
            grad = turned * c - pltpu.roll(turned, width // 2, 1) * s
            n = 0 if is_q else 8
            back, part = rms_back(raw[here, at : at + width], heads[n : n + 1, :], grad)
            qkv_grad[here, at : at + width] = back.astype(bf16)
            head_grads[n : n + 8, :] += jnp.sum(part.reshape(size // 8, 8, width), axis=0)
        qkv_grad[here, q_cols + kv_cols :] = v_acc[here, :].astype(bf16)
        dest[...] = dot_nt(qkv_grad[here, :], weight[:, :n_in]).astype(bf16)

    reduce = Reduce(wire, beside, own, landed, total)
    heads_back(3, beside.at[1])
    reduce.send_beside()
    heads_back(1, beside.at[0])
    reduce.forward()
    heads_back(2, own.at[1])
    reduce.send_own()
    heads_back(0, own.at[0])
    need("normed")

    def in_block(n):
        columns = slice(n * half_rows // 2, (n + 1) * half_rows // 2)
        in_total[columns, :] = dot_tn(normed[:, columns], qkv_grad[...]).astype(bf16)

    for n in (1, 3):
        in_block(n)
    scatter_in.send(bits - 1)
    for n in (0, 2):
        in_block(n)
    need("gains", "grad", "acts", "second")
    back, part = rms_back(acts[...].astype(f32), gains[0:1, :], reduce.result())
    tokens_own[...] = (state_grad[...] + back).astype(bf16)
    tokens_here = swap_out(tokens_own, tokens_landed)

    shared[0:1, :model] = jnp.sum(part, axis=0, keepdims=True)
    shared[1:2, :model] = second[0:1, :]
    shared[2:8, :model] = jnp.zeros((6, model), f32)
    shared[0:1, model:] = jnp.sum(head_grads[0:8, :], axis=0, keepdims=True)
    shared[1:2, model:] = jnp.sum(head_grads[8:16, :], axis=0, keepdims=True)
    shared[2:8, model:] = jnp.zeros((6, width), f32)
    from_core = wire.post_one(shared, shared_landed.at[0], wire.core)
    scatter_o.add(bits - 1)
    from_core()
    shared_landed[1] = shared[...] + shared_landed[0]
    from_near = wire.post_one(shared_landed.at[1], shared_landed.at[2], wire.near)
    scatter_in.add(bits - 1)
    if bits > 1:
        scatter_in.send(bits - 2)
        scatter_o.send(bits - 2)
    from_near()
    summed = shared_landed[1] + shared_landed[2]
    spread[...] = jnp.zeros_like(spread)
    spread[0:2, :] = summed[0:2, :model]
    piece = min(block, width)
    for which in range(2):
        for j in range(width // piece):
            row = summed[which : which + 1, model + j * piece : model + (j + 1) * piece]
            if piece < block:
                row = jnp.concatenate([row, jnp.zeros((1, block - piece), f32)], axis=1)
            n = 2 + which * (width // piece) + j
            spread[n : n + 1, :] = jnp.concatenate([row] * dp, axis=1)
    gain_total[...] = spread[...].T.astype(bf16)
    scatter_gain.send(bits - 1)
    layer_here()
    write(layer_landed, layer_o)
    scatter_unit.store(unit_o)
    scatter_gain.add(bits - 1)
    for step in range(bits - 2, -1, -1):
        scatter_gain.send(step)
        scatter_in.add(step)
        scatter_o.add(step)
        if step:
            scatter_in.send(step - 1)
            scatter_o.send(step - 1)
        scatter_gain.add(step)
    scatter_in.finish()
    scatter_o.finish()
    scatter_gain.finish()
    tokens_here()
    tokens_out[...] = tokens_landed[...].astype(f32)
    write(tokens_out, tokens_o)
    scatter_in.store(in_o)
    scatter_o.store(o_o)
    scatter_gain.store(gain_o)
    for copy in outs:
        copy.wait()
    wire.drain()


VMEM_SPEC = pl.BlockSpec(memory_space=pltpu.VMEM)
ANY_SPEC = pl.BlockSpec(memory_space=pl.ANY)


def forward(links, shards, tokens, out_grad, ids, inverse, width, head_part, reorder, length):
    q_w, k_w, v_w, gains_w, o_w, gate_w, up_w, down_w = shards
    cols = Columns(q_w.shape[1], k_w.shape[1], gate_w.shape[1])
    model = tokens.shape[1]
    size = length // 4
    shape = jax.ShapeDtypeStruct
    n_qk, units = cols.q_cols + cols.kv_cols, cols.units
    n_totals = 4 * cols.kv_cols // width
    outs = [
        ((length, model), bf16),
        ((length, cols.n_in), bf16),
        ((length, n_qk), f32),
        ((length, cols.q_cols), bf16),
        ((n_totals, 2 * size), f32),
        ((length, model), bf16),
        ((size, model), f32),
        ((size, model), bf16),
        ((model // 2, 3 * units), bf16),
        ((8, model), f32),
        ((model, cols.back), bf16),
        ((8, model), f32),
        ((16, width), f32),
        ((length, width), f32),
        ((length, width), f32),
        ((8, length), f32),
        ((length, 128), f32),
        ((size, model), bf16),
    ]
    reduce_set = [((2, size, model), bf16)] * 2 + [((3, size, model), bf16), ((size, model), bf16)]
    scratch = (
        [((model, cols.total), bf16)]
        + [((length, model), bf16)] * 5
        + [
            ((length, cols.n_in), bf16),
            ((length, n_qk), f32),
            ((length, cols.q_cols), bf16),
            ((n_totals, 2 * size), f32),
            ((length, width), f32),
            ((length, width), f32),
            ((length, units), f32),
            ((length, units), f32),
            ((length, units), bf16),
            ((length, units), bf16),
            ((length, units), bf16),
            ((model, 3 * units), bf16),
            ((2, model // 4, 3 * units), bf16),
            ((8, model), f32),
            ((16, width), f32),
            ((8, length), f32),
            ((length, 128), f32),
            ((size, model), f32),
            ((size, model), f32),
            ((size, model), bf16),
            ((8, model), f32),
        ]
        + reduce_set * 2
    )
    n_wire = 2 * 5 * (links.bits + 1) + 32
    args = list(shards) + [tokens, out_grad, ids]
    return pl.pallas_call(
        partial(forward_kernel, links.bits, links.slots, cols, width, head_part, reorder),
        name="forward",
        out_shape=[shape(*o) for o in outs],
        in_specs=[ANY_SPEC] * len(args) + [VMEM_SPEC],
        out_specs=[ANY_SPEC] * len(outs),
        scratch_shapes=[pltpu.VMEM(*s) for s in scratch]
        + [pltpu.SemaphoreType.DMA((n_wire,))] * 2
        + [pltpu.SemaphoreType.DMA((32,))],
        compiler_params=pltpu.CompilerParams(
            vmem_limit_bytes=66 * 10**6, collective_id=0, has_side_effects=True
        ),
    )(*args, inverse)


def backward(links, args, cols, width, restore):
    weight, qkv, unit, acts = args[0], args[1], args[-1], args[14]
    length, (size, model) = qkv.shape[0], acts.shape
    block = model // links.dp
    q_cols, kv_cols, n_in, units = cols.q_cols, cols.kv_cols, cols.n_in, cols.units
    shape = jax.ShapeDtypeStruct
    outs = [
        ((size, model), bf16),
        ((size, model), f32),
        ((block, n_in), f32),
        ((block, q_cols), f32),
        ((block, 3 * units), f32),
        ((block, 128), f32),
    ]
    loaded = [args[n] for n in range(18) if n != 16]
    scratch = [(a.shape, a.dtype) for a in loaded] + [
        ((length, q_cols), bf16),
        ((length, q_cols), f32),
        ((length, kv_cols), f32),
        ((length, kv_cols), f32),
        ((length, n_in), bf16),
        ((model, n_in), bf16),
        ((model, q_cols), bf16),
        ((model, 128), bf16),
        ((model, n_in), bf16),
        ((model, q_cols), bf16),
        (unit.shape, bf16),
        ((model, 128), bf16),
        ((size, model), bf16),
        ((size, model), bf16),
        ((size, model), bf16),
        ((size, model), f32),
        ((block, n_in), f32),
        ((block, q_cols), f32),
        ((block, 3 * units), f32),
        ((block, 128), f32),
        ((16, width), f32),
        ((8, model + width), f32),
        ((3, 8, model + width), f32),
        ((128, model), f32),
        ((2, size, model), bf16),
        ((2, size, model), bf16),
        ((3, size, model), bf16),
        ((size, model), bf16),
    ]
    n_wire = 4 * 2 * (links.bits + 1) + 16
    return pl.pallas_call(
        partial(back_kernel, links.bits, links.slots, cols, width, restore),
        name="backward",
        out_shape=[shape(*o) for o in outs],
        in_specs=[ANY_SPEC] * len(args),
        out_specs=[ANY_SPEC] * len(outs),
        scratch_shapes=[pltpu.VMEM(*s) for s in scratch]
        + [pltpu.SemaphoreType.DMA((n_wire,))] * 2
        + [pltpu.SemaphoreType.DMA((32,))] * 2,
        compiler_params=pltpu.CompilerParams(
            vmem_limit_bytes=66 * 10**6, collective_id=1, has_side_effects=True
        ),
    )(*args)


def body(
    links,
    tokens,
    block_ids,
    norm1_gain,
    q_weight,
    key_projection,
    value_projection,
    q_gain,
    k_gain,
    o_weight,
    norm2_gain,
    gate_weight,
    up_weight,
    down_weight,
    out_grad,
):
    dp, slots = links.dp, links.slots
    dp_index = lax.axis_index("dp")

    length, model = block_ids.shape[1], tokens.shape[1]
    gain_width, head_part = norm1_gain.shape[0], q_gain.shape[0]
    width = head_part * dp
    q_cols, kv_cols, units = q_weight.shape[1], key_projection.shape[1], gate_weight.shape[1]

    piece = min(gain_width, width)

    def as_columns(part):
        whole = lax.dynamic_update_slice(jnp.zeros((width,), bf16), part, (dp_index * head_part,))
        columns = whole.reshape(width // piece, piece).T
        return jnp.pad(columns, ((0, gain_width - piece), (0, 0)))

    gains_tile = jnp.concatenate(
        [norm1_gain[:, None], norm2_gain[:, None], as_columns(q_gain), as_columns(k_gain)], axis=1
    )
    gains_tile = jnp.pad(gains_tile, ((0, 0), (0, 128 - gains_tile.shape[1])))
    inverse = BASE_FREQ ** (-2.0 * (np.arange(width) % (width // 2)) / width)
    inverse = jnp.asarray(np.broadcast_to(inverse[None, :], (8, width)), f32)
    reorder = gain_width % 128 == 0
    if not reorder:
        tokens = reorder_columns(tokens, dp_index, slots)
        out_grad = reorder_columns(out_grad, dp_index, slots)
    shards = [
        q_weight,
        key_projection,
        value_projection,
        gains_tile,
        o_weight.T,
        gate_weight,
        up_weight,
        down_weight.T,
    ]
    (
        normed,
        qkv,
        raw,
        mixed,
        totals,
        state_low,
        state_grad,
        layer_sum,
        unit_total,
        second_part,
        weight,
        gains,
        heads,
        cosine,
        sine,
        block_of,
        block_rep,
        acts,
    ) = forward(
        links,
        shards,
        tokens,
        out_grad,
        jnp.broadcast_to(block_ids.astype(f32), (8, length)),
        inverse,
        width,
        head_part,
        reorder,
        length,
    )
    layer_out, tokens_grad, in_sum, o_sum, unit_sum, gain_sum = backward(
        links,
        [
            weight, qkv, raw, mixed, totals, state_low, normed, cosine, sine, block_of, block_rep,
            gains, heads, state_grad, acts, second_part, layer_sum, unit_total,
        ],
        Columns(q_cols, kv_cols, units),
        width,
        reorder,
    )
    if not reorder:
        layer_out = restore_columns(layer_out, dp_index, slots)
        tokens_grad = restore_columns(tokens_grad, dp_index, slots)
    first_total, second_total = gain_sum[:, 0], gain_sum[:, 1]
    pieces = width // piece

    def own_part(column):
        whole = gain_sum[:piece, column : column + pieces].T.reshape(-1)
        return lax.dynamic_slice(whole, (dp_index * head_part,), (head_part,))

    qs_total, ks_total = own_part(2), own_part(2 + pieces)
    o_sum = o_sum.T
    return (
        layer_out,
        tokens_grad,
        first_total,
        in_sum[:, :q_cols],
        in_sum[:, q_cols : q_cols + kv_cols],
        in_sum[:, q_cols + kv_cols :],
        qs_total,
        ks_total,
        o_sum,
        second_total,
        unit_sum[:, :units],
        unit_sum[:, units : 2 * units],
        unit_sum[:, 2 * units :].T,
    )


def solution(mesh):
    links = Links(mesh.shape["dp"], mesh.shape["tensor"])
    return jax.shard_map(
        partial(body, links),
        mesh=mesh,
        in_specs=(
            P(("dp", "tensor"), None),
            P("dp", None),
            P("dp"),
            P("dp", "tensor"),
            P("dp", "tensor"),
            P("dp", "tensor"),
            P("dp"),
            P("dp"),
            P("tensor", "dp"),
            P("dp"),
            P("dp", "tensor"),
            P("dp", "tensor"),
            P("tensor", "dp"),
            P(("dp", "tensor"), None),
        ),
        out_specs=(
            P(("dp", "tensor"), None),
            P(("dp", "tensor"), None),
            P("dp"),
            P("dp", "tensor"),
            P("dp", "tensor"),
            P("dp", "tensor"),
            P("dp"),
            P("dp"),
            P("tensor", "dp"),
            P("dp"),
            P("dp", "tensor"),
            P("dp", "tensor"),
            P("tensor", "dp"),
        ),
        check_vma=False,
    )
```

```python
from functools import partial

import jax
import jax.numpy as jnp
import numpy as np
from jax import lax
from jax.experimental import pallas as pl
from jax.experimental.pallas import tpu as pltpu
from jax.sharding import PartitionSpec as P

EPSILON = 1e-06
BASE_FREQ = 1000000.0
AXES = ("dp", "tensor")
LOG2E = 1.4426950408889634


bf16, f32 = jnp.bfloat16, jnp.float32
NT = (((1,), (1,)), ((), ()))
TN = (((0,), (0,)), ((), ()))


def dot(left, right):
    return jnp.dot(left, right, preferred_element_type=f32)


def dot_nt(left, right):
    return lax.dot_general(left, right, NT, preferred_element_type=f32)


def dot_tn(left, right):
    return lax.dot_general(left, right, TN, preferred_element_type=f32)


def rms_rate(values):
    return lax.rsqrt(jnp.mean(values * values, axis=-1, keepdims=True) + EPSILON)


def rms_back(values, gain, grad):
    rate = rms_rate(values)
    shape = values * rate
    inward = grad * gain
    back = rate * (inward - shape * jnp.mean(inward * shape, axis=-1, keepdims=True))
    return back, grad * shape


class Links:
    def __init__(self, dp, tensor):
        assert tensor == 4 and dp % 2 == 0 and dp & (dp - 1) == 0
        self.dp = dp
        self.bits = (dp // 2).bit_length() - 1
        self.paths = (list(range(self.bits)), list(range(self.bits))[::-1])
        self.slots = []
        for half, path in enumerate(self.paths):
            for p in range(dp // 2):
                offset = sum(1 << bit for j, bit in enumerate(path) if p >> j & 1)
                self.slots.append(2 * offset + half)


def reorder_columns(x, index, slots):
    rows, width = x.shape[0], x.shape[1] // len(slots)
    return jnp.concatenate(
        [lax.dynamic_slice(x, (0, (index ^ r) * width), (rows, width)) for r in slots], axis=1
    )


def restore_columns(x, index, slots):
    rows, width = x.shape[0], x.shape[1] // len(slots)
    place = [0] * len(slots)
    for n, r in enumerate(slots):
        place[r] = n
    place = jnp.asarray(place, jnp.int32)
    return jnp.concatenate(
        [
            lax.dynamic_slice(x, (0, place[index ^ b] * width), (rows, width))
            for b in range(len(slots))
        ],
        axis=1,
    )


def rows_of(part, size):
    return pl.ds(pl.multiple_of(part * size, size), size)


MESH = pl.DeviceIdType.MESH


def flip_bits(value, mask, bits):
    out = value
    for b in range(bits):
        if mask >> b & 1:
            out = out + (1 << b) * (1 - 2 * lax.rem(lax.div(value, 1 << b), 2))
    return out


class Wire:
    def __init__(self, bits, send_sem, recv_sem):
        dp, t = lax.axis_index("dp"), lax.axis_index("tensor")
        self.dp, self.bits = dp, bits
        self.c, self.a = lax.rem(dp, 2), lax.div(dp, 2)
        self.zh, self.zl = lax.div(t, 2), lax.rem(t, 2)
        self.send_sem, self.recv_sem = send_sem, recv_sem
        self.count, self.drains = 0, []
        c, a, zh, zl = self.c, self.a, self.zh, self.zl
        self.core = (2 * a + 1 - c, t)
        self.near = (dp, 2 * zh + 1 - zl)
        self.swapped = (2 * a + zh, 2 * c + zl)
        self.crossed = (2 * a + zh, 2 * (1 - c) + zl)
        self.crossed_back = (2 * a + 1 - zh, 2 * c + zl)
        self.far = [(2 * a + n, 2 * (1 - zh) + zl) for n in range(2)]
        self.plane = [(2 * flip_bits(a, 1 << b, bits) + c, t) for b in range(bits)]
        self.moves = c != zh

    def barrier(self):
        sem = pltpu.get_barrier_semaphore()
        peers = [self.core, self.near] + self.far + self.plane
        for peer in peers:
            pl.semaphore_signal(sem, inc=1, device_id=peer, device_id_type=MESH)
        pl.semaphore_wait(sem, len(peers))

    def part(self, k):
        c, zl = self.c, self.zl
        return 2 * (1 - c if k & 2 else c) + (1 - zl if k & 1 else zl)

    def slot(self, quarter):
        high, low = lax.div(quarter, 2), lax.rem(quarter, 2)
        return 2 * (high + self.c - 2 * high * self.c) + (low + self.zl - 2 * low * self.zl)

    def describe(self, src, dst, n, peer):
        return pltpu.make_async_remote_copy(
            src_ref=src,
            dst_ref=dst,
            send_sem=self.send_sem.at[n],
            recv_sem=self.recv_sem.at[n],
            device_id=peer,
            device_id_type=MESH,
        )

    def post(self, pairs, whole, peer):
        n = self.count
        self.count += 1
        for src, dst in pairs:
            self.describe(src, dst, n, peer).start()
        together = self.describe(whole, whole, n, peer)
        self.drains.append(together.wait_send)
        return together.wait_recv

    def post_one(self, src, dst, peer):
        return self.post([(src, dst)], dst, peer)

    def post_swap(self, pairs, whole):
        n = self.count
        self.count += 1
        together = self.describe(whole, whole, n, self.swapped)
        stays = pltpu.make_async_copy(whole, whole, self.recv_sem.at[n])

        @pl.when(self.moves)
        def _():
            for src, dst in pairs:
                self.describe(src, dst, n, self.swapped).start()

        @pl.when(jnp.logical_not(self.moves))
        def _():
            for src, dst in pairs:
                pltpu.make_async_copy(src, dst, self.recv_sem.at[n]).start()

        def arrive():
            pl.when(self.moves)(together.wait_recv)
            pl.when(jnp.logical_not(self.moves))(stays.wait)

        self.drains.append(lambda: pl.when(self.moves)(together.wait_send))
        return arrive

    def drain(self):
        for wait in self.drains:
            wait()
        self.drains = []


def spread_rows(wire, array):
    size = array.shape[0] // 4
    beside = wire.post_one(array.at[0:size, :], array.at[size : 2 * size, :], wire.near)
    partner = wire.post_one(array.at[0:size, :], array.at[2 * size : 3 * size, :], wire.core)

    def relay():
        beside()
        return wire.post_one(array.at[size : 2 * size, :], array.at[3 * size :, :], wire.core)

    return partner, relay


class Reduce:
    def __init__(self, wire, beside, own, landed, total):
        self.wire, self.beside, self.own = wire, beside, own
        self.landed, self.total = landed, total

    def drain(self):
        for n in self.sent:
            self.wire.drains[n]()
            self.wire.drains[n] = lambda: None

    def send_beside(self):
        self.sent = [len(self.wire.drains)]
        self.first = self.wire.post_one(self.beside.at[1], self.landed.at[0], self.wire.core)

    def forward(self):
        self.first()
        self.total[...] = (self.beside[0].astype(f32) + self.landed[0].astype(f32)).astype(bf16)
        self.sent.append(len(self.wire.drains))
        self.third = self.wire.post_one(self.total, self.landed.at[2], self.wire.near)

    def send_own(self):
        self.sent.append(len(self.wire.drains))
        self.second = self.wire.post_one(self.own.at[1], self.landed.at[1], self.wire.core)

    def result(self):
        self.second()
        self.third()
        return self.own[0].astype(f32) + self.landed[1].astype(f32) + self.landed[2].astype(f32)


class Scatter:
    def __init__(self, wire, total, landed, block, paths):
        self.wire, self.total, self.landed = wire, total, landed
        self.block, self.paths, self.waits = block, paths, {}
        self.half_rows = total.shape[0] // 2

    def send(self, step):
        have = self.block << step
        for half in range(2):
            start = half * self.half_rows
            there = slice(start + have, start + 2 * have)
            self.waits[half, step] = self.wire.post_one(
                self.total.at[there, :],
                self.landed.at[there, :],
                self.wire.plane[self.paths[half][step]],
            )

    def add(self, step):
        have = self.block << step
        chunk = min(have, 64)
        for half in range(2):
            start = half * self.half_rows
            self.waits.pop((half, step))()

            def body(n, carry):
                at = pl.multiple_of(n * chunk, chunk)
                to = pl.ds(start + at, chunk)
                more = self.landed[pl.ds(start + have + at, chunk), :]
                self.total[to, :] = (
                    self.total[to, :].astype(f32) + more.astype(f32)
                ).astype(bf16)
                return carry

            lax.fori_loop(0, have // chunk, body, 0)

    def finish(self):
        first = slice(0, self.block)
        other = slice(self.half_rows, self.half_rows + self.block)
        self.waits[0] = self.wire.post_swap(
            [(self.total.at[first, :], self.landed.at[first, :])], self.landed.at[first, :]
        )
        self.waits[1] = self.wire.post_one(
            self.total.at[other, :], self.landed.at[other, :], self.wire.crossed_back
        )

    def step(self, step):
        self.add(step)
        if step:
            self.send(step - 1)
        else:
            self.finish()

    def store(self, dest, write):
        self.waits.pop(0)()
        self.waits.pop(1)()
        other = slice(self.half_rows, self.half_rows + self.block)
        write(self.landed.at[0 : self.block, :], dest.at[0])
        write(self.landed.at[other, :], dest.at[1])


class Columns:
    def __init__(self, q_cols, kv_cols, units):
        self.q_cols, self.kv_cols, self.units = q_cols, kv_cols, units
        self.n_in = q_cols + 2 * kv_cols
        self.gains = self.n_in
        self.o = self.gains + 128
        self.gate = self.o + q_cols
        self.up = self.gate + units
        self.down = self.up + units
        self.total = self.down + units
        self.back = self.gate


def forward_kernel(bits, slots, cols, width, head_part, reorder, *refs):
    (
        q_w, k_w, v_w, gate_w, up_w, tokens, out_grad, ids_in,
        o_in, down_in, first_in, second_in, q_in, k_in, inverse,
        normed_o, qkv_o, raw_o, mixed_o, totals_o, low_o, grad_o, layer_o, passed_o, gate_o, up_o, down_o, second_o,
        weight_o, gains_o, heads_o, cos_o, sin_o, ids_o, rep_o, acts_o,
        weight, acts, grad, normed_two, state_low, normed, qkv, raw, mixed, totals, cos, sin,
        gate, up, inner, gate_grad, up_grad, gate_total, up_total, down_total, gate_landed, up_landed, gains, heads, ids, rep, state, state_grad,
        layer, second, beside_a, own_a, landed_a, total_a, beside_b, own_b, landed_b, total_b,
        gains_w, o_w, down_w, ids_low,
        send_sem, recv_sem, out_sem,
    ) = refs
    wire = Wire(bits, send_sem, recv_sem)
    size, model = tokens.shape
    q_cols, kv_cols, units = cols.q_cols, cols.kv_cols, cols.units
    n_in = cols.n_in
    dp = len(slots)
    block = model // dp
    half_rows = model // 2
    outs = []

    def write(src, dst):
        outs.append(pltpu.make_async_copy(src, dst, out_sem.at[len(outs)]))
        outs[-1].start()

    def rows(k):
        return slice(k * size, (k + 1) * size)

    piece = min(block, width)
    lane = lax.broadcasted_iota(jnp.int32, (1, width), 1)
    mine = lax.div(lane, head_part) == wire.dp
    tile_rows = [first_in[...].astype(f32), second_in[...].astype(f32)]
    for ref in (q_in, k_in):
        placed = jnp.where(mine, jnp.concatenate([ref[...].astype(f32)] * dp, axis=1), 0.0)
        for at in range(0, width, piece):
            row = placed[:, at : at + piece]
            if piece < block:
                row = jnp.concatenate([row, jnp.zeros((1, block - piece), f32)], axis=1)
            tile_rows.append(row)
    tile_rows.append(jnp.zeros((128 - len(tile_rows), block), f32))
    gains_w[...] = jnp.concatenate(tile_rows, axis=0).T.astype(bf16)
    o_w[...] = o_in[...].T
    down_w[...] = down_in[...].T
    wire.barrier()

    groups = {
        "in": (0, cols.o, [q_w, k_w, v_w, gains_w]),
        "o": (cols.o, cols.gate, [o_w]),
        "gate": (cols.gate, cols.up, [gate_w]),
        "up": (cols.up, cols.down, [up_w]),
        "down": (cols.down, cols.total, [down_w]),
    }
    paths = (list(range(bits)), list(range(bits))[::-1])
    pending = {}

    def start_weights(name):
        low, high, shards = groups[name]
        for half in range(2):
            there = pl.ds(half * half_rows, block)
            pairs, at = [], low
            for shard in shards:
                pairs.append((shard, weight.at[there, at : at + shard.shape[1]]))
                at += shard.shape[1]
            whole = weight.at[there, low:high]
            if half == 0:
                pending[name, half, 0] = wire.post_swap(pairs, whole)
            else:
                pending[name, half, 0] = wire.post(pairs, whole, wire.crossed)

    def step_weights(name, step):
        low, high, _ = groups[name]
        for half in range(2):
            pending.pop((name, half, step))()
            if step < bits:
                have = block << step
                start = half * half_rows
                pending[name, half, step + 1] = wire.post_one(
                    weight.at[start : start + have, low:high],
                    weight.at[start + have : start + 2 * have, low:high],
                    wire.plane[paths[half][step]],
                )

    def swap_rows(source, dest):
        own = dest.at[0:size, :]
        if reorder:
            pairs = [
                (
                    source.at[
                        :,
                        pl.ds(
                            pl.multiple_of(flip_bits(wire.dp, r, bits + 1) * block, block), block
                        ),
                    ],
                    dest.at[0:size, n * block : (n + 1) * block],
                )
                for n, r in enumerate(slots)
            ]
        else:
            pairs = [(source, own)]
        return wire.post_swap(pairs, own)

    start_weights("in")

    base = lax.broadcasted_iota(jnp.int32, (size, width), 0).astype(f32) * inverse[0:1, :]
    base_cos, base_sin = jnp.cos(base), jnp.sin(base)
    sign = jnp.where(lax.broadcasted_iota(jnp.int32, (1, width), 1) < width // 2, -1.0, 1.0)
    for k in range(4):
        more = (wire.part(k) * size).astype(f32) * inverse[...]
        more_cos, more_sin = jnp.cos(more)[0:1], jnp.sin(more)[0:1]
        cos[rows(k), :] = base_cos * more_cos - base_sin * more_sin
        sin[rows(k), :] = (base_sin * more_cos + base_cos * more_sin) * sign
    write(cos, cos_o)
    write(sin, sin_o)

    step_weights("in", 0)
    acts_here = swap_rows(tokens, acts)
    ids_here = wire.post_swap([(ids_in, ids_low)], ids_low)
    start_weights("o")
    for step in range(1, bits):
        step_weights("in", step)
    acts_here()
    acts_partner, acts_relay = spread_rows(wire, acts)
    start_weights("gate")
    start_weights("up")
    ids_here()
    ids[...] = jnp.broadcast_to(ids_low[...].astype(f32), ids.shape)
    rep[...] = jnp.broadcast_to(ids[0:1, :], (128, 4 * size)).T
    write(ids, ids_o)
    write(rep, rep_o)
    write(acts.at[0:size, :], acts_o)
    step_weights("o", 0)
    step_weights("in", bits)

    turned = weight[:, cols.gains : cols.gains + 128].astype(f32).T
    gains[...] = turned[0:8, :]
    for which in range(2):
        parts = []
        for j in range(width // piece):
            row = turned[2 + which * (width // piece) + j :][:1]
            part = row[:, 0:piece]
            for n in range(1, dp):
                part = part + row[:, n * block : n * block + piece]
            parts.append(part)
        heads[which * 8 : which * 8 + 8, :] = jnp.broadcast_to(
            jnp.concatenate(parts, axis=1), (8, width)
        )
    write(gains, gains_o)
    write(heads, heads_o)
    first_gain, second_gain = gains[0:1, :], gains[1:2, :]
    q_gain, k_gain = heads[0:1, :], heads[8:9, :]

    def front(k):
        here = rows(k)
        values = acts[here, :].astype(f32)
        low = (values * rms_rate(values) * first_gain).astype(bf16)
        normed[here, :] = low
        product = dot(low, weight[:, :n_in])
        c, s = cos[here, :], sin[here, :]
        for at in range(0, q_cols + kv_cols, width):
            head = product[:, at : at + width]
            raw[here, at : at + width] = head
            head = head * rms_rate(head) * (q_gain if at < q_cols else k_gain)
            turn = head * c + pltpu.roll(head, width // 2, 1) * s
            qkv[here, at : at + width] = turn.astype(bf16)
        qkv[here, q_cols + kv_cols :] = product[:, q_cols + kv_cols :].astype(bf16)

    front(0)
    acts_partner()
    front(2)
    for step in range(1, bits):
        step_weights("o", step)
    acts_across = acts_relay()
    front(1)
    acts_across()
    front(3)
    write(normed, normed_o)
    write(qkv, qkv_o)
    write(raw, raw_o)

    factor = width ** (-0.5) * LOG2E
    ones = jnp.ones((4 * size, width), bf16)
    assert q_cols == 2 * kv_cols

    def attend(quarter, count, masked):
        place = pl.multiple_of(wire.slot(quarter) * size, size)
        here = pl.ds(place, size)
        seen_by = rep[pl.ds(pl.multiple_of(quarter * size, size), size), :]
        seen_by = jnp.concatenate([seen_by] * (size // 128), axis=1)
        for h in range(kv_cols // width):
            q_at, k_at = 2 * h * width, q_cols + h * width
            v_at = k_at + kv_cols
            query = jnp.concatenate(
                [qkv[here, q_at : q_at + width], qkv[here, q_at + width : q_at + 2 * width]], 0
            )
            probs, values = [], []
            for n in range(count):
                there = rows_of(wire.slot(jnp.int32(n)), size)
                prob = jnp.exp2(dot_nt(query, qkv[there, k_at : k_at + width]) * factor)
                if n in masked:
                    seen = ids[0:1, n * size : (n + 1) * size] <= seen_by
                    prob = jnp.where(jnp.concatenate([seen, seen], 0), prob, 0.0)
                probs.append(prob.astype(bf16))
                values.append(qkv[there, v_at : v_at + width])
            value = jnp.concatenate([jnp.concatenate(values, 0), ones[: count * size]], axis=1)
            out = dot(jnp.concatenate(probs, axis=1), value)
            total = out[:, width:]
            out = (out[:, :width] / total).astype(bf16)
            mixed[here, q_at : q_at + width] = out[:size]
            mixed[here, q_at + width : q_at + 2 * width] = out[size:]
            totals[pl.ds(quarter * (kv_cols // width) + h, 1), :] = total.T[0:1]
        return here

    def attend_pair(first, dest):
        here = attend(first, 3, (0, 1, 2))
        dest[wire.c] = dot_nt(mixed[here, :], weight[:, cols.o : cols.gate]).astype(bf16)
        here = attend(first + 2, 4, (2, 3))
        dest[1 - wire.c] = dot_nt(mixed[here, :], weight[:, cols.o : cols.gate]).astype(bf16)

    grad_here = swap_rows(out_grad, grad)
    start_weights("down")
    step_weights("o", bits)
    reduce_o = Reduce(wire, beside_a, own_a, landed_a, total_a)
    attend_pair(1 - wire.zl, beside_a)
    reduce_o.send_beside()
    step_weights("gate", 0)
    step_weights("up", 0)
    reduce_o.forward()
    attend_pair(wire.zl, own_a)
    reduce_o.send_own()
    for step in range(1, bits):
        step_weights("gate", step)
        step_weights("up", step)
    write(mixed, mixed_o)
    write(totals, totals_o)
    write(weight.at[:, : cols.back], weight_o)
    state[...] = acts[0:size, :].astype(f32) + reduce_o.result()
    values = state[...]
    normed_two[0:size, :] = (values * rms_rate(values) * second_gain).astype(bf16)
    two_partner, two_relay = spread_rows(wire, normed_two)
    grad_here()
    step_weights("down", 0)
    step_weights("gate", bits)
    step_weights("up", bits)

    def units_forward(k):
        values = normed_two[rows(k), :]
        gate[rows(k), :] = dot(values, weight[:, cols.gate : cols.up])
        up[rows(k), :] = dot(values, weight[:, cols.up : cols.down])

    def units_back(k, dest):
        here = rows(k)
        gate_here, up_here = gate[here, :], up[here, :]
        inward = dot(grad[here, :], weight[:, cols.down : cols.total])
        sg = jax.nn.sigmoid(gate_here)
        silu = gate_here * sg
        inner[here, :] = (silu * up_here).astype(bf16)
        d_gate = (inward * up_here * sg * (1.0 + gate_here * (1.0 - sg))).astype(bf16)
        d_up = (inward * silu).astype(bf16)
        gate_grad[here, :] = d_gate
        up_grad[here, :] = d_up
        dest[...] = (
            dot_nt(d_gate, weight[:, cols.gate : cols.up])
            + dot_nt(d_up, weight[:, cols.up : cols.down])
        ).astype(bf16)

    units_forward(0)
    two_partner()
    units_forward(2)
    two_across = two_relay()
    grad_partner, grad_relay = spread_rows(wire, grad)
    units_forward(1)
    two_across()
    units_forward(3)
    for step in range(1, bits):
        step_weights("down", step)
    grad_partner()
    grad_across = grad_relay()
    grad_across()
    step_weights("down", bits)
    reduce_two = Reduce(wire, beside_b, own_b, landed_b, total_b)
    units_back(3, beside_b.at[1])
    reduce_two.send_beside()
    units_back(1, beside_b.at[0])
    reduce_two.forward()
    units_back(2, own_b.at[1])
    reduce_two.send_own()
    units_back(0, own_b.at[0])

    quarter_rows = half_rows // 2

    def unit_block(total, left, right, n):
        columns = slice(n * quarter_rows, (n + 1) * quarter_rows)
        total[columns, :] = dot_tn(left[:, columns], right[...]).astype(bf16)

    scatter_gate = Scatter(wire, gate_total, gate_landed, block, paths)
    scatter_up = Scatter(wire, up_total, up_landed, block, paths)
    for n in (1, 3):
        unit_block(gate_total, normed_two, gate_grad, n)
    scatter_gate.send(bits - 1)
    for n in (1, 3):
        unit_block(up_total, normed_two, up_grad, n)
    scatter_up.send(bits - 1)
    for n in (0, 2):
        unit_block(gate_total, normed_two, gate_grad, n)
        unit_block(up_total, normed_two, up_grad, n)
    back, gain_part = rms_back(state[...], second_gain, reduce_two.result())
    second[...] = jnp.broadcast_to(jnp.sum(gain_part, axis=0, keepdims=True), second.shape)
    state_grad[...] = grad[0:size, :].astype(f32) + back
    state_low[0:size, :] = state_grad[...].astype(bf16)
    reduce_o.drain()
    low_partner, low_relay = spread_rows(wire, state_low)
    write(second, second_o)
    write(state_grad, grad_o)
    for n in range(4):
        unit_block(down_total, grad, inner, n)
    write(down_total, down_o)
    scatter_gate.step(bits - 1)

    def layer_part(k):
        return dot_nt(inner[rows(k), :], weight[:, cols.down : cols.total])

    beside_a[1] = layer_part(3).astype(bf16)
    layer_first = wire.post_one(beside_a.at[1], landed_a.at[0], wire.core)
    own_a[1] = layer_part(2).astype(bf16)
    layer_second = wire.post_one(own_a.at[1], landed_a.at[1], wire.core)
    passing = layer_part(1)
    layer_first()
    total_a[...] = (passing + landed_a[0].astype(f32)).astype(bf16)
    write(total_a, passed_o)
    staying = layer_part(0)
    layer_second()
    layer[...] = state[...] + staying + landed_a[1].astype(f32)
    write(layer, layer_o)
    scatter_up.add(bits - 1)
    if bits > 1:
        scatter_up.send(bits - 2)
    low_partner()
    low_across = low_relay()
    for step in range(bits - 2, -1, -1):
        scatter_gate.step(step)
        scatter_up.add(step)
        if step:
            scatter_up.send(step - 1)
    for half in range(2):
        start = half * half_rows
        write(up_total.at[start : start + block, :], up_o.at[half])
    low_across()
    write(state_low, low_o)
    scatter_gate.store(gate_o, write)
    for copy in outs:
        copy.wait()
    wire.drain()


def back_kernel(bits, slots, cols, width, restore, *refs):
    (
        weight_i, qkv_i, raw_i, mixed_i, totals_i, low_i, normed_i, cos_i, sin_i, ids_i, rep_i,
        gains_i, heads_i, grad_i, acts_i, second_i, layer_i, unit_i, passed_i, up_i,
        layer_o, tokens_o, in_o, o_o, unit_o, gain_o, up_o,
        weight, qkv, raw, mixed, totals, state_low, normed, cos, sin, ids, rep, gains, heads,
        state_grad, acts, second, layer, unit,
        mixed_grad, q_grad, k_acc, v_acc, qkv_grad, in_total, o_total, gain_total,
        in_landed, o_landed, unit_landed, gain_landed, up_landed, layer_near, layer_own, layer_landed,
        tokens_own, tokens_landed, head_grads, shared, shared_landed, spread,
        beside, own, landed, total, send_sem, recv_sem, in_sem, out_sem,
    ) = refs
    wire = Wire(bits, send_sem, recv_sem)
    size, model = acts.shape
    q_cols, kv_cols, units, n_in = cols.q_cols, cols.kv_cols, cols.units, cols.n_in
    dp = len(slots)
    block, half_rows = model // dp, model // 2
    paths = (list(range(bits)), list(range(bits))[::-1])
    loads, outs = {}, []

    def load(name, src, dst):
        loads[name] = pltpu.make_async_copy(src, dst, in_sem.at[len(loads)])
        loads[name].start()

    taken = set()

    def need(*names):
        for name in names:
            if name not in taken:
                taken.add(name)
                loads[name].wait()

    def write(src, dst):
        outs.append(pltpu.make_async_copy(src, dst, out_sem.at[len(outs)]))
        outs[-1].start()

    def rows(k):
        return slice(k * size, (k + 1) * size)

    for name, src, dst in (
        ("low", low_i, state_low),
        ("weight", weight_i, weight),
        ("mixed", mixed_i, mixed),
        ("unit", unit_i, unit),
        ("qkv", qkv_i, qkv),
        ("totals", totals_i, totals),
        ("ids", ids_i, ids),
        ("rep", rep_i, rep),
        ("cos", cos_i, cos),
        ("sin", sin_i, sin),
        ("raw", raw_i, raw),
        ("heads", heads_i, heads),
        ("normed", normed_i, normed),
        ("gains", gains_i, gains),
        ("grad", grad_i, state_grad),
        ("acts", acts_i, acts),
        ("second", second_i, second),
        ("layer", layer_i, layer),
    ):
        load(name, src, dst)
    wire.barrier()

    def swap_out(source, dest):
        if restore:
            seq = 2 * wire.a + wire.zh
            pairs = [
                (
                    source.at[:, n * block : (n + 1) * block],
                    dest.at[
                        :,
                        pl.ds(
                            pl.multiple_of(flip_bits(seq, r, bits + 1) * block, block), block
                        ),
                    ],
                )
                for n, r in enumerate(slots)
            ]
        else:
            pairs = [(source, dest)]
        return wire.post_swap(pairs, dest)

    up_here = [
        wire.post_swap([(up_i.at[0], up_landed.at[0])], up_landed.at[0]),
        wire.post_one(up_i.at[1], up_landed.at[1], wire.crossed_back),
    ]
    layer_beside = wire.post_one(passed_i, layer_near, wire.near)
    scatter_unit = Scatter(wire, unit, unit_landed, block, paths)
    need("unit")
    scatter_unit.send(bits - 1)
    scatter_in = Scatter(wire, in_total, in_landed, block, paths)
    scatter_o = Scatter(wire, o_total, o_landed, block, paths)
    scatter_gain = Scatter(wire, gain_total, gain_landed, block, paths)

    need("low", "weight")
    for k in range(4):
        mixed_grad[rows(k), :] = dot(
            state_low[rows(k), :], weight[:, cols.o : cols.o + q_cols]
        ).astype(bf16)
    need("mixed")
    scale = width ** (-0.5)
    factor = scale * LOG2E
    k_acc[...] = jnp.zeros_like(k_acc)
    v_acc[...] = jnp.zeros_like(v_acc)
    ones = jnp.ones((8, width), bf16)
    need("qkv", "totals", "ids", "rep")

    def there_of(quarter):
        return rows_of(wire.slot(jnp.int32(quarter)), size)

    def attend_back(quarter):
        here, count = there_of(quarter), min(quarter + 2, 4)
        row_ids = ids[0:1, quarter * size : (quarter + 1) * size]
        row_ids = jnp.concatenate([row_ids, row_ids], axis=1)
        for h in range(kv_cols // width):
            q_at, k_at = 2 * h * width, q_cols + h * width
            v_at = k_at + kv_cols

            def both(ref):
                return jnp.concatenate(
                    [ref[here, q_at : q_at + width], ref[here, q_at + width : q_at + 2 * width]], 0
                )

            query, out_grad = both(qkv), both(mixed_grad)
            product = out_grad.astype(f32) * both(mixed).astype(f32)
            product_high = product.astype(bf16)
            product_low = (product - product_high.astype(f32)).astype(bf16)
            centre = (dot_nt(ones, product_high) + dot_nt(ones, product_low))[0:1]
            n = quarter * (kv_cols // width) + h
            level = -jnp.log2(totals[n : n + 1, :])
            columns = slice(h * width, (h + 1) * width)
            score_grads, keys = [], []
            for m in range(count):
                there = there_of(m)
                key, value = qkv[there, k_at : k_at + width], qkv[there, v_at : v_at + width]
                prob = jnp.exp2(dot_nt(key, query) * factor + level)
                if m >= quarter:
                    key_ids = rep[m * size : (m + 1) * size, :]
                    seen = jnp.concatenate([key_ids] * (2 * size // 128), axis=1) <= row_ids
                    prob = jnp.where(seen, prob, 0.0)
                score_grad = (prob * (dot_nt(value, out_grad) - centre)).astype(bf16)
                v_acc[there, columns] += dot(prob.astype(bf16), out_grad)
                k_acc[there, columns] += dot(score_grad, query)
                score_grads.append(score_grad)
                keys.append(key)
            back = dot_tn(jnp.concatenate(score_grads, 0), jnp.concatenate(keys, 0))
            q_grad[here, q_at : q_at + width] = back[:size]
            q_grad[here, q_at + width : q_at + 2 * width] = back[size:]

    def o_block(n):
        columns = slice(n * half_rows // 2, (n + 1) * half_rows // 2)
        o_total[columns, :] = dot_tn(state_low[:, columns], mixed[...]).astype(bf16)

    for n in range(4):
        o_block(n)
    scatter_o.send(bits - 1)
    attend_back(3)
    attend_back(2)
    need("layer")
    layer_beside()
    layer_own[...] = (layer[...] + layer_near[...].astype(f32)).astype(bf16)
    layer_here = swap_out(layer_own, layer_landed)
    attend_back(1)
    scatter_unit.step(bits - 1)
    attend_back(0)

    need("cos", "sin", "raw", "heads")
    head_grads[...] = jnp.zeros_like(head_grads)

    def heads_back(k, dest):
        here = rows(k)
        c, s = cos[here, :], sin[here, :]
        for at in range(0, q_cols + kv_cols, width):
            is_q = at < q_cols
            source = q_grad[here, at : at + width] if is_q else k_acc[here, at - q_cols :][:, :width]
            turned = source * scale
            grad = turned * c - pltpu.roll(turned, width // 2, 1) * s
            n = 0 if is_q else 8
            back, part = rms_back(raw[here, at : at + width], heads[n : n + 1, :], grad)
            qkv_grad[here, at : at + width] = back.astype(bf16)
            head_grads[n : n + 8, :] += jnp.sum(part.reshape(size // 8, 8, width), axis=0)
        qkv_grad[here, q_cols + kv_cols :] = v_acc[here, :].astype(bf16)
        dest[...] = dot_nt(qkv_grad[here, :], weight[:, :n_in]).astype(bf16)

    reduce = Reduce(wire, beside, own, landed, total)
    heads_back(3, beside.at[1])
    reduce.send_beside()
    heads_back(1, beside.at[0])
    reduce.forward()
    for step in range(bits - 1, -1, -1):
        scatter_o.add(step)
        if step:
            scatter_o.send(step - 1)
            scatter_unit.step(step - 1)
    heads_back(2, own.at[1])
    reduce.send_own()
    heads_back(0, own.at[0])
    need("normed")

    def in_block(n):
        columns = slice(n * half_rows // 2, (n + 1) * half_rows // 2)
        in_total[columns, :] = dot_tn(normed[:, columns], qkv_grad[...]).astype(bf16)

    for n in (1, 3):
        in_block(n)
    scatter_in.send(bits - 1)
    for n in (0, 2):
        in_block(n)
    need("gains", "grad", "acts", "second")
    inward = reduce.result()
    back, part = rms_back(acts[...].astype(f32), gains[0:1, :], inward)
    tokens_own[...] = (state_grad[...] + back).astype(bf16)
    tokens_here = swap_out(tokens_own, tokens_landed)

    shared[0:1, :model] = jnp.sum(part, axis=0, keepdims=True)
    shared[1:2, :model] = second[0:1, :]
    shared[2:8, :model] = jnp.zeros((6, model), f32)
    shared[0:1, model:] = jnp.sum(head_grads[0:8, :], axis=0, keepdims=True)
    shared[1:2, model:] = jnp.sum(head_grads[8:16, :], axis=0, keepdims=True)
    shared[2:8, model:] = jnp.zeros((6, width), f32)
    from_core = wire.post_one(shared, shared_landed.at[0], wire.core)
    scatter_in.add(bits - 1)
    if bits > 1:
        scatter_in.send(bits - 2)
    from_core()
    shared_landed[1] = shared[...] + shared_landed[0]
    from_near = wire.post_one(shared_landed.at[1], shared_landed.at[2], wire.near)
    from_near()
    summed = shared_landed[1] + shared_landed[2]
    spread[...] = jnp.zeros_like(spread)
    spread[0:2, :] = summed[0:2, :model]
    piece = min(block, width)
    for which in range(2):
        for j in range(width // piece):
            row = summed[which : which + 1, model + j * piece : model + (j + 1) * piece]
            if piece < block:
                row = jnp.concatenate([row, jnp.zeros((1, block - piece), f32)], axis=1)
            n = 2 + which * (width // piece) + j
            spread[n : n + 1, :] = jnp.concatenate([row] * dp, axis=1)
    gain_total[...] = spread[...].T.astype(bf16)
    scatter_gain.send(bits - 1)
    for half in range(2):
        up_here[half]()
    write(up_landed, up_o)
    scatter_unit.store(unit_o, write)
    scatter_gain.add(bits - 1)
    for step in range(bits - 2, -1, -1):
        scatter_gain.send(step)
        scatter_in.add(step)
        if step:
            scatter_in.send(step - 1)
        else:
            scatter_in.finish()
        scatter_gain.add(step)
    if bits == 1:
        scatter_in.finish()
    scatter_gain.finish()
    scatter_o.finish()
    tokens_here()
    write(tokens_landed, tokens_o)
    scatter_in.store(in_o, write)
    layer_here()
    write(layer_landed, layer_o)
    scatter_gain.store(gain_o, write)
    scatter_o.store(o_o, write)
    for copy in outs:
        copy.wait()
    wire.drain()


def finish_kernel(cols, width, head_part, *refs):
    (
        layer_i, tokens_i, in_i, o_i, down_i, gain_i, up_i, gate_i,
        layer_o, tokens_o, first_o, q_o, k_o, v_o, qs_o, ks_o, o_o, second_o, gate_o, up_o, down_o,
    ) = refs
    q_cols, kv_cols, units = cols.q_cols, cols.kv_cols, cols.units
    layer_o[...] = layer_i[...]
    tokens_o[...] = tokens_i[...].astype(f32)

    def both(ref, low, high):
        return ref[0, :, low:high].astype(f32) + ref[1, :, low:high].astype(f32)

    q_o[...] = both(in_i, 0, q_cols)
    k_o[...] = both(in_i, q_cols, q_cols + kv_cols)
    v_o[...] = both(in_i, q_cols + kv_cols, cols.n_in)
    o_o[...] = both(o_i, 0, q_cols).T
    gate_o[...] = both(gate_i, 0, units)
    up_o[...] = both(up_i, 0, units)
    down_o[...] = both(down_i, 0, units).T
    turned = both(gain_i, 0, 128).T
    first_o[...] = turned[0:1, :]
    second_o[...] = turned[1:2, :]
    block = turned.shape[1]
    piece = min(block, width)
    count = width // piece
    dp = lax.axis_index("dp")
    for which, ref in enumerate((qs_o, ks_o)):
        at = 2 + which * count
        whole = jnp.concatenate([turned[at + j : at + j + 1, :piece] for j in range(count)], axis=1)
        out = jnp.zeros((1, head_part), f32)
        for n in range(width // head_part):
            out = jnp.where(dp == n, whole[:, n * head_part : (n + 1) * head_part], out)
        ref[...] = out


VMEM_SPEC = pl.BlockSpec(memory_space=pltpu.VMEM)
ANY_SPEC = pl.BlockSpec(memory_space=pl.ANY)


def forward(links, shards, tokens, out_grad, ids, small, width, head_part, reorder):
    q_w, k_w, gate_w = shards[0], shards[1], shards[3]
    cols = Columns(q_w.shape[1], k_w.shape[1], gate_w.shape[1])
    length, model = ids.shape[1], tokens.shape[1]
    size, block = length // 4, q_w.shape[0]
    shape = jax.ShapeDtypeStruct
    n_qk, units = cols.q_cols + cols.kv_cols, cols.units
    n_totals = 4 * cols.kv_cols // width
    outs = [
        ((length, model), bf16),
        ((length, cols.n_in), bf16),
        ((length, n_qk), f32),
        ((length, cols.q_cols), bf16),
        ((n_totals, 2 * size), f32),
        ((length, model), bf16),
        ((size, model), f32),
        ((size, model), f32),
        ((size, model), bf16),
        ((2, block, units), bf16),
        ((2, block, units), bf16),
        ((model, units), bf16),
        ((8, model), f32),
        ((model, cols.back), bf16),
        ((8, model), f32),
        ((16, width), f32),
        ((length, width), f32),
        ((length, width), f32),
        ((8, length), f32),
        ((length, 128), f32),
        ((size, model), bf16),
    ]
    reduce_set = [((2, size, model), bf16)] * 2 + [((3, size, model), bf16), ((size, model), bf16)]
    scratch = (
        [((model, cols.total), bf16)]
        + [((length, model), bf16)] * 5
        + [
            ((length, cols.n_in), bf16),
            ((length, n_qk), f32),
            ((length, cols.q_cols), bf16),
            ((n_totals, 2 * size), f32),
            ((length, width), f32),
            ((length, width), f32),
            ((length, units), f32),
            ((length, units), f32),
            ((length, units), bf16),
            ((length, units), bf16),
            ((length, units), bf16),
            ((model, units), bf16),
            ((model, units), bf16),
            ((model, units), bf16),
            ((model, units), bf16),
            ((model, units), bf16),
            ((8, model), f32),
            ((16, width), f32),
            ((8, length), f32),
            ((length, 128), f32),
            ((size, model), f32),
            ((size, model), f32),
            ((size, model), f32),
            ((8, model), f32),
        ]
        + reduce_set * 2
        + [((block, 128), bf16), ((block, cols.q_cols), bf16), ((block, units), bf16)]
        + [((1, length), jnp.int32)]
    )
    n_wire = 2 * 7 * (links.bits + 1) + 36
    args = list(shards) + [tokens, out_grad, ids]
    return pl.pallas_call(
        partial(forward_kernel, links.bits, links.slots, cols, width, head_part, reorder),
        name="forward",
        out_shape=[shape(*o) for o in outs],
        in_specs=[ANY_SPEC] * len(args) + [VMEM_SPEC] * len(small),
        out_specs=[ANY_SPEC] * len(outs),
        scratch_shapes=[pltpu.VMEM(*s) for s in scratch]
        + [pltpu.SemaphoreType.DMA((n_wire,))] * 2
        + [pltpu.SemaphoreType.DMA((32,))],
        compiler_params=pltpu.CompilerParams(
            vmem_limit_bytes=66 * 10**6, collective_id=0, has_side_effects=True
        ),
    )(*args, *small)


def backward(links, args, cols, width, restore):
    weight, qkv, unit, acts = args[0], args[1], args[17], args[14]
    length, (size, model) = qkv.shape[0], acts.shape
    block = model // links.dp
    q_cols, kv_cols, n_in, units = cols.q_cols, cols.kv_cols, cols.n_in, cols.units
    shape = jax.ShapeDtypeStruct
    outs = [
        ((size, model), bf16),
        ((size, model), bf16),
        ((2, block, n_in), bf16),
        ((2, block, q_cols), bf16),
        ((2, block, units), bf16),
        ((2, block, 128), bf16),
        ((2, block, units), bf16),
    ]
    loaded = args[:18]
    scratch = [(a.shape, a.dtype) for a in loaded] + [
        ((length, q_cols), bf16),
        ((length, q_cols), f32),
        ((length, kv_cols), f32),
        ((length, kv_cols), f32),
        ((length, n_in), bf16),
        ((model, n_in), bf16),
        ((model, q_cols), bf16),
        ((model, 128), bf16),
        ((model, n_in), bf16),
        ((model, q_cols), bf16),
        (unit.shape, bf16),
        ((model, 128), bf16),
        ((2, block, units), bf16),
        ((size, model), bf16),
        ((size, model), bf16),
        ((size, model), bf16),
        ((size, model), bf16),
        ((size, model), bf16),
        ((16, width), f32),
        ((8, model + width), f32),
        ((3, 8, model + width), f32),
        ((128, model), f32),
        ((2, size, model), bf16),
        ((2, size, model), bf16),
        ((3, size, model), bf16),
        ((size, model), bf16),
    ]
    n_wire = 4 * 2 * (links.bits + 1) + 16
    return pl.pallas_call(
        partial(back_kernel, links.bits, links.slots, cols, width, restore),
        name="backward",
        out_shape=[shape(*o) for o in outs],
        in_specs=[ANY_SPEC] * len(args),
        out_specs=[ANY_SPEC] * len(outs),
        scratch_shapes=[pltpu.VMEM(*s) for s in scratch]
        + [pltpu.SemaphoreType.DMA((n_wire,))] * 2
        + [pltpu.SemaphoreType.DMA((32,))] * 2,
        compiler_params=pltpu.CompilerParams(
            vmem_limit_bytes=66 * 10**6, collective_id=1, has_side_effects=True
        ),
    )(*args)


def finish(sums, cols, width, head_part):
    block, (size, model) = sums[2].shape[1], sums[0].shape
    shape = jax.ShapeDtypeStruct
    outs = [
        (block_out, f32)
        for block_out in (
            (size, model),
            (1, block),
            (block, cols.q_cols),
            (block, cols.kv_cols),
            (block, cols.kv_cols),
            (1, head_part),
            (1, head_part),
            (cols.q_cols, block),
            (1, block),
            (block, cols.units),
            (block, cols.units),
            (cols.units, block),
        )
    ]
    return pl.pallas_call(
        partial(finish_kernel, cols, width, head_part),
        name="finish",
        out_shape=[shape((size, model), bf16)] + [shape(*o) for o in outs],
        in_specs=[VMEM_SPEC] * len(sums),
        out_specs=[VMEM_SPEC] * (1 + len(outs)),
    )(*sums)


def body(
    links,
    tokens,
    block_ids,
    norm1_gain,
    q_weight,
    key_projection,
    value_projection,
    q_gain,
    k_gain,
    o_weight,
    norm2_gain,
    gate_weight,
    up_weight,
    down_weight,
    out_grad,
):
    dp, slots = links.dp, links.slots
    dp_index = lax.axis_index("dp")

    length, model = block_ids.shape[1], tokens.shape[1]
    gain_width, head_part = norm1_gain.shape[0], q_gain.shape[0]
    width = head_part * dp
    cols = Columns(q_weight.shape[1], key_projection.shape[1], gate_weight.shape[1])
    inverse = BASE_FREQ ** (-2.0 * (np.arange(width) % (width // 2)) / width)
    inverse = jnp.asarray(np.broadcast_to(inverse[None, :], (8, width)), f32)
    reorder = gain_width % 128 == 0
    if not reorder:
        tokens = reorder_columns(tokens, dp_index, slots)
        out_grad = reorder_columns(out_grad, dp_index, slots)
    (
        normed,
        qkv,
        raw,
        mixed,
        totals,
        state_low,
        state_grad,
        layer_sum,
        passed,
        gate_sum,
        up_sum,
        down_total,
        second_part,
        weight,
        gains,
        heads,
        cosine,
        sine,
        block_of,
        block_rep,
        acts,
    ) = forward(
        links,
        [q_weight, key_projection, value_projection, gate_weight, up_weight],
        tokens,
        out_grad,
        block_ids,
        [o_weight, down_weight]
        + [gain[None, :] for gain in (norm1_gain, norm2_gain, q_gain, k_gain)]
        + [inverse],
        width,
        head_part,
        reorder,
    )
    sums = backward(
        links,
        [
            weight, qkv, raw, mixed, totals, state_low, normed, cosine, sine, block_of, block_rep,
            gains, heads, state_grad, acts, second_part, layer_sum, down_total, passed, up_sum,
        ],
        cols,
        width,
        reorder,
    )
    if not reorder:
        sums = list(sums)
        sums[:2] = [restore_columns(x, dp_index, slots) for x in sums[:2]]
    outs = list(finish(list(sums) + [gate_sum], cols, width, head_part))
    for n in (2, 6, 7, 9):
        outs[n] = outs[n][0]
    return tuple(outs)


def solution(mesh):
    links = Links(mesh.shape["dp"], mesh.shape["tensor"])
    return jax.shard_map(
        partial(body, links),
        mesh=mesh,
        in_specs=(
            P(("dp", "tensor"), None),
            P("dp", None),
            P("dp"),
            P("dp", "tensor"),
            P("dp", "tensor"),
            P("dp", "tensor"),
            P("dp"),
            P("dp"),
            P("tensor", "dp"),
            P("dp"),
            P("dp", "tensor"),
            P("dp", "tensor"),
            P("tensor", "dp"),
            P(("dp", "tensor"), None),
        ),
        out_specs=(
            P(("dp", "tensor"), None),
            P(("dp", "tensor"), None),
            P("dp"),
            P("dp", "tensor"),
            P("dp", "tensor"),
            P("dp", "tensor"),
            P("dp"),
            P("dp"),
            P("tensor", "dp"),
            P("dp"),
            P("dp", "tensor"),
            P("dp", "tensor"),
            P("tensor", "dp"),
        ),
        check_vma=False,
    )
```

```python
from functools import partial

import jax
import jax.numpy as jnp
import numpy as np
from jax import lax
from jax.experimental import pallas as pl
from jax.experimental.pallas import tpu as pltpu
from jax.sharding import PartitionSpec as P

EPSILON = 1e-06
BASE_FREQ = 1000000.0
AXES = ("dp", "tensor")
LOG2E = 1.4426950408889634


bf16, f32 = jnp.bfloat16, jnp.float32
NT = (((1,), (1,)), ((), ()))
TN = (((0,), (0,)), ((), ()))


def dot(left, right):
    return jnp.dot(left, right, preferred_element_type=f32)


def dot_nt(left, right):
    return lax.dot_general(left, right, NT, preferred_element_type=f32)


def dot_tn(left, right):
    return lax.dot_general(left, right, TN, preferred_element_type=f32)


def rms_rate(values):
    return lax.rsqrt(jnp.mean(values * values, axis=-1, keepdims=True) + EPSILON)


def rms_back(values, gain, grad):
    rate = rms_rate(values)
    shape = values * rate
    inward = grad * gain
    back = rate * (inward - shape * jnp.mean(inward * shape, axis=-1, keepdims=True))
    return back, grad * shape


class Links:
    def __init__(self, dp, tensor):
        assert tensor == 4 and dp % 2 == 0 and dp & (dp - 1) == 0
        self.dp = dp
        self.bits = (dp // 2).bit_length() - 1
        self.paths = (list(range(self.bits)), list(range(self.bits))[::-1])
        self.slots = []
        for half, path in enumerate(self.paths):
            for p in range(dp // 2):
                offset = sum(1 << bit for j, bit in enumerate(path) if p >> j & 1)
                self.slots.append(2 * offset + half)


def reorder_columns(x, index, slots):
    rows, width = x.shape[0], x.shape[1] // len(slots)
    return jnp.concatenate(
        [lax.dynamic_slice(x, (0, (index ^ r) * width), (rows, width)) for r in slots], axis=1
    )


def restore_columns(x, index, slots):
    rows, width = x.shape[0], x.shape[1] // len(slots)
    place = [0] * len(slots)
    for n, r in enumerate(slots):
        place[r] = n
    place = jnp.asarray(place, jnp.int32)
    return jnp.concatenate(
        [
            lax.dynamic_slice(x, (0, place[index ^ b] * width), (rows, width))
            for b in range(len(slots))
        ],
        axis=1,
    )


def rows_of(part, size):
    return pl.ds(pl.multiple_of(part * size, size), size)


MESH = pl.DeviceIdType.MESH


def repeat(count, step):
    def body(n, carry):
        step(n)
        return carry

    lax.fori_loop(0, count, body, 0)


def blocks_that_leave_first(step, leave):
    def each(n):
        step(2 * n + 1 - 5 * lax.div(n, 2))
        pl.when(n == 1)(leave)

    repeat(4, each)


def twice(step, after_first=None):
    def both(n):
        step(n)
        if after_first is not None:
            pl.when(n == 0)(after_first)

    repeat(2, both)


def flip_bits(value, mask, bits):
    out = value
    for b in range(bits):
        if mask >> b & 1:
            out = out + (1 << b) * (1 - 2 * lax.rem(lax.div(value, 1 << b), 2))
    return out


class Wire:
    def __init__(self, bits, send_sem, recv_sem):
        dp, t = lax.axis_index("dp"), lax.axis_index("tensor")
        self.dp, self.bits = dp, bits
        self.c, self.a = lax.rem(dp, 2), lax.div(dp, 2)
        self.zh, self.zl = lax.div(t, 2), lax.rem(t, 2)
        self.send_sem, self.recv_sem = send_sem, recv_sem
        self.count, self.drains = 0, []
        c, a, zh, zl = self.c, self.a, self.zh, self.zl
        self.core = (2 * a + 1 - c, t)
        self.near = (dp, 2 * zh + 1 - zl)
        self.swapped = (2 * a + zh, 2 * c + zl)
        self.crossed = (2 * a + zh, 2 * (1 - c) + zl)
        self.crossed_back = (2 * a + 1 - zh, 2 * c + zl)
        self.far = [(2 * a + n, 2 * (1 - zh) + zl) for n in range(2)]
        self.plane = [(2 * flip_bits(a, 1 << b, bits) + c, t) for b in range(bits)]
        self.moves = c != zh

    def barrier(self):
        sem = pltpu.get_barrier_semaphore()
        peers = [self.core, self.near] + self.far + self.plane
        for peer in peers:
            pl.semaphore_signal(sem, inc=1, device_id=peer, device_id_type=MESH)
        pl.semaphore_wait(sem, len(peers))

    def part(self, k):
        c, zl = self.c, self.zl
        return 2 * (1 - c if k & 2 else c) + (1 - zl if k & 1 else zl)

    def slot(self, quarter):
        high, low = lax.div(quarter, 2), lax.rem(quarter, 2)
        return 2 * (high + self.c - 2 * high * self.c) + (low + self.zl - 2 * low * self.zl)

    def describe(self, src, dst, n, peer):
        return pltpu.make_async_remote_copy(
            src_ref=src,
            dst_ref=dst,
            send_sem=self.send_sem.at[n],
            recv_sem=self.recv_sem.at[n],
            device_id=peer,
            device_id_type=MESH,
        )

    def post(self, pairs, whole, peer):
        n = self.count
        self.count += 1
        for src, dst in pairs:
            self.describe(src, dst, n, peer).start()
        together = self.describe(whole, whole, n, peer)
        self.drains.append(together.wait_send)
        return together.wait_recv

    def post_one(self, src, dst, peer):
        return self.post([(src, dst)], dst, peer)

    def later(self, src, dst, peer):
        n = self.count
        self.count += 1
        copy = self.describe(src, dst, n, peer)
        self.drains.append(copy.wait_send)
        return copy.wait_recv, copy.start

    def post_swap(self, pairs, whole):
        n = self.count
        self.count += 1
        together = self.describe(whole, whole, n, self.swapped)
        stays = pltpu.make_async_copy(whole, whole, self.recv_sem.at[n])

        @pl.when(self.moves)
        def _():
            for src, dst in pairs:
                self.describe(src, dst, n, self.swapped).start()

        @pl.when(jnp.logical_not(self.moves))
        def _():
            for src, dst in pairs:
                pltpu.make_async_copy(src, dst, self.recv_sem.at[n]).start()

        def arrive():
            pl.when(self.moves)(together.wait_recv)
            pl.when(jnp.logical_not(self.moves))(stays.wait)

        self.drains.append(lambda: pl.when(self.moves)(together.wait_send))
        return arrive

    def drain(self):
        for wait in self.drains:
            wait()
        self.drains = []


def spread_rows(wire, array):
    size = array.shape[0] // 4
    beside = wire.post_one(array.at[0:size, :], array.at[size : 2 * size, :], wire.near)
    partner = wire.post_one(array.at[0:size, :], array.at[2 * size : 3 * size, :], wire.core)

    def relay():
        beside()
        return wire.post_one(array.at[size : 2 * size, :], array.at[3 * size :, :], wire.core)

    return partner, relay


class Reduce:
    def __init__(self, wire, beside, own, landed, total):
        self.wire, self.beside, self.own = wire, beside, own
        self.landed, self.total = landed, total

    def drain(self):
        for n in self.sent:
            self.wire.drains[n]()
            self.wire.drains[n] = lambda: None

    def send_beside(self):
        self.begin_beside()()

    def begin_beside(self):
        self.sent = [len(self.wire.drains)]
        self.first, start = self.wire.later(self.beside.at[1], self.landed.at[0], self.wire.core)
        return start

    def forward(self):
        self.first()
        self.total[...] = (self.beside[0].astype(f32) + self.landed[0].astype(f32)).astype(bf16)
        self.sent.append(len(self.wire.drains))
        self.third = self.wire.post_one(self.total, self.landed.at[2], self.wire.near)

    def send_own(self):
        self.begin_own()()

    def begin_own(self):
        self.sent.append(len(self.wire.drains))
        self.second, start = self.wire.later(self.own.at[1], self.landed.at[1], self.wire.core)
        return start

    def result(self):
        self.second()
        self.third()
        return self.own[0].astype(f32) + self.landed[1].astype(f32) + self.landed[2].astype(f32)


class Scatter:
    def __init__(self, wire, total, landed, block, paths):
        self.wire, self.total, self.landed = wire, total, landed
        self.block, self.paths, self.waits = block, paths, {}
        self.half_rows = total.shape[0] // 2

    def send(self, step, source=None):
        self.begin(step, source)()

    def begin(self, step, source=None):
        have, starts = self.block << step, []
        source = self.total if source is None else source
        for half in range(2):
            start = half * self.half_rows
            there = slice(start + have, start + 2 * have)
            self.waits[half, step], go = self.wire.later(
                source.at[there, :],
                self.landed.at[there, :],
                self.wire.plane[self.paths[half][step]],
            )
            starts.append(go)

        def start_all():
            for go in starts:
                go()

        return start_all

    def add(self, step):
        have = self.block << step
        chunk = min(have, 64)
        for half in range(2):
            start = half * self.half_rows
            self.waits.pop((half, step))()

            def body(n, carry):
                at = pl.multiple_of(n * chunk, chunk)
                to = pl.ds(start + at, chunk)
                more = self.landed[pl.ds(start + have + at, chunk), :]
                self.total[to, :] = (
                    self.total[to, :].astype(f32) + more.astype(f32)
                ).astype(bf16)
                return carry

            lax.fori_loop(0, have // chunk, body, 0)

    def finish(self):
        first = slice(0, self.block)
        other = slice(self.half_rows, self.half_rows + self.block)
        self.waits[0] = self.wire.post_swap(
            [(self.total.at[first, :], self.landed.at[first, :])], self.landed.at[first, :]
        )
        self.waits[1] = self.wire.post_one(
            self.total.at[other, :], self.landed.at[other, :], self.wire.crossed_back
        )

    def step(self, step):
        self.add(step)
        if step:
            self.send(step - 1)
        else:
            self.finish()

    def store(self, dest, write):
        self.waits.pop(0)()
        self.waits.pop(1)()
        other = slice(self.half_rows, self.half_rows + self.block)
        write(self.landed.at[0 : self.block, :], dest.at[0])
        write(self.landed.at[other, :], dest.at[1])


class Columns:
    def __init__(self, q_cols, kv_cols, units):
        self.q_cols, self.kv_cols, self.units = q_cols, kv_cols, units
        self.n_in = q_cols + 2 * kv_cols
        self.o = self.n_in
        self.gate = self.o + q_cols
        self.up = self.gate + units
        self.down = self.up + units
        self.total = self.down + units
        self.back = self.gate


def forward_kernel(bits, slots, cols, width, head_part, reorder, *refs):
    (
        q_w, k_w, v_w, gate_w, up_w, tokens, out_grad, ids_in,
        o_in, down_in, first_in, second_in, q_in, k_in, inverse,
        normed_o, qkv_o, raw_o, mixed_o, totals_o, low_o, grad_o, layer_o, passed_o, unit_o, down_o, second_o,
        weight_o, gains_o, heads_o, cos_o, sin_o, ids_o, rep_o, acts_o,
        weight, acts, grad, normed_two, state_low, normed, qkv, raw, mixed, totals, cos, sin,
        gate, up, inner, gate_grad, up_grad, gate_total, up_total, down_total, gate_landed, up_landed, gains, heads, ids, rep, state, state_grad,
        layer, second, beside_a, own_a, landed_a, total_a, beside_b, own_b, landed_b, total_b,
        gains_w, gain_blocks, o_w, down_w, ids_low,
        send_sem, recv_sem, out_sem,
    ) = refs
    wire = Wire(bits, send_sem, recv_sem)
    size, model = tokens.shape
    q_cols, kv_cols, units = cols.q_cols, cols.kv_cols, cols.units
    n_in = cols.n_in
    dp = len(slots)
    block = model // dp
    half_rows = model // 2
    outs = []

    def write(src, dst):
        outs.append(pltpu.make_async_copy(src, dst, out_sem.at[len(outs)]))
        outs[-1].start()

    def rows(k):
        return slice(k * size, (k + 1) * size)

    lane = lax.broadcasted_iota(jnp.int32, (1, width), 1)
    mine = lax.div(lane, head_part) == wire.dp
    gains_w[...] = jnp.zeros_like(gains_w)
    gains_w[0:1, :block] = first_in[...].astype(f32)
    gains_w[1:2, :block] = second_in[...].astype(f32)
    for n, ref in ((2, q_in), (3, k_in)):
        gains_w[n : n + 1, :width] = jnp.where(
            mine, jnp.concatenate([ref[...].astype(f32)] * dp, axis=1), 0.0
        )
    o_w[...] = o_in[...].T
    down_w[...] = down_in[...].T
    wire.barrier()

    groups = {
        "in": (0, cols.o, [q_w, k_w, v_w]),
        "o": (cols.o, cols.gate, [o_w]),
        "gate": (cols.gate, cols.up, [gate_w]),
        "up": (cols.up, cols.down, [up_w]),
        "down": (cols.down, cols.total, [down_w]),
    }
    paths = (list(range(bits)), list(range(bits))[::-1])
    pending = {}

    def start_weights(name):
        low, high, shards = groups[name]
        for half in range(2):
            there = pl.ds(half * half_rows, block)
            pairs, at = [], low
            for shard in shards:
                pairs.append((shard, weight.at[there, at : at + shard.shape[1]]))
                at += shard.shape[1]
            whole = weight.at[there, low:high]
            if half == 0:
                pending[name, half, 0] = wire.post_swap(pairs, whole)
            else:
                pending[name, half, 0] = wire.post(pairs, whole, wire.crossed)

    def start_gains():
        pending["gains", 0, 0] = wire.post_swap([(gains_w, gain_blocks.at[0])], gain_blocks.at[0])
        there = gain_blocks.at[dp // 2]
        pending["gains", 1, 0] = wire.post([(gains_w, there)], there, wire.crossed)

    def step_gains(step):
        for half in range(2):
            pending.pop(("gains", half, step))()
            if step < bits:
                have, start = 1 << step, half * (dp // 2)
                pending["gains", half, step + 1] = wire.post_one(
                    gain_blocks.at[start : start + have],
                    gain_blocks.at[start + have : start + 2 * have],
                    wire.plane[paths[half][step]],
                )

    def step_weights(name, step):
        low, high, _ = groups[name]
        for half in range(2):
            pending.pop((name, half, step))()
            if step < bits:
                have = block << step
                start = half * half_rows
                pending[name, half, step + 1] = wire.post_one(
                    weight.at[start : start + have, low:high],
                    weight.at[start + have : start + 2 * have, low:high],
                    wire.plane[paths[half][step]],
                )

    def swap_rows(source, dest):
        own = dest.at[0:size, :]
        if reorder:
            pairs = [
                (
                    source.at[
                        :,
                        pl.ds(
                            pl.multiple_of(flip_bits(wire.dp, r, bits + 1) * block, block), block
                        ),
                    ],
                    dest.at[0:size, n * block : (n + 1) * block],
                )
                for n, r in enumerate(slots)
            ]
        else:
            pairs = [(source, own)]
        return wire.post_swap(pairs, own)

    start_gains()
    start_weights("in")

    base = lax.broadcasted_iota(jnp.int32, (size, width), 0).astype(f32) * inverse[0:1, :]
    base_cos, base_sin = jnp.cos(base), jnp.sin(base)
    sign = jnp.where(lax.broadcasted_iota(jnp.int32, (1, width), 1) < width // 2, -1.0, 1.0)
    for k in range(4):
        more = (wire.part(k) * size).astype(f32) * inverse[...]
        more_cos, more_sin = jnp.cos(more)[0:1], jnp.sin(more)[0:1]
        cos[rows(k), :] = base_cos * more_cos - base_sin * more_sin
        sin[rows(k), :] = (base_sin * more_cos + base_cos * more_sin) * sign
    write(cos, cos_o)
    write(sin, sin_o)

    step_gains(0)
    step_weights("in", 0)
    acts_here = swap_rows(tokens, acts)
    ids_here = wire.post_swap([(ids_in, ids_low)], ids_low)
    start_weights("o")
    for step in range(1, bits):
        step_gains(step)
        step_weights("in", step)
    acts_here()
    acts_partner, acts_relay = spread_rows(wire, acts)
    start_weights("gate")
    start_weights("up")
    ids_here()
    ids[...] = jnp.broadcast_to(ids_low[...].astype(f32), ids.shape)
    rep[...] = jnp.broadcast_to(ids[0:1, :], (128, 4 * size)).T
    write(ids, ids_o)
    write(rep, rep_o)
    write(acts.at[0:size, :], acts_o)
    step_weights("o", 0)
    step_gains(bits)
    step_weights("in", bits)

    for n in range(dp):
        gains[:, n * block : (n + 1) * block] = gain_blocks[n, :, :block]
    summed = gain_blocks[0, :, :width]
    for n in range(1, dp):
        summed = summed + gain_blocks[n, :, :width]
    heads[0:8, :] = jnp.broadcast_to(summed[2:3, :], (8, width))
    heads[8:16, :] = jnp.broadcast_to(summed[3:4, :], (8, width))
    write(gains, gains_o)
    write(heads, heads_o)
    first_gain, second_gain = gains[0:1, :], gains[1:2, :]
    q_gain, k_gain = heads[0:1, :], heads[8:9, :]

    def front(k):
        here = rows_of(k, size)
        values = acts[here, :].astype(f32)
        low = (values * rms_rate(values) * first_gain).astype(bf16)
        normed[here, :] = low
        product = dot(low, weight[:, :n_in])
        c, s = cos[here, :], sin[here, :]
        for at in range(0, q_cols + kv_cols, width):
            head = product[:, at : at + width]
            raw[here, at : at + width] = head
            head = head * rms_rate(head) * (q_gain if at < q_cols else k_gain)
            turn = head * c + pltpu.roll(head, width // 2, 1) * s
            qkv[here, at : at + width] = turn.astype(bf16)
        qkv[here, q_cols + kv_cols :] = product[:, q_cols + kv_cols :].astype(bf16)

    acts_partner()
    twice(lambda n: front(2 * n))
    for step in range(1, bits):
        step_weights("o", step)
    acts_across = acts_relay()
    acts_across()
    twice(lambda n: front(2 * n + 1))
    write(normed, normed_o)
    write(qkv, qkv_o)
    write(raw, raw_o)

    factor = width ** (-0.5) * LOG2E
    ones = jnp.ones((4 * size, width), bf16)
    assert q_cols == 2 * kv_cols

    def attend(quarter, count, masked):
        place = pl.multiple_of(wire.slot(quarter) * size, size)
        here = pl.ds(place, size)
        seen_by = rep[pl.ds(pl.multiple_of(quarter * size, size), size), :]
        seen_by = jnp.concatenate([seen_by] * (size // 128), axis=1)

        def lanes(at):
            return pl.ds(pl.multiple_of(at, width), width)

        def head(h):
            first, second = lanes(2 * h * width), lanes((2 * h + 1) * width)
            key_at, value_at = lanes(q_cols + h * width), lanes(q_cols + kv_cols + h * width)
            query = jnp.concatenate([qkv[here, first], qkv[here, second]], 0)
            probs, values = [], []
            for n in range(count):
                there = rows_of(wire.slot(jnp.int32(n)), size)
                prob = jnp.exp2(dot_nt(query, qkv[there, key_at]) * factor)
                if n in masked:
                    seen = ids[0:1, n * size : (n + 1) * size] <= seen_by
                    prob = jnp.where(jnp.concatenate([seen, seen], 0), prob, 0.0)
                probs.append(prob.astype(bf16))
                values.append(qkv[there, value_at])
            value = jnp.concatenate([jnp.concatenate(values, 0), ones[: count * size]], axis=1)
            out = dot(jnp.concatenate(probs, axis=1), value)
            total = out[:, width:]
            out = (out[:, :width] / total).astype(bf16)
            mixed[here, first] = out[:size]
            mixed[here, second] = out[size:]
            totals[pl.ds(quarter * (kv_cols // width) + h, 1), :] = total.T[0:1]

        repeat(kv_cols // width, head)
        return here

    def attend_pair(first, dest):
        here = attend(first, 3, (0, 1, 2))
        dest[wire.c] = dot_nt(mixed[here, :], weight[:, cols.o : cols.gate]).astype(bf16)
        here = attend(first + 2, 4, (2, 3))
        dest[1 - wire.c] = dot_nt(mixed[here, :], weight[:, cols.o : cols.gate]).astype(bf16)

    grad_here = swap_rows(out_grad, grad)
    start_weights("down")
    step_weights("o", bits)
    reduce_o = Reduce(wire, beside_a, own_a, landed_a, total_a)
    attend_pair(1 - wire.zl, beside_a)
    reduce_o.send_beside()
    step_weights("gate", 0)
    step_weights("up", 0)
    reduce_o.forward()
    attend_pair(wire.zl, own_a)
    reduce_o.send_own()
    for step in range(1, bits):
        step_weights("gate", step)
        step_weights("up", step)
    write(mixed, mixed_o)
    write(totals, totals_o)
    write(weight.at[:, : cols.back], weight_o)
    state[...] = acts[0:size, :].astype(f32) + reduce_o.result()
    values = state[...]
    normed_two[0:size, :] = (values * rms_rate(values) * second_gain).astype(bf16)
    two_partner, two_relay = spread_rows(wire, normed_two)
    grad_here()
    step_weights("down", 0)
    step_weights("gate", bits)
    step_weights("up", bits)

    def units_forward(k):
        here = rows_of(k, size)
        values = normed_two[here, :]
        gate[here, :] = dot(values, weight[:, cols.gate : cols.up])
        up[here, :] = dot(values, weight[:, cols.up : cols.down])

    def units_back(k, dest):
        here = rows_of(k, size)
        gate_here, up_here = gate[here, :], up[here, :]
        inward = dot(grad[here, :], weight[:, cols.down : cols.total])
        sg = jax.nn.sigmoid(gate_here)
        silu = gate_here * sg
        inner[here, :] = (silu * up_here).astype(bf16)
        d_gate = (inward * up_here * sg * (1.0 + gate_here * (1.0 - sg))).astype(bf16)
        d_up = (inward * silu).astype(bf16)
        gate_grad[here, :] = d_gate
        up_grad[here, :] = d_up
        dest[...] = (
            dot_nt(d_gate, weight[:, cols.gate : cols.up])
            + dot_nt(d_up, weight[:, cols.up : cols.down])
        ).astype(bf16)

    two_partner()
    twice(lambda n: units_forward(2 * n))
    two_across = two_relay()
    grad_partner, grad_relay = spread_rows(wire, grad)
    two_across()
    twice(lambda n: units_forward(2 * n + 1))
    for step in range(1, bits):
        step_weights("down", step)
    grad_partner()
    grad_across = grad_relay()
    grad_across()
    step_weights("down", bits)
    reduce_two = Reduce(wire, beside_b, own_b, landed_b, total_b)
    twice(lambda n: units_back(3 - 2 * n, beside_b.at[1 - n]), reduce_two.begin_beside())
    reduce_two.forward()
    twice(lambda n: units_back(2 - 2 * n, own_b.at[1 - n]), reduce_two.begin_own())

    quarter_rows = half_rows // 2

    def unit_block(total, left, right, n):
        columns = rows_of(n, quarter_rows)
        total[columns, :] = dot_tn(left[:, columns], right[...]).astype(bf16)

    scatter_gate = Scatter(wire, gate_total, gate_landed, block, paths)
    scatter_up = Scatter(wire, up_total, up_landed, block, paths)
    def unit_blocks(scatter, total, left, right):
        blocks_that_leave_first(
            lambda n: unit_block(total, left, right, n), scatter.begin(bits - 1)
        )

    unit_blocks(scatter_gate, gate_total, normed_two, gate_grad)
    unit_blocks(scatter_up, up_total, normed_two, up_grad)
    back, gain_part = rms_back(state[...], second_gain, reduce_two.result())
    second[...] = jnp.broadcast_to(jnp.sum(gain_part, axis=0, keepdims=True), second.shape)
    state_grad[...] = grad[0:size, :].astype(f32) + back
    state_low[0:size, :] = state_grad[...].astype(bf16)
    reduce_o.drain()
    low_partner, low_relay = spread_rows(wire, state_low)
    write(second, second_o)
    write(state_grad, grad_o)
    repeat(4, lambda n: unit_block(down_total, grad, inner, n))
    write(down_total, down_o)
    scatter_gate.add(bits - 1)
    if bits > 1:
        scatter_gate.send(bits - 2)

    def layer_part(k):
        return dot_nt(inner[rows(k), :], weight[:, cols.down : cols.total])

    beside_a[1] = layer_part(3).astype(bf16)
    layer_first = wire.post_one(beside_a.at[1], landed_a.at[0], wire.core)
    own_a[1] = layer_part(2).astype(bf16)
    layer_second = wire.post_one(own_a.at[1], landed_a.at[1], wire.core)
    passing = layer_part(1)
    layer_first()
    total_a[...] = (passing + landed_a[0].astype(f32)).astype(bf16)
    write(total_a, passed_o)
    staying = layer_part(0)
    layer_second()
    layer[...] = state[...] + staying + landed_a[1].astype(f32)
    write(layer, layer_o)
    scatter_up.add(bits - 1)
    if bits > 1:
        scatter_up.send(bits - 2)
    low_partner()
    low_across = low_relay()
    for step in range(bits - 2, -1, -1):
        for scatter in (scatter_gate, scatter_up):
            scatter.add(step)
            if step:
                scatter.send(step - 1)
    for half in range(2):
        start = half * half_rows
        write(gate_total.at[start : start + block, :], unit_o.at[0, half])
        write(up_total.at[start : start + block, :], unit_o.at[1, half])
    low_across()
    write(state_low, low_o)
    for copy in outs:
        copy.wait()
    wire.drain()


def back_kernel(bits, slots, cols, width, restore, *refs):
    (
        weight_i, qkv_i, raw_i, mixed_i, totals_i, low_i, normed_i, cos_i, sin_i, ids_i, rep_i,
        gains_i, heads_i, grad_i, acts_i, second_i, layer_i, unit_i, passed_i, up_i,
        layer_o, tokens_o, in_o, o_o, unit_o, gain_o, up_o,
        weight, qkv, raw, mixed, totals, state_low, normed, cos, sin, ids, rep, gains, heads,
        state_grad, acts, second, layer, unit,
        mixed_grad, q_grad, k_acc, v_acc, qkv_grad, in_total, o_total, gain_total,
        in_landed, o_landed, unit_landed, gain_landed, up_landed, layer_near, layer_own, layer_landed,
        tokens_own, tokens_landed, head_grads, shared, shared_landed, spread,
        beside, own, landed, total, send_sem, recv_sem, in_sem, out_sem,
    ) = refs
    wire = Wire(bits, send_sem, recv_sem)
    size, model = acts.shape
    q_cols, kv_cols, units, n_in = cols.q_cols, cols.kv_cols, cols.units, cols.n_in
    dp = len(slots)
    block, half_rows = model // dp, model // 2
    paths = (list(range(bits)), list(range(bits))[::-1])
    loads, outs = {}, []

    def load(name, src, dst):
        loads[name] = pltpu.make_async_copy(src, dst, in_sem.at[len(loads)])
        loads[name].start()

    taken = set()

    def need(*names):
        for name in names:
            if name not in taken:
                taken.add(name)
                loads[name].wait()

    def write(src, dst):
        outs.append(pltpu.make_async_copy(src, dst, out_sem.at[len(outs)]))
        outs[-1].start()

    def rows(k):
        return slice(k * size, (k + 1) * size)

    for name, src, dst in (
        ("low", low_i, state_low),
        ("weight", weight_i, weight),
        ("mixed", mixed_i, mixed),
        ("unit", unit_i, unit),
        ("qkv", qkv_i, qkv),
        ("totals", totals_i, totals),
        ("ids", ids_i, ids),
        ("rep", rep_i, rep),
        ("cos", cos_i, cos),
        ("sin", sin_i, sin),
        ("raw", raw_i, raw),
        ("heads", heads_i, heads),
        ("normed", normed_i, normed),
        ("gains", gains_i, gains),
        ("grad", grad_i, state_grad),
        ("acts", acts_i, acts),
        ("second", second_i, second),
        ("layer", layer_i, layer),
    ):
        load(name, src, dst)
    wire.barrier()

    def swap_out(source, dest):
        if restore:
            seq = 2 * wire.a + wire.zh
            pairs = [
                (
                    source.at[:, n * block : (n + 1) * block],
                    dest.at[
                        :,
                        pl.ds(
                            pl.multiple_of(flip_bits(seq, r, bits + 1) * block, block), block
                        ),
                    ],
                )
                for n, r in enumerate(slots)
            ]
        else:
            pairs = [(source, dest)]
        return wire.post_swap(pairs, dest)

    up_here = []
    for n in range(2):
        first, other = up_landed.at[n, 0], up_landed.at[n, 1]
        up_here.append(wire.post_swap([(up_i.at[n, 0], first)], first))
        up_here.append(wire.post_one(up_i.at[n, 1], other, wire.crossed_back))
    layer_beside = wire.post_one(passed_i, layer_near, wire.near)
    scatter_unit = Scatter(wire, unit, unit_landed, block, paths)
    scatter_unit.send(bits - 1, unit_i)
    scatter_in = Scatter(wire, in_total, in_landed, block, paths)
    scatter_o = Scatter(wire, o_total, o_landed, block, paths)
    scatter_gain = Scatter(wire, gain_total, gain_landed, block, paths)

    need("low", "weight")

    def project(k):
        here = rows_of(k, size)
        mixed_grad[here, :] = dot(state_low[here, :], weight[:, cols.o : cols.o + q_cols]).astype(
            bf16
        )

    repeat(4, project)
    need("mixed")
    scale = width ** (-0.5)
    factor = scale * LOG2E
    k_acc[...] = jnp.zeros_like(k_acc)
    v_acc[...] = jnp.zeros_like(v_acc)
    ones = jnp.ones((8, width), bf16)
    need("qkv", "totals", "ids", "rep")

    def there_of(quarter):
        return rows_of(wire.slot(jnp.int32(quarter)), size)

    def attend_back(quarter):
        here, count = there_of(quarter), min(quarter + 2, 4)
        row_ids = ids[0:1, quarter * size : (quarter + 1) * size]
        row_ids = jnp.concatenate([row_ids, row_ids], axis=1)
        for h in range(kv_cols // width):
            q_at, k_at = 2 * h * width, q_cols + h * width
            v_at = k_at + kv_cols

            def both(ref):
                return jnp.concatenate(
                    [ref[here, q_at : q_at + width], ref[here, q_at + width : q_at + 2 * width]], 0
                )

            query, out_grad = both(qkv), both(mixed_grad)
            product = out_grad.astype(f32) * both(mixed).astype(f32)
            product_high = product.astype(bf16)
            product_low = (product - product_high.astype(f32)).astype(bf16)
            centre = (dot_nt(ones, product_high) + dot_nt(ones, product_low))[0:1]
            n = quarter * (kv_cols // width) + h
            level = -jnp.log2(totals[n : n + 1, :])
            columns = slice(h * width, (h + 1) * width)
            score_grads, keys = [], []
            for m in range(count):
                there = there_of(m)
                key, value = qkv[there, k_at : k_at + width], qkv[there, v_at : v_at + width]
                prob = jnp.exp2(dot_nt(key, query) * factor + level)
                if m >= quarter:
                    key_ids = rep[m * size : (m + 1) * size, :]
                    seen = jnp.concatenate([key_ids] * (2 * size // 128), axis=1) <= row_ids
                    prob = jnp.where(seen, prob, 0.0)
                score_grad = (prob * (dot_nt(value, out_grad) - centre)).astype(bf16)
                v_acc[there, columns] += dot(prob.astype(bf16), out_grad)
                k_acc[there, columns] += dot(score_grad, query)
                score_grads.append(score_grad)
                keys.append(key)
            back = dot_tn(jnp.concatenate(score_grads, 0), jnp.concatenate(keys, 0))
            q_grad[here, q_at : q_at + width] = back[:size]
            q_grad[here, q_at + width : q_at + 2 * width] = back[size:]

    def o_block(n):
        columns = rows_of(n, half_rows // 2)
        o_total[columns, :] = dot_tn(state_low[:, columns], mixed[...]).astype(bf16)

    repeat(4, o_block)
    scatter_o.send(bits - 1)
    attend_back(3)
    attend_back(2)
    attend_back(1)
    need("unit")
    scatter_unit.step(bits - 1)
    attend_back(0)
    need("layer")
    layer_beside()
    layer_own[...] = (layer[...] + layer_near[...].astype(f32)).astype(bf16)
    layer_here = swap_out(layer_own, layer_landed)

    need("cos", "sin", "raw", "heads")
    head_grads[...] = jnp.zeros_like(head_grads)

    def heads_back(k, dest):
        here = rows_of(k, size)
        c, s = cos[here, :], sin[here, :]
        for at in range(0, q_cols + kv_cols, width):
            is_q = at < q_cols
            source = q_grad[here, at : at + width] if is_q else k_acc[here, at - q_cols : at - q_cols + width]
            turned = source * scale
            grad = turned * c - pltpu.roll(turned, width // 2, 1) * s
            n = 0 if is_q else 8
            back, part = rms_back(raw[here, at : at + width], heads[n : n + 1, :], grad)
            qkv_grad[here, at : at + width] = back.astype(bf16)
            head_grads[n : n + 8, :] += jnp.sum(part.reshape(size // 8, 8, width), axis=0)
        qkv_grad[here, q_cols + kv_cols :] = v_acc[here, :].astype(bf16)
        dest[...] = dot_nt(qkv_grad[here, :], weight[:, :n_in]).astype(bf16)

    reduce = Reduce(wire, beside, own, landed, total)
    twice(lambda n: heads_back(3 - 2 * n, beside.at[1 - n]), reduce.begin_beside())
    reduce.forward()
    for step in range(bits - 1, 0, -1):
        scatter_o.add(step)
        scatter_o.send(step - 1)
        scatter_unit.step(step - 1)
    twice(lambda n: heads_back(2 - 2 * n, own.at[1 - n]), reduce.begin_own())
    need("normed")

    def in_block(n):
        columns = rows_of(n, half_rows // 2)
        in_total[columns, :] = dot_tn(normed[:, columns], qkv_grad[...]).astype(bf16)

    blocks_that_leave_first(in_block, scatter_in.begin(bits - 1))
    need("gains", "grad", "acts", "second")
    inward = reduce.result()
    back, part = rms_back(acts[...].astype(f32), gains[0:1, :], inward)
    tokens_own[...] = (state_grad[...] + back).astype(bf16)
    tokens_here = swap_out(tokens_own, tokens_landed)

    shared[0:1, :model] = jnp.sum(part, axis=0, keepdims=True)
    shared[1:2, :model] = second[0:1, :]
    shared[2:8, :model] = jnp.zeros((6, model), f32)
    shared[0:1, model:] = jnp.sum(head_grads[0:8, :], axis=0, keepdims=True)
    shared[1:2, model:] = jnp.sum(head_grads[8:16, :], axis=0, keepdims=True)
    shared[2:8, model:] = jnp.zeros((6, width), f32)
    from_core = wire.post_one(shared, shared_landed.at[0], wire.core)
    scatter_in.add(bits - 1)
    if bits > 1:
        scatter_in.send(bits - 2)
    from_core()
    shared_landed[1] = shared[...] + shared_landed[0]
    from_near = wire.post_one(shared_landed.at[1], shared_landed.at[2], wire.near)
    from_near()
    summed = shared_landed[1] + shared_landed[2]
    spread[...] = jnp.zeros_like(spread)
    spread[0:2, :] = summed[0:2, :model]
    piece = min(block, width)
    for which in range(2):
        for j in range(width // piece):
            row = summed[which : which + 1, model + j * piece : model + (j + 1) * piece]
            if piece < block:
                row = jnp.concatenate([row, jnp.zeros((1, block - piece), f32)], axis=1)
            n = 2 + which * (width // piece) + j
            spread[n : n + 1, :] = jnp.concatenate([row] * dp, axis=1)
    gain_total[...] = spread[...].T.astype(bf16)
    scatter_gain.send(bits - 1)
    for arrive in up_here:
        arrive()
    write(up_landed, up_o)
    scatter_unit.store(unit_o, write)
    scatter_gain.add(bits - 1)
    for step in range(bits - 2, -1, -1):
        scatter_gain.send(step)
        scatter_in.add(step)
        if step:
            scatter_in.send(step - 1)
        else:
            scatter_in.finish()
        scatter_gain.add(step)
    if bits == 1:
        scatter_in.finish()
    scatter_gain.finish()
    scatter_o.add(0)
    scatter_o.finish()
    tokens_here()
    write(tokens_landed, tokens_o)
    scatter_in.store(in_o, write)
    layer_here()
    write(layer_landed, layer_o)
    scatter_gain.store(gain_o, write)
    scatter_o.store(o_o, write)
    for copy in outs:
        copy.wait()
    wire.drain()


def finish_kernel(cols, width, head_part, *refs):
    (
        layer_i, tokens_i, in_i, o_i, down_i, gain_i, unit_i,
        layer_o, tokens_o, first_o, q_o, k_o, v_o, qs_o, ks_o, o_o, second_o, gate_o, up_o, down_o,
    ) = refs
    q_cols, kv_cols, units = cols.q_cols, cols.kv_cols, cols.units
    layer_o[...] = layer_i[...]
    tokens_o[...] = tokens_i[...].astype(f32)

    def both(ref, low, high):
        return ref[0, :, low:high].astype(f32) + ref[1, :, low:high].astype(f32)

    q_o[...] = both(in_i, 0, q_cols)
    k_o[...] = both(in_i, q_cols, q_cols + kv_cols)
    v_o[...] = both(in_i, q_cols + kv_cols, cols.n_in)
    o_o[...] = both(o_i, 0, q_cols).T
    gate_o[...] = both(unit_i.at[0], 0, units)
    up_o[...] = both(unit_i.at[1], 0, units)
    down_o[...] = both(down_i, 0, units).T
    turned = both(gain_i, 0, 128).T
    first_o[...] = turned[0:1, :]
    second_o[...] = turned[1:2, :]
    block = turned.shape[1]
    piece = min(block, width)
    count = width // piece
    dp = lax.axis_index("dp")
    for which, ref in enumerate((qs_o, ks_o)):
        at = 2 + which * count
        whole = jnp.concatenate([turned[at + j : at + j + 1, :piece] for j in range(count)], axis=1)
        out = jnp.zeros((1, head_part), f32)
        for n in range(width // head_part):
            out = jnp.where(dp == n, whole[:, n * head_part : (n + 1) * head_part], out)
        ref[...] = out


VMEM_SPEC = pl.BlockSpec(memory_space=pltpu.VMEM)
ANY_SPEC = pl.BlockSpec(memory_space=pl.ANY)


def forward(links, shards, tokens, out_grad, ids, small, width, head_part, reorder):
    q_w, k_w, gate_w = shards[0], shards[1], shards[3]
    cols = Columns(q_w.shape[1], k_w.shape[1], gate_w.shape[1])
    length, model = ids.shape[1], tokens.shape[1]
    size, block = length // 4, q_w.shape[0]
    shape = jax.ShapeDtypeStruct
    n_qk, units = cols.q_cols + cols.kv_cols, cols.units
    n_totals = 4 * cols.kv_cols // width
    outs = [
        ((length, model), bf16),
        ((length, cols.n_in), bf16),
        ((length, n_qk), f32),
        ((length, cols.q_cols), bf16),
        ((n_totals, 2 * size), f32),
        ((length, model), bf16),
        ((size, model), f32),
        ((size, model), f32),
        ((size, model), bf16),
        ((2, 2, block, units), bf16),
        ((model, units), bf16),
        ((8, model), f32),
        ((model, cols.back), bf16),
        ((8, model), f32),
        ((16, width), f32),
        ((length, width), f32),
        ((length, width), f32),
        ((8, length), f32),
        ((length, 128), f32),
        ((size, model), bf16),
    ]
    reduce_set = [((2, size, model), bf16)] * 2 + [((3, size, model), bf16), ((size, model), bf16)]
    scratch = (
        [((model, cols.total), bf16)]
        + [((length, model), bf16)] * 5
        + [
            ((length, cols.n_in), bf16),
            ((length, n_qk), f32),
            ((length, cols.q_cols), bf16),
            ((n_totals, 2 * size), f32),
            ((length, width), f32),
            ((length, width), f32),
            ((length, units), f32),
            ((length, units), f32),
            ((length, units), bf16),
            ((length, units), bf16),
            ((length, units), bf16),
            ((model, units), bf16),
            ((model, units), bf16),
            ((model, units), bf16),
            ((model, units), bf16),
            ((model, units), bf16),
            ((8, model), f32),
            ((16, width), f32),
            ((8, length), f32),
            ((length, 128), f32),
            ((size, model), f32),
            ((size, model), f32),
            ((size, model), f32),
            ((8, model), f32),
        ]
        + reduce_set * 2
        + [((8, max(block, 128)), f32), ((links.dp, 8, max(block, 128)), f32)]
        + [((block, cols.q_cols), bf16), ((block, units), bf16)]
        + [((1, length), jnp.int32)]
    )
    n_wire = 2 * 8 * (links.bits + 1) + 36
    args = list(shards) + [tokens, out_grad, ids]
    return pl.pallas_call(
        partial(forward_kernel, links.bits, links.slots, cols, width, head_part, reorder),
        name="forward",
        out_shape=[shape(*o) for o in outs],
        in_specs=[ANY_SPEC] * len(args) + [VMEM_SPEC] * len(small),
        out_specs=[ANY_SPEC] * len(outs),
        scratch_shapes=[pltpu.VMEM(*s) for s in scratch]
        + [pltpu.SemaphoreType.DMA((n_wire,))] * 2
        + [pltpu.SemaphoreType.DMA((32,))],
        compiler_params=pltpu.CompilerParams(
            vmem_limit_bytes=66 * 10**6, collective_id=0, has_side_effects=True
        ),
    )(*args, *small)


def backward(links, args, cols, width, restore):
    weight, qkv, unit, acts = args[0], args[1], args[17], args[14]
    length, (size, model) = qkv.shape[0], acts.shape
    block = model // links.dp
    q_cols, kv_cols, n_in, units = cols.q_cols, cols.kv_cols, cols.n_in, cols.units
    shape = jax.ShapeDtypeStruct
    outs = [
        ((size, model), bf16),
        ((size, model), bf16),
        ((2, block, n_in), bf16),
        ((2, block, q_cols), bf16),
        ((2, block, units), bf16),
        ((2, block, 128), bf16),
        ((2, 2, block, units), bf16),
    ]
    loaded = args[:18]
    scratch = [(a.shape, a.dtype) for a in loaded] + [
        ((length, q_cols), bf16),
        ((length, q_cols), f32),
        ((length, kv_cols), f32),
        ((length, kv_cols), f32),
        ((length, n_in), bf16),
        ((model, n_in), bf16),
        ((model, q_cols), bf16),
        ((model, 128), bf16),
        ((model, n_in), bf16),
        ((model, q_cols), bf16),
        (unit.shape, bf16),
        ((model, 128), bf16),
        ((2, 2, block, units), bf16),
        ((size, model), bf16),
        ((size, model), bf16),
        ((size, model), bf16),
        ((size, model), bf16),
        ((size, model), bf16),
        ((16, width), f32),
        ((8, model + width), f32),
        ((3, 8, model + width), f32),
        ((128, model), f32),
        ((2, size, model), bf16),
        ((2, size, model), bf16),
        ((3, size, model), bf16),
        ((size, model), bf16),
    ]
    n_wire = 4 * 2 * (links.bits + 1) + 16
    return pl.pallas_call(
        partial(back_kernel, links.bits, links.slots, cols, width, restore),
        name="backward",
        out_shape=[shape(*o) for o in outs],
        in_specs=[ANY_SPEC] * len(args),
        out_specs=[ANY_SPEC] * len(outs),
        scratch_shapes=[pltpu.VMEM(*s) for s in scratch]
        + [pltpu.SemaphoreType.DMA((n_wire,))] * 2
        + [pltpu.SemaphoreType.DMA((32,))] * 2,
        compiler_params=pltpu.CompilerParams(
            vmem_limit_bytes=66 * 10**6, collective_id=1, has_side_effects=True
        ),
    )(*args)


def finish(sums, cols, width, head_part):
    block, (size, model) = sums[2].shape[1], sums[0].shape
    shape = jax.ShapeDtypeStruct
    outs = [
        (block_out, f32)
        for block_out in (
            (size, model),
            (1, block),
            (block, cols.q_cols),
            (block, cols.kv_cols),
            (block, cols.kv_cols),
            (1, head_part),
            (1, head_part),
            (cols.q_cols, block),
            (1, block),
            (block, cols.units),
            (block, cols.units),
            (cols.units, block),
        )
    ]
    return pl.pallas_call(
        partial(finish_kernel, cols, width, head_part),
        name="finish",
        out_shape=[shape((size, model), bf16)] + [shape(*o) for o in outs],
        in_specs=[VMEM_SPEC] * len(sums),
        out_specs=[VMEM_SPEC] * (1 + len(outs)),
    )(*sums)


def body(
    links,
    tokens,
    block_ids,
    norm1_gain,
    q_weight,
    key_projection,
    value_projection,
    q_gain,
    k_gain,
    o_weight,
    norm2_gain,
    gate_weight,
    up_weight,
    down_weight,
    out_grad,
):
    dp, slots = links.dp, links.slots
    dp_index = lax.axis_index("dp")

    length, model = block_ids.shape[1], tokens.shape[1]
    gain_width, head_part = norm1_gain.shape[0], q_gain.shape[0]
    width = head_part * dp
    cols = Columns(q_weight.shape[1], key_projection.shape[1], gate_weight.shape[1])
    inverse = BASE_FREQ ** (-2.0 * (np.arange(width) % (width // 2)) / width)
    inverse = jnp.asarray(np.broadcast_to(inverse[None, :], (8, width)), f32)
    reorder = gain_width % 128 == 0
    if not reorder:
        tokens = reorder_columns(tokens, dp_index, slots)
        out_grad = reorder_columns(out_grad, dp_index, slots)
    (
        normed,
        qkv,
        raw,
        mixed,
        totals,
        state_low,
        state_grad,
        layer_sum,
        passed,
        unit_sum,
        down_total,
        second_part,
        weight,
        gains,
        heads,
        cosine,
        sine,
        block_of,
        block_rep,
        acts,
    ) = forward(
        links,
        [q_weight, key_projection, value_projection, gate_weight, up_weight],
        tokens,
        out_grad,
        block_ids,
        [o_weight, down_weight]
        + [gain[None, :] for gain in (norm1_gain, norm2_gain, q_gain, k_gain)]
        + [inverse],
        width,
        head_part,
        reorder,
    )
    sums = backward(
        links,
        [
            weight, qkv, raw, mixed, totals, state_low, normed, cosine, sine, block_of, block_rep,
            gains, heads, state_grad, acts, second_part, layer_sum, down_total, passed, unit_sum,
        ],
        cols,
        width,
        reorder,
    )
    if not reorder:
        sums = list(sums)
        sums[:2] = [restore_columns(x, dp_index, slots) for x in sums[:2]]
    outs = list(finish(sums, cols, width, head_part))
    for n in (2, 6, 7, 9):
        outs[n] = outs[n][0]
    return tuple(outs)


def solution(mesh):
    links = Links(mesh.shape["dp"], mesh.shape["tensor"])
    return jax.shard_map(
        partial(body, links),
        mesh=mesh,
        in_specs=(
            P(("dp", "tensor"), None),
            P("dp", None),
            P("dp"),
            P("dp", "tensor"),
            P("dp", "tensor"),
            P("dp", "tensor"),
            P("dp"),
            P("dp"),
            P("tensor", "dp"),
            P("dp"),
            P("dp", "tensor"),
            P("dp", "tensor"),
            P("tensor", "dp"),
            P(("dp", "tensor"), None),
        ),
        out_specs=(
            P(("dp", "tensor"), None),
            P(("dp", "tensor"), None),
            P("dp"),
            P("dp", "tensor"),
            P("dp", "tensor"),
            P("dp", "tensor"),
            P("dp"),
            P("dp"),
            P("tensor", "dp"),
            P("dp"),
            P("dp", "tensor"),
            P("dp", "tensor"),
            P("tensor", "dp"),
        ),
        check_vma=False,
    )
```
